128 devices in a mesh: dp: 1, cp: 16 (over z, y), tp: 8 (over x, core).
Axes of the slice: x: 4, y: 4, z: 4, core: 2. Of those that a mesh axis runs over, the one named last changes fastest.
Arguments:
- x: bfloat16 [1, 16384, 4096], P('dp', ('cp', 'tp'))
- g_attn: bfloat16 [4096], replicated
- w_q: bfloat16 [4096, 32, 128], P(None, 'tp')
- w_k: bfloat16 [4096, 8, 128], P(None, 'tp')
- w_v: bfloat16 [4096, 8, 128], P(None, 'tp')
- w_o: bfloat16 [32, 128, 4096], P('tp')
- g_mlp: bfloat16 [4096], replicated
- w_gate: bfloat16 [4096, 14336], P(None, 'tp')
- w_up: bfloat16 [4096, 14336], P(None, 'tp')
- w_down: bfloat16 [14336, 4096], P('tp')
Outputs:
- output: bfloat16 [1, 16384, 4096], P('dp', ('cp', 'tp'))
All inputs are finite; a program needn't handle non-finite values.
Results may differ from the reference program's by a relative error of at most 0.02.
Values are sent between devices in bfloat16 or wider.
A program may use at most 1 GiB of HBM per device.

```python
import math
import jax
import jax.numpy as jnp
from jax import lax

SEQ_LEN = 16384
MODEL_DIM = 4096
N_HEADS = 32
N_KV_HEADS = 8
HEAD_DIM = 128
FFN_DIM = 14336
CP_SIZE = 16
Q_BLOCK = 128
NORM_EPS = 1e-5
ROPE_THETA = 500000.0


def stored_positions(row_ids):
    piece_len = SEQ_LEN // (2 * CP_SIZE)
    owner_cp = row_ids // (2 * piece_len)
    within = row_ids % (2 * piece_len)
    return jnp.where(within < piece_len, owner_cp * piece_len + within,
                     (2 * CP_SIZE - 1 - owner_cp) * piece_len + within - piece_len)


def rms_norm(rows_in, gain_vec):
    rows_f32 = rows_in.astype(jnp.float32)
    mean_sq = jnp.mean(rows_f32 * rows_f32, axis=-1, keepdims=True)
    return (rows_f32 * lax.rsqrt(mean_sq + NORM_EPS) * gain_vec.astype(jnp.float32)).astype(jnp.bfloat16)


def apply_rope(heads_in, positions):
    half_dim = HEAD_DIM // 2
    inv_freq = ROPE_THETA ** (-2.0 * jnp.arange(half_dim, dtype=jnp.float32) / HEAD_DIM)
    angles = positions.astype(jnp.float32)[:, None] * inv_freq[None, :]
    angles = jnp.concatenate([angles, angles], axis=-1)[:, None, :]
    heads_f32 = heads_in.astype(jnp.float32)
    rotated = jnp.concatenate([-heads_f32[..., half_dim:], heads_f32[..., :half_dim]], axis=-1)
    return (heads_f32 * jnp.cos(angles) + rotated * jnp.sin(angles)).astype(jnp.bfloat16)


def draw_weight(key_in, weight_shape, std_dev):
    return (std_dev * jax.random.normal(key_in, weight_shape, jnp.float32)).astype(jnp.bfloat16)


def setup_inputs(seed: int = 0, part: int = 0) -> dict:
    key_list = jax.random.split(jax.random.key(seed), 10)
    qk_std = math.log(SEQ_LEN / 32.0) ** 0.25 / math.sqrt(MODEL_DIM)
    x = 0.5 * jax.random.normal(jax.random.fold_in(key_list[0], part), (1, SEQ_LEN, MODEL_DIM), jnp.float32)
    return {
        'x': x.astype(jnp.bfloat16),
        'g_attn': (0.5 + jax.random.uniform(key_list[1], (MODEL_DIM,), jnp.float32)).astype(jnp.bfloat16),
        'w_q': draw_weight(key_list[2], (MODEL_DIM, N_HEADS, HEAD_DIM), qk_std),
        'w_k': draw_weight(key_list[3], (MODEL_DIM, N_KV_HEADS, HEAD_DIM), qk_std),
        'w_v': draw_weight(key_list[4], (MODEL_DIM, N_KV_HEADS, HEAD_DIM), MODEL_DIM ** -0.5),
        'w_o': draw_weight(key_list[5], (N_HEADS, HEAD_DIM, MODEL_DIM), 2.0 * (N_HEADS * HEAD_DIM) ** -0.5),
        'g_mlp': (0.5 + jax.random.uniform(key_list[6], (MODEL_DIM,), jnp.float32)).astype(jnp.bfloat16),
        'w_gate': draw_weight(key_list[7], (MODEL_DIM, FFN_DIM), MODEL_DIM ** -0.5),
        'w_up': draw_weight(key_list[8], (MODEL_DIM, FFN_DIM), MODEL_DIM ** -0.5),
        'w_down': draw_weight(key_list[9], (FFN_DIM, MODEL_DIM), FFN_DIM ** -0.5),
    }


def reference(x, g_attn, w_q, w_k, w_v, w_o, g_mlp, w_gate, w_up, w_down):
    group_size = N_HEADS // N_KV_HEADS
    n_blocks = SEQ_LEN // Q_BLOCK
    positions = stored_positions(jnp.arange(SEQ_LEN, dtype=jnp.int32))
    x_rows = x[0]
    normed = rms_norm(x_rows, g_attn)
    q_all = jnp.dot(normed, w_q.reshape(MODEL_DIM, N_HEADS * HEAD_DIM), preferred_element_type=jnp.float32).astype(jnp.bfloat16)
    k_all = jnp.dot(normed, w_k.reshape(MODEL_DIM, N_KV_HEADS * HEAD_DIM), preferred_element_type=jnp.float32).astype(jnp.bfloat16)
    v_all = jnp.dot(normed, w_v.reshape(MODEL_DIM, N_KV_HEADS * HEAD_DIM), preferred_element_type=jnp.float32).astype(jnp.bfloat16)
    q_all = apply_rope(q_all.reshape(SEQ_LEN, N_HEADS, HEAD_DIM), positions)
    k_all = apply_rope(k_all.reshape(SEQ_LEN, N_KV_HEADS, HEAD_DIM), positions).astype(jnp.float32)
    v_all = v_all.reshape(SEQ_LEN, N_KV_HEADS, HEAD_DIM).astype(jnp.float32)
    w_o_flat = w_o.reshape(N_HEADS * HEAD_DIM, MODEL_DIM)
    score_scale = HEAD_DIM ** -0.5

    def one_block(block_in):
        q_blk, pos_blk, x_blk = block_in
        q_grp = q_blk.reshape(Q_BLOCK, N_KV_HEADS, group_size, HEAD_DIM).astype(jnp.float32)
        scores = jnp.einsum('qgrd,kgd->gqrk', q_grp, k_all) * score_scale
        visible = pos_blk[None, :, None, None] >= positions[None, None, None, :]
        scores = jnp.where(visible, scores, -1e30)
        weights = jnp.exp(scores - jnp.max(scores, axis=-1, keepdims=True))
        row_sum = jnp.sum(weights, axis=-1, keepdims=True)
        mixed_vals = jnp.einsum('gqrk,kgd->gqrd', weights.astype(jnp.bfloat16).astype(jnp.float32), v_all) / row_sum
        attn_rows = jnp.transpose(mixed_vals, (1, 0, 2, 3)).astype(jnp.bfloat16).reshape(Q_BLOCK, N_HEADS * HEAD_DIM)
        attn_proj = jnp.dot(attn_rows, w_o_flat, preferred_element_type=jnp.float32).astype(jnp.bfloat16)
        resid_rows = (x_blk.astype(jnp.float32) + attn_proj.astype(jnp.float32)).astype(jnp.bfloat16)
        normed_mlp = rms_norm(resid_rows, g_mlp)
        gate_proj = jnp.dot(normed_mlp, w_gate, preferred_element_type=jnp.float32)
        up_proj = jnp.dot(normed_mlp, w_up, preferred_element_type=jnp.float32)
        hidden = (jax.nn.silu(gate_proj) * up_proj).astype(jnp.bfloat16)
        down_proj = jnp.dot(hidden, w_down, preferred_element_type=jnp.float32).astype(jnp.bfloat16)
        return (resid_rows.astype(jnp.float32) + down_proj.astype(jnp.float32)).astype(jnp.bfloat16)

    blocks = lax.map(one_block, (q_all.reshape(n_blocks, Q_BLOCK, N_HEADS, HEAD_DIM),
                                 positions.reshape(n_blocks, Q_BLOCK),
                                 x_rows.reshape(n_blocks, Q_BLOCK, MODEL_DIM)))
    return blocks.reshape(1, SEQ_LEN, MODEL_DIM)
```

```python
import functools
import math
import jax
import jax.numpy as jnp
from jax import lax
from jax.experimental import pallas as pl
from jax.experimental.pallas import tpu as pltpu
from jax.sharding import PartitionSpec as P

NORM_EPS = 1e-5
ROPE_THETA = 500000.0
CP = 16
PIECE = 512
HD = 128


def rms_norm(rows_in, gain_vec):
    rows_f32 = rows_in.astype(jnp.float32)
    mean_sq = jnp.mean(rows_f32 * rows_f32, axis=-1, keepdims=True)
    return (rows_f32 * lax.rsqrt(mean_sq + NORM_EPS) * gain_vec.astype(jnp.float32)).astype(jnp.bfloat16)


def rope_tables(positions):
    inv_freq = ROPE_THETA ** (-2.0 * jnp.arange(HD // 2, dtype=jnp.float32) / HD)
    angles = positions.astype(jnp.float32)[:, None] * inv_freq[None, :]
    c, s = jnp.cos(angles), jnp.sin(angles)
    return jnp.concatenate([c, c], axis=-1), jnp.concatenate([-s, s], axis=-1)


def rope(v, cos, sin):
    f = v.astype(jnp.float32)
    swapped = jnp.concatenate([f[..., HD // 2:], f[..., :HD // 2]], axis=-1)
    return (f * cos + swapped * sin).astype(jnp.bfloat16)


def flash_kernel(n_heads, q_ref, k_ref, v_ref, o_ref, m_ref, l_ref, acc_ref):
    me = lax.axis_index('cp')
    scale = HD ** -0.5 * math.log2(math.e)

    def block(q_row, src, kv_row, masked):
        k = k_ref[src, pl.ds(kv_row, PIECE), :]
        v = v_ref[src, pl.ds(kv_row, PIECE), :]
        for h in range(n_heads):
            cols = slice(h * HD, (h + 1) * HD)
            q = q_ref[q_row:q_row + PIECE, cols]
            s = lax.dot_general(q, k, (((1,), (1,)), ((), ())), preferred_element_type=jnp.float32) * scale
            if masked:
                row = lax.broadcasted_iota(jnp.int32, (PIECE, PIECE), 0)
                col = lax.broadcasted_iota(jnp.int32, (PIECE, PIECE), 1)
                s = jnp.where(row >= col, s, -1e30)
            m_old = m_ref[:, cols]
            m_new = jnp.maximum(m_old, jnp.max(s, axis=1, keepdims=True))
            alpha = jnp.exp2(m_old - m_new)
            p = [jnp.exp2(s[:, i * HD:(i + 1) * HD] - m_new) for i in range(PIECE // HD)]
            psum = p[0]
            for part in p[1:]:
                psum = psum + part
            l_ref[:, cols] = l_ref[:, cols] * alpha + psum
            pb = jnp.concatenate([part.astype(jnp.bfloat16) for part in p], axis=1)
            pv = jnp.dot(pb, v, preferred_element_type=jnp.float32)
            acc_ref[:, cols] = acc_ref[:, cols] * alpha + pv
            m_ref[:, cols] = m_new

    for half in range(2):
        q_row = half * PIECE
        m_ref[...] = jnp.full_like(m_ref, -1e30)
        l_ref[...] = jnp.zeros_like(l_ref)
        acc_ref[...] = jnp.zeros_like(acc_ref)
        n_low = me if half == 0 else CP

        @pl.loop(0, n_low)
        def _(j):
            block(q_row, j, 0, False)

        if half == 1:
            @pl.loop(me + 1, CP)
            def _(j):
                block(q_row, j, PIECE, False)

        block(q_row, me, q_row, True)
        for h in range(n_heads):
            cols = slice(h * HD, (h + 1) * HD)
            total = jnp.sum(l_ref[:, cols], axis=1, keepdims=True)
            o_ref[q_row:q_row + PIECE, cols] = (acc_ref[:, cols] / total).astype(jnp.bfloat16)


def flash(q, k, v):
    rows, width = q.shape
    vmem = pl.BlockSpec(memory_space=pltpu.VMEM)
    return pl.pallas_call(
        functools.partial(flash_kernel, width // HD),
        out_shape=jax.ShapeDtypeStruct((rows, width), jnp.bfloat16),
        in_specs=[vmem] * 3,
        out_specs=vmem,
        scratch_shapes=[pltpu.VMEM((PIECE, width), jnp.float32)] * 3,
        compiler_params=pltpu.CompilerParams(vmem_limit_bytes=50 * 2 ** 20),
        cost_estimate=pl.CostEstimate(flops=18 * 10 ** 9, bytes_accessed=10 * 2 ** 20, transcendentals=35 * 10 ** 6),
    )(q, k, v)


def solution(mesh):
    row_spec = P('dp', ('cp', 'tp'), None)
    head_cols = P(None, 'tp', None)

    def local_layer(x, g_attn, w_q, w_k, w_v, w_o, g_mlp, w_gate, w_up, w_down):
        x_rows = x[0]
        cp_index = lax.axis_index('cp')
        normed = lax.all_gather(rms_norm(x_rows, g_attn), 'tp', axis=0, tiled=True)
        rows = normed.shape[0]
        j = jnp.arange(rows, dtype=jnp.int32)
        positions = jnp.where(j < PIECE, cp_index * PIECE + j, (2 * CP - 1 - cp_index) * PIECE + j - PIECE)
        cos, sin = rope_tables(positions)
        n_heads = w_q.shape[1]
        dim = w_q.shape[0]
        q = jnp.dot(normed, w_q.reshape(dim, n_heads * HD), preferred_element_type=jnp.float32).astype(jnp.bfloat16)
        q = rope(q.reshape(rows, n_heads, HD), cos[:, None], sin[:, None]).reshape(rows, n_heads * HD)
        k = rope(jnp.dot(normed, w_k.reshape(dim, HD), preferred_element_type=jnp.float32).astype(jnp.bfloat16), cos, sin)
        v = jnp.dot(normed, w_v.reshape(dim, HD), preferred_element_type=jnp.float32).astype(jnp.bfloat16)
        k_seq = lax.all_gather(k, 'cp', axis=0, tiled=False)
        v_seq = lax.all_gather(v, 'cp', axis=0, tiled=False)
        attn_out = flash(q, k_seq, v_seq)
        attn_part = jnp.dot(attn_out, w_o.reshape(n_heads * HD, dim), preferred_element_type=jnp.float32).astype(jnp.bfloat16)
        attn_rows = lax.psum_scatter(attn_part, 'tp', scatter_dimension=0, tiled=True)
        resid_rows = (x_rows.astype(jnp.float32) + attn_rows.astype(jnp.float32)).astype(jnp.bfloat16)
        normed_mlp = lax.all_gather(rms_norm(resid_rows, g_mlp), 'tp', axis=0, tiled=True)
        gate_proj = jnp.dot(normed_mlp, w_gate, preferred_element_type=jnp.float32)
        up_proj = jnp.dot(normed_mlp, w_up, preferred_element_type=jnp.float32)
        hidden = (jax.nn.silu(gate_proj) * up_proj).astype(jnp.bfloat16)
        down_part = jnp.dot(hidden, w_down, preferred_element_type=jnp.float32).astype(jnp.bfloat16)
        down_rows = lax.psum_scatter(down_part, 'tp', scatter_dimension=0, tiled=True)
        z_rows = (resid_rows.astype(jnp.float32) + down_rows.astype(jnp.float32)).astype(jnp.bfloat16)
        return z_rows[None]

    return jax.shard_map(local_layer, mesh=mesh,
                         in_specs=(row_spec, P(), head_cols, head_cols, head_cols, P('tp', None, None),
                                   P(), P(None, 'tp'), P(None, 'tp'), P('tp', None)),
                         out_specs=row_spec, check_vma=False)
```

```python
import functools
import math
import jax
import jax.numpy as jnp
from jax import lax
from jax.experimental import pallas as pl
from jax.experimental.pallas import tpu as pltpu
from jax.sharding import PartitionSpec as P

NORM_EPS = 1e-5
ROPE_THETA = 500000.0
HD = 128
NX = 4
MESH = pl.DeviceIdType.MESH
F32 = jnp.float32
BF16 = jnp.bfloat16


def params(cid, vmem_mib):
    return pltpu.CompilerParams(collective_id=cid, has_side_effects=True, vmem_limit_bytes=min(vmem_mib * 2 ** 20, 67043328))


def vmem_spec():
    return pl.BlockSpec(memory_space=pltpu.VMEM)


def any_spec():
    return pl.BlockSpec(memory_space=pl.ANY)


def rope_tables(positions):
    inv_freq = ROPE_THETA ** (-2.0 * jnp.arange(HD // 2, dtype=F32) / HD)
    angles = positions.astype(F32)[:, None] * inv_freq[None, :]
    c, s = jnp.cos(angles), jnp.sin(angles)
    return jnp.concatenate([c, c], axis=-1), jnp.concatenate([-s, s], axis=-1)


def enter(peers):
    barrier = pltpu.get_barrier_semaphore()
    for peer in peers:
        pl.semaphore_signal(barrier, inc=1, device_id=peer, device_id_type=MESH)
    pl.semaphore_wait(barrier, len(peers))


def tp_place():
    t = lax.axis_index('tp')
    x, c = t // 2, t % 2
    side = lambda d: {'tp': ((x + d) % NX) * 2 + c}
    return x, c, {'tp': x * 2 + 1 - c}, side(1), side(NX - 1)


GATHER_PARTS = (((0, 0), (0, 1), (1, 0), (1, 1)), ((2, 0), (3, 0), (4, 1), (5, 1)),
                ((2, 1), (3, 1), (4, 0), (5, 0)), ((6, 0), (6, 1), (7, 0), (7, 1)))
GATHER_PLACE = {name: i for i, name in enumerate(n for part in GATHER_PARTS for n in part)}


def norm_into(x_ref, g_ref, full, rows):
    gain = g_ref[...].astype(F32)
    step = min(16, rows)

    @pl.loop(0, rows // step)
    def _(i):
        where = pl.ds(pl.multiple_of(i * step, step), step)
        r = x_ref[where, :].astype(F32)
        mean_sq = jnp.mean(r * r, axis=-1, keepdims=True)
        full[where, :] = (r * lax.rsqrt(mean_sq + NORM_EPS) * gain).astype(BF16)


def gather_and(full, send_sem, recv_sem, half, before, compute):
    x, c, partner, right, left = tp_place()
    started, landing = [], {}

    def send(src, dst, h, device):
        copy = pltpu.make_async_remote_copy(
            src_ref=full.at[pl.ds(GATHER_PLACE[src, h] * half, half)],
            dst_ref=full.at[pl.ds(GATHER_PLACE[dst, h] * half, half)],
            send_sem=send_sem.at[len(started)], recv_sem=recv_sem.at[GATHER_PLACE[dst, h]],
            device_id=device, device_id_type=MESH)
        copy.start()
        started.append(copy)
        landing[dst, h] = copy

    def arrived(*names):
        for name in names:
            landing[name].wait_recv()

    before()
    enter([partner, right, left])
    send(0, 2, 0, right)
    send(0, 4, 1, left)
    send(0, 1, 0, partner)
    send(0, 1, 1, partner)
    send(0, 2, 1, right)
    send(0, 4, 0, left)
    arrived((1, 0), (1, 1))
    compute(0, 0)
    arrived((2, 0))
    send(2, 6, 0, right)
    send(2, 3, 0, partner)
    arrived((4, 1))
    send(4, 6, 1, left)
    send(4, 5, 1, partner)
    compute(0, 1)
    arrived((3, 0), (5, 1))
    compute(1, 0)
    arrived((2, 1))
    send(2, 3, 1, partner)
    arrived((4, 0))
    send(4, 5, 0, partner)
    compute(1, 1)
    arrived((3, 1), (5, 0))
    compute(2, 0)
    arrived((6, 0))
    send(6, 7, 0, partner)
    arrived((6, 1))
    send(6, 7, 1, partner)
    compute(2, 1)
    arrived((7, 0), (7, 1))
    compute(3, 0)
    compute(3, 1)
    for copy in started:
        copy.wait_send()


def part_rows(part, block):
    t = lax.axis_index('tp')
    x, c = t // 2, t % 2
    rows = []
    for name, h in GATHER_PARTS[part]:
        dx, other = (0, 3, 1, 2)[name // 2], name % 2
        core = 1 - c if other else c
        rows.append((((x + dx) % NX) * 2 + core) * block + h * (block // 2))
    return rows


N_SENDS = 14
GATHER_SEMS = [pltpu.SemaphoreType.DMA((N_SENDS,)), pltpu.SemaphoreType.DMA((16,))]


def qkv_kernel(n_heads, x_ref, g_ref, cos_ref, sin_ref, wq_hbm, wk_hbm, wv_hbm, q_ref, kv_ref, full, w, send_sem, recv_sem, w_sem):
    block = x_ref.shape[0]
    half = block // 2
    piece = kv_ref.shape[2]
    width = n_heads * HD
    loads = [pltpu.make_async_copy(wq_hbm, w.at[:, 0:width], w_sem.at[0]),
             pltpu.make_async_copy(wk_hbm, w.at[:, width:width + HD], w_sem.at[1]),
             pltpu.make_async_copy(wv_hbm, w.at[:, width + HD:width + 2 * HD], w_sem.at[2])]

    def before():
        for load in loads:
            load.start()
        norm_into(x_ref, g_ref, full, block)

    def rotate(v, cos, sin):
        f = v.astype(BF16).astype(F32)
        return (f * cos + pltpu.roll(f, HD // 2, 1) * sin).astype(BF16)

    def compute(part, stage):
        rows = [pl.multiple_of(r, half) for r in part_rows(part, block)]
        a = full[part * 4 * half:(part + 1) * 4 * half, :]
        if stage == 0:
            if part == 0:
                for load in loads:
                    load.wait()
            out = jnp.dot(a, w[:, width:width + 2 * HD], preferred_element_type=F32)
            for i, r in enumerate(rows):
                here = slice(i * half, (i + 1) * half)
                where = pl.ds(pl.multiple_of(r % piece, half), half)
                kv_ref[r // piece, 0, where, :] = rotate(out[here, :HD], cos_ref[pl.ds(r, half), :], sin_ref[pl.ds(r, half), :])
                kv_ref[r // piece, 1, where, :] = out[here, HD:].astype(BF16)
            return
        for pair in range(n_heads // 2):
            out = jnp.dot(a, w[:, pair * 2 * HD:(pair + 1) * 2 * HD], preferred_element_type=F32)
            for i, r in enumerate(rows):
                here = slice(i * half, (i + 1) * half)
                cos, sin = cos_ref[pl.ds(r, half), :], sin_ref[pl.ds(r, half), :]
                for k in range(2):
                    q_ref[pl.ds(r, half), (pair * 2 + k) * HD:(pair * 2 + k + 1) * HD] = rotate(out[here, k * HD:(k + 1) * HD], cos, sin)

    gather_and(full, send_sem, recv_sem, half, before, compute)


def gather_qkv(x_rows, g, cos, sin, w_q, w_k, w_v, n_heads, piece):
    block, dim = x_rows.shape
    rows = 2 * NX * block
    width = n_heads * HD
    return pl.pallas_call(
        functools.partial(qkv_kernel, n_heads),
        out_shape=(jax.ShapeDtypeStruct((rows, width), BF16), jax.ShapeDtypeStruct((2, 2, piece, HD), BF16)),
        in_specs=[vmem_spec()] * 4 + [any_spec()] * 3,
        out_specs=(vmem_spec(), vmem_spec()),
        scratch_shapes=[pltpu.VMEM((rows, dim), BF16), pltpu.VMEM((dim, width + 2 * HD), BF16)] + GATHER_SEMS
        + [pltpu.SemaphoreType.DMA((3,))],
        compiler_params=params(0, 48), name='gather_qkv',
        cost_estimate=pl.CostEstimate(flops=2 * rows * dim * (width + 2 * HD), bytes_accessed=2 * dim * (width + 2 * HD), transcendentals=0),
    )(x_rows, g, cos, sin, w_q, w_k, w_v)


def mlp_in_kernel(x_ref, g_ref, wg_hbm, wu_hbm, h_ref, full, wg, wu, send_sem, recv_sem, w_sem):
    block = x_ref.shape[0]
    half = block // 2
    cols = wg.shape[1]
    step = 256
    n_steps = cols // step
    loads = []
    for n in range(n_steps):
        at = slice(n * step, (n + 1) * step)
        loads.append((pltpu.make_async_copy(wg_hbm.at[:, at], wg.at[:, at], w_sem.at[2 * n]),
                      pltpu.make_async_copy(wu_hbm.at[:, at], wu.at[:, at], w_sem.at[2 * n + 1])))

    def before():
        for pair in loads:
            for load in pair:
                load.start()
        norm_into(x_ref, g_ref, full, block)

    def compute(part, stage):
        rows = [pl.multiple_of(r, half) for r in part_rows(part, block)]

        def tile(n, a):
            at = pl.ds(pl.multiple_of(n * step, step), step)
            gate = jnp.dot(a, wg[:, at], preferred_element_type=F32)
            up = jnp.dot(a, wu[:, at], preferred_element_type=F32)
            out = (jax.nn.silu(gate) * up).astype(BF16)
            for i, r in enumerate(rows):
                h_ref[pl.ds(r, half), at] = out[i * half:(i + 1) * half, :]

        split = (n_steps + 1) // 2
        lo, hi = (0, split) if stage == 0 else (split, n_steps)
        if part == 0:
            for n in range(lo, hi):
                for load in loads[n]:
                    load.wait()

        @pl.loop(lo, hi)
        def _(n):
            tile(n, full[part * 4 * half:(part + 1) * 4 * half, :])

    gather_and(full, send_sem, recv_sem, half, before, compute)


def gather_mlp_in(y_rows, g, w_gate, w_up):
    block, dim = y_rows.shape
    rows = 2 * NX * block
    cols = w_gate.shape[1]
    return pl.pallas_call(
        mlp_in_kernel,
        out_shape=jax.ShapeDtypeStruct((rows, cols), BF16),
        in_specs=[vmem_spec()] * 2 + [any_spec()] * 2,
        out_specs=vmem_spec(),
        scratch_shapes=[pltpu.VMEM((rows, dim), BF16), pltpu.VMEM((dim, cols), BF16), pltpu.VMEM((dim, cols), BF16)] + GATHER_SEMS
        + [pltpu.SemaphoreType.DMA((2 * (cols // 256),))],
        compiler_params=params(1, 64), name='gather_mlp_in',
        cost_estimate=pl.CostEstimate(flops=4 * rows * dim * cols, bytes_accessed=4 * dim * cols, transcendentals=rows * cols),
    )(y_rows, g, w_gate, w_up)


def scatter_kernel(h_ref, w_hbm, res_ref, out_ref, w, give, mine, got, passing, last, w_sem, give_sem, got_sem, send_sem, recv_sem):
    x, c, partner, right, left = tp_place()
    block, dim = res_ref.shape
    half = block // 2
    step = 512
    n_steps = dim // step
    loads = []
    for n in range(n_steps):
        at = slice(n * step, (n + 1) * step)
        loads.append(pltpu.make_async_copy(w_hbm.at[:, at], w.at[:, at], w_sem.at[n]))
        loads[-1].start()
    enter([partner, right, left])
    h0, h1 = slice(0, half), slice(half, block)

    def product(dx, core, dst, wait_w=False):
        start = pl.multiple_of((((x + dx) % NX) * 2 + core) * block, block)
        if wait_w:
            for load in loads:
                load.wait()

        @pl.loop(0, n_steps)
        def _(n):
            at = pl.ds(pl.multiple_of(n * step, step), step)
            dst[:, at] = jnp.dot(h_ref[pl.ds(start, block), :], w[:, at], preferred_element_type=F32).astype(BF16)

    def exchange(b, dx, wait_w=False):
        product(dx, 1 - c, give.at[b], wait_w)
        copy = pltpu.make_async_remote_copy(src_ref=give.at[b], dst_ref=got.at[b], send_sem=give_sem.at[b],
                                            recv_sem=got_sem.at[b], device_id=partner, device_id_type=MESH)
        copy.start()
        product(dx, c, mine.at[b])
        return copy

    def add(dst, a, b, rows):
        step_r = min(16, rows)

        @pl.loop(0, rows // step_r)
        def _(i):
            at = pl.ds(pl.multiple_of(i * step_r, step_r), step_r)
            dst[at, :] = (a[at, :].astype(F32) + b[at, :].astype(F32)).astype(BF16)

    started = []

    def send(src, dst, device):
        n = len(started)
        copy = pltpu.make_async_remote_copy(src_ref=src, dst_ref=dst, send_sem=send_sem.at[n], recv_sem=recv_sem.at[n],
                                            device_id=device, device_id_type=MESH)
        copy.start()
        started.append(copy)
        return copy

    pair = exchange(0, 2, True)
    pair.wait_recv()
    add(mine.at[0], mine.at[0], got.at[0], block)
    pass_right = send(mine.at[0, h0], passing.at[0], right)
    pass_left = send(mine.at[0, h1], passing.at[1], left)
    pair_r = exchange(1, 1)
    pair_l = exchange(2, NX - 1)
    pair_r.wait_recv()
    add(mine.at[1], mine.at[1], got.at[1], block)
    to_right_1 = send(mine.at[1, h1], last.at[0, h1], right)
    pair_l.wait_recv()
    add(mine.at[2], mine.at[2], got.at[2], block)
    to_left_0 = send(mine.at[2, h0], last.at[1, h0], left)
    pair_o = exchange(3, 0)
    pass_right.wait_recv()
    add(mine.at[1, h0], mine.at[1, h0], passing.at[0], half)
    to_right_0 = send(mine.at[1, h0], last.at[0, h0], right)
    pass_left.wait_recv()
    add(mine.at[2, h1], mine.at[2, h1], passing.at[1], half)
    to_left_1 = send(mine.at[2, h1], last.at[1, h1], left)
    pair_o.wait_recv()
    for copy in (to_right_1, to_left_0, to_right_0, to_left_1):
        copy.wait_recv()
    step_r = min(16, block)

    @pl.loop(0, block // step_r)
    def _(i):
        at = pl.ds(pl.multiple_of(i * step_r, step_r), step_r)
        total = (mine[3, at, :].astype(F32) + got[3, at, :].astype(F32)) + (last[0, at, :].astype(F32) + last[1, at, :].astype(F32))
        out_ref[at, :] = (res_ref[at, :].astype(F32) + total.astype(BF16).astype(F32)).astype(BF16)

    for copy in (pair, pair_r, pair_l, pair_o, *started):
        copy.wait_send()


def scatter_product(h, w, res, cid):
    rows, depth = h.shape
    block, dim = res.shape
    half = block // 2
    sem = pltpu.SemaphoreType.DMA
    return pl.pallas_call(
        scatter_kernel,
        out_shape=jax.ShapeDtypeStruct((block, dim), BF16),
        in_specs=[vmem_spec(), any_spec(), vmem_spec()],
        out_specs=vmem_spec(),
        scratch_shapes=[pltpu.VMEM((depth, dim), BF16)] + [pltpu.VMEM((4, block, dim), BF16)] * 3
        + [pltpu.VMEM((2, half, dim), BF16), pltpu.VMEM((2, block, dim), BF16),
           sem((max(1, dim // 512),)), sem((4,)), sem((4,)), sem((6,)), sem((6,))],
        compiler_params=params(cid, 48), name='scatter_product_%d' % cid,
        cost_estimate=pl.CostEstimate(flops=2 * rows * dim * depth, bytes_accessed=2 * dim * depth, transcendentals=0),
    )(h, w, res)


def attention_order():
    seq = [((0, 0), 0)]
    waits = {}

    def then(actions, *units):
        waits.setdefault(len(seq), []).extend(actions)
        seq.extend(units)

    first = lambda *s: [(p, 0) for p in s]
    both = lambda *s: [(p, w) for p in s for w in (0, 1)]
    then(['T1'], *first((1, 0), (3, 0)))
    then(['F0'], *first((0, 1), (0, 3)))
    then(['T2'], *first((2, 0)), ((0, 1), 1), ((0, 3), 1))
    then(['F1'], ((1, 0), 1), ((3, 0), 1))
    then(['F3'], *both((1, 1), (1, 3)))
    then(['F2'], *both((3, 1), (3, 3)))
    then(['E0'], ((2, 0), 1), *both((0, 2)))
    then(['E1', 'E3'], *both((1, 2), (3, 2), (2, 1), (2, 3)))
    then(['E2'], *both((2, 2)))
    return seq, waits


def pick(index, values):
    out = index * 0 + values[0]
    for i, v in enumerate(values[1:], 1):
        if v != values[i - 1]:
            out = jnp.where(index >= i, v, out)
    return out


def attention_kernel(n_heads, q_ref, kv_ref, o_ref, m_ref, l_ref, acc_ref, buf, send_sem, recv_sem):
    piece = kv_ref.shape[2]
    me = lax.axis_index('cp')
    y, z = me % NX, me // NX
    scale = HD ** -0.5 * math.log2(math.e)
    at_y = lambda d: {'cp': z * NX + (y + d) % NX}
    at_z = lambda d: {'cp': ((z + d) % NX) * NX + y}
    enter([at_y(1), at_y(3), at_z(1), at_z(3)])
    axes = ((at_y, at_z), (at_z, at_y))

    def slot(kind, da, db):
        dy, dz = (da, db) if kind == 0 else (db, da)
        return dz * NX + dy

    started, landing = [], {}

    def copy_of(kind, src, dst, axis, d, part, n):
        source = kv_ref.at[kind] if src == (0, 0) else buf.at[kind, slot(kind, *src)]
        target = buf.at[kind, slot(kind, *dst)]
        if part is not None:
            source, target = source.at[part], target.at[part]
        return pltpu.make_async_remote_copy(
            src_ref=source, dst_ref=target, send_sem=send_sem.at[n],
            recv_sem=recv_sem.at[kind, slot(kind, *dst), part or 0],
            device_id=axes[kind][axis](d), device_id_type=MESH)

    def send(kind, src, dst, axis, d, part=None):
        key = (kind, src, dst, axis, d, part, len(started))
        copy_of(*key).start()
        started.append(key)
        landing[kind, dst, part] = key

    def landed(*key):
        copy_of(*landing[key]).wait_recv()

    def arrived(kind, *names):
        for name in names:
            for part in ((0, 1) if 2 in name else (None,)):
                landed(kind, name, part)

    def along_b(kind, da):
        send(kind, (da, 0), (da, 3), 1, 1)
        send(kind, (da, 0), (da, 1), 1, 3)

    def act(name):
        step, da = name[0], int(name[1])
        for kind in range(2):
            if name == 'T1':
                arrived(kind, (1, 0), (3, 0))
                send(kind, (3, 0), (2, 0), 0, 1, 0)
                send(kind, (1, 0), (2, 0), 0, 3, 1)
                along_b(kind, 1)
                along_b(kind, 3)
            elif name == 'T2':
                arrived(kind, (2, 0))
                along_b(kind, 2)
            elif step == 'F':
                for db, d, part in ((3, 1, 0), (1, 3, 1)):
                    if da == 2:
                        landed(kind, (2, db), None)
                    else:
                        arrived(kind, (da, db))
                    send(kind, (da, db), (da, 2), 1, d, part)
            else:
                for part in (0, 1):
                    landed(kind, (da, 2), part)

    kinds = (0, 1)
    for kind in kinds:
        send(kind, (0, 0), (3, 0), 0, 1)
        send(kind, (0, 0), (1, 0), 0, 3)
    for kind in kinds:
        along_b(kind, 0)

    m_ref[...] = jnp.full_like(m_ref, -1e30)
    l_ref[...] = jnp.zeros_like(l_ref)
    acc_ref[...] = jnp.zeros_like(acc_ref)

    def unit(q_row, k, v, masked):
        rows = pl.ds(pl.multiple_of(q_row, piece), piece)
        for h in range(n_heads):
            cols = slice(h * HD, (h + 1) * HD)
            s = lax.dot_general(q_ref[rows, cols], k, (((1,), (1,)), ((), ())), preferred_element_type=F32) * scale
            if masked:
                row = lax.broadcasted_iota(jnp.int32, (piece, piece), 0)
                col = lax.broadcasted_iota(jnp.int32, (piece, piece), 1)
                s = jnp.where(row >= col, s, -1e30)
            m_old = m_ref[rows, cols]
            m_new = jnp.maximum(m_old, jnp.max(s, axis=1, keepdims=True))
            alpha = jnp.exp2(m_old - m_new)
            p = [jnp.exp2(s[:, i * HD:(i + 1) * HD] - m_new) for i in range(piece // HD)]
            psum = p[0]
            for part in p[1:]:
                psum = psum + part
            l_ref[rows, cols] = l_ref[rows, cols] * alpha + psum
            pb = jnp.concatenate([part.astype(BF16) for part in p], axis=1)
            pv = jnp.dot(pb, v, preferred_element_type=F32)
            acc_ref[rows, cols] = acc_ref[rows, cols] * alpha + pv
            m_ref[rows, cols] = m_new

    @pl.loop(0, 2)
    def _(kind):
        unit(kind * piece, kv_ref[kind, 0], kv_ref[kind, 1], True)

    unit(piece, kv_ref[0, 0], kv_ref[0, 1], False)
    seq, waits = attention_order()
    marks = sorted(waits) + [len(seq)]

    @pl.loop(1, len(seq))
    def _(u):
        for mark in marks[:-1]:
            @pl.when(u == mark)
            def _():
                for name in waits[mark]:
                    act(name)

        dy = pick(u, [p[0] for p, _ in seq])
        dz = pick(u, [p[1] for p, _ in seq])
        which = pick(u, [w for _, w in seq])
        src = ((z + dz) % NX) * NX + (y + dy) % NX
        late = jnp.where(src > me, 1, 0)
        q_row = jnp.where(which == 0, 1, late) * piece
        kind = which * late
        at = dz * NX + dy
        unit(q_row, buf[kind, at, 0], buf[kind, at, 1], False)

    @pl.loop(0, 2)
    def _(part):
        rows = pl.ds(pl.multiple_of(part * piece, piece), piece)
        for h in range(n_heads):
            cols = slice(h * HD, (h + 1) * HD)
            total = jnp.sum(l_ref[rows, cols], axis=1, keepdims=True)
            o_ref[rows, cols] = (acc_ref[rows, cols] / total).astype(BF16)

    for key in started:
        copy_of(*key).wait_send()


def attention(q, kv):
    rows, width = q.shape
    piece = kv.shape[2]
    sem = pltpu.SemaphoreType.DMA
    return pl.pallas_call(
        functools.partial(attention_kernel, width // HD),
        out_shape=jax.ShapeDtypeStruct((rows, width), BF16),
        in_specs=[vmem_spec()] * 2,
        out_specs=vmem_spec(),
        scratch_shapes=[pltpu.VMEM((rows, width), F32)] * 3 + [pltpu.VMEM((2, NX * NX, 2, piece, HD), BF16),
                                                              sem((40,)), sem((2, NX * NX, 2))],
        compiler_params=params(2, 48), name='attention',
        cost_estimate=pl.CostEstimate(flops=18 * 10 ** 9, bytes_accessed=10 * 2 ** 20, transcendentals=35 * 10 ** 6),
    )(q, kv)


def solution(mesh):
    row_spec = P('dp', ('cp', 'tp'), None)
    head_cols = P(None, 'tp', None)
    cp_size = mesh.shape['cp']

    def local_layer(x, g_attn, w_q, w_k, w_v, w_o, g_mlp, w_gate, w_up, w_down):
        x_rows = x[0]
        block, dim = x_rows.shape
        rows = block * mesh.shape['tp']
        piece = rows // 2
        cp_index = lax.axis_index('cp')
        n_heads = w_q.shape[1]
        j = jnp.arange(rows, dtype=jnp.int32)
        positions = jnp.where(j < piece, cp_index * piece + j, (2 * cp_size - 1 - cp_index) * piece + j - piece)
        cos, sin = rope_tables(positions)
        q, kv = gather_qkv(x_rows, g_attn.reshape(1, dim), cos, sin, w_q.reshape(dim, n_heads * HD),
                           w_k.reshape(dim, HD), w_v.reshape(dim, HD), n_heads, piece)
        o = attention(q, kv)
        y_rows = scatter_product(o, w_o.reshape(n_heads * HD, dim), x_rows, 3)
        hidden = gather_mlp_in(y_rows, g_mlp.reshape(1, dim), w_gate, w_up)
        z_rows = scatter_product(hidden, w_down, y_rows, 4)
        return z_rows[None]

    return jax.shard_map(local_layer, mesh=mesh,
                         in_specs=(row_spec, P(), head_cols, head_cols, head_cols, P('tp', None, None),
                                   P(), P(None, 'tp'), P(None, 'tp'), P('tp', None)),
                         out_specs=row_spec, check_vma=False)
```

```python
import functools
import math
import jax
import jax.numpy as jnp
from jax import lax
from jax.experimental import pallas as pl
from jax.experimental.pallas import tpu as pltpu
from jax.sharding import PartitionSpec as P

NORM_EPS = 1e-5
ROPE_THETA = 500000.0
HD = 128
NX = 4
MESH = pl.DeviceIdType.MESH
F32 = jnp.float32
BF16 = jnp.bfloat16


def params(cid, vmem_mib):
    return pltpu.CompilerParams(collective_id=cid, has_side_effects=True, vmem_limit_bytes=min(vmem_mib * 2 ** 20, 67043328))


def vmem_spec():
    return pl.BlockSpec(memory_space=pltpu.VMEM)


def any_spec():
    return pl.BlockSpec(memory_space=pl.ANY)


def rope_tables(positions):
    inv_freq = ROPE_THETA ** (-2.0 * jnp.arange(HD // 2, dtype=F32) / HD)
    angles = positions.astype(F32)[:, None] * inv_freq[None, :]
    c, s = jnp.cos(angles), jnp.sin(angles)
    return jnp.concatenate([c, c], axis=-1), jnp.concatenate([-s, s], axis=-1)


def enter(peers):
    barrier = pltpu.get_barrier_semaphore()
    for peer in peers:
        pl.semaphore_signal(barrier, inc=1, device_id=peer, device_id_type=MESH)
    pl.semaphore_wait(barrier, len(peers))


def tp_place():
    t = lax.axis_index('tp')
    x, c = t // 2, t % 2
    side = lambda d: {'tp': ((x + d) % NX) * 2 + c}
    return x, c, {'tp': x * 2 + 1 - c}, side(1), side(NX - 1)


OWN, MATE, LEFT, LEFT_MATE, RIGHT, RIGHT_MATE, FAR, FAR_MATE = range(8)
LO, HI = range(2)
NEAR_PART, FIRST_PART, LAST_PART, FAR_PART = range(4)
GATHER_PARTS = (((OWN, LO), (OWN, HI), (MATE, LO), (MATE, HI)),
                ((LEFT, LO), (RIGHT, HI), (LEFT_MATE, LO), (RIGHT_MATE, HI)),
                ((LEFT, HI), (RIGHT, LO), (LEFT_MATE, HI), (RIGHT_MATE, LO)),
                ((FAR, LO), (FAR, HI), (FAR_MATE, LO), (FAR_MATE, HI)))
GATHER_PLACE = {name: i for i, name in enumerate(n for part in GATHER_PARTS for n in part)}
N_PLACES = len(GATHER_PLACE)


def norm_into(x_ref, g_ref, full, rows):
    gain = g_ref[...].astype(F32)
    step = min(16, rows)

    @pl.loop(0, rows // step)
    def _(i):
        where = pl.ds(pl.multiple_of(i * step, step), step)
        r = x_ref[where, :].astype(F32)
        mean_sq = jnp.mean(r * r, axis=-1, keepdims=True)
        full[where, :] = (r * lax.rsqrt(mean_sq + NORM_EPS) * gain).astype(BF16)


class Gather:
    def __init__(self, full, send_sem, recv_sem, half):
        self.full, self.send_sem, self.recv_sem, self.half = full, send_sem, recv_sem, half
        _, _, self.mate, self.right, self.left = tp_place()
        self.started, self.landing = [], {}

    def enter(self):
        enter([self.mate, self.right, self.left])

    def send(self, src, dst, h, device):
        rows = [pl.ds(GATHER_PLACE[slot, h] * self.half, self.half) for slot in (src, dst)]
        copy = pltpu.make_async_remote_copy(
            src_ref=self.full.at[rows[0]], dst_ref=self.full.at[rows[1]],
            send_sem=self.send_sem.at[len(self.started)], recv_sem=self.recv_sem.at[GATHER_PLACE[dst, h]],
            device_id=device, device_id_type=MESH)
        copy.start()
        self.started.append(copy)
        self.landing[dst, h] = copy

    def arrived(self, *names):
        for name in names:
            self.landing[name].wait_recv()

    def start(self):
        self.send(OWN, LEFT, LO, self.right)
        self.send(OWN, RIGHT, HI, self.left)
        for h in (LO, HI):
            self.send(OWN, MATE, h, self.mate)

    def relay(self):
        self.arrived((LEFT, LO))
        self.send(LEFT, FAR, LO, self.right)
        self.send(OWN, LEFT, HI, self.right)
        self.arrived((RIGHT, HI))
        self.send(RIGHT, FAR, HI, self.left)
        self.send(OWN, RIGHT, LO, self.left)
        self.send(LEFT, LEFT_MATE, LO, self.mate)
        self.send(RIGHT, RIGHT_MATE, HI, self.mate)

    def share_far(self):
        for h in (LO, HI):
            self.arrived((FAR, h))
            self.send(FAR, FAR_MATE, h, self.mate)

    def share_last(self):
        self.arrived((LEFT, HI))
        self.send(LEFT, LEFT_MATE, HI, self.mate)
        self.arrived((RIGHT, LO))
        self.send(RIGHT, RIGHT_MATE, LO, self.mate)

    def sent(self, *which):
        for copy in self.started:
            copy.wait_send()


def part_rows(part, block):
    t = lax.axis_index('tp')
    x, c = t // 2, t % 2
    rows = []
    for name, h in GATHER_PARTS[part]:
        dx, other = {OWN: 0, LEFT: NX - 1, RIGHT: 1, FAR: 2}[name // 2 * 2], name % 2
        core = 1 - c if other else c
        rows.append((((x + dx) % NX) * 2 + core) * block + h * (block // 2))
    return rows


N_SENDS = 14
GATHER_SEMS = [pltpu.SemaphoreType.DMA((N_SENDS,)), pltpu.SemaphoreType.DMA((N_PLACES,))]


def qkv_kernel(n_heads, x_ref, g_ref, cos_ref, sin_ref, wq_hbm, wk_hbm, wv_hbm, q_ref, kv_ref, full, w, send_sem, recv_sem, w_sem):
    block = x_ref.shape[0]
    half = block // 2
    piece = kv_ref.shape[2]
    width = n_heads * HD
    loads = [pltpu.make_async_copy(wq_hbm, w.at[:, 0:width], w_sem.at[0]),
             pltpu.make_async_copy(wk_hbm, w.at[:, width:width + HD], w_sem.at[1]),
             pltpu.make_async_copy(wv_hbm, w.at[:, width + HD:width + 2 * HD], w_sem.at[2])]

    def rotate(v, cos, sin):
        f = v.astype(BF16).astype(F32)
        return (f * cos + pltpu.roll(f, HD // 2, 1) * sin).astype(BF16)

    def keys_values(part, rows, a):
        out = jnp.dot(a, w[:, width:], preferred_element_type=F32)
        for i, r in enumerate(rows):
            here = slice(i * half, (i + 1) * half)
            where = pl.ds(pl.multiple_of(r % piece, half), half)
            kv_ref[r // piece, 0, where, :] = rotate(out[here, :HD], cos_ref[pl.ds(r, half), :], sin_ref[pl.ds(r, half), :])
            kv_ref[r // piece, 1, where, :] = out[here, HD:].astype(BF16)

    def queries(part, rows, a):
        for start in range(0, width, 2 * HD):
            out = jnp.dot(a, w[:, start:start + 2 * HD], preferred_element_type=F32)
            for i, r in enumerate(rows):
                here = slice(i * half, (i + 1) * half)
                cos, sin = cos_ref[pl.ds(r, half), :], sin_ref[pl.ds(r, half), :]
                for k in (0, HD):
                    q_ref[pl.ds(r, half), start + k:start + k + HD] = rotate(out[here, k:k + HD], cos, sin)

    def compute(part):
        rows = [pl.multiple_of(r, half) for r in part_rows(part, block)]
        n = len(rows) * half
        a = full[part * n:(part + 1) * n, :]
        keys_values(part, rows, a)
        queries(part, rows, a)

    gather = Gather(full, send_sem, recv_sem, half)
    for load in loads:
        load.start()
    norm_into(x_ref, g_ref, full, block)
    gather.enter()
    gather.start()
    gather.arrived((MATE, LO), (MATE, HI))
    for load in loads:
        load.wait()
    compute(NEAR_PART)
    gather.relay()
    gather.arrived((LEFT_MATE, LO), (RIGHT_MATE, HI))
    compute(FIRST_PART)
    gather.share_far()
    gather.arrived((FAR_MATE, LO), (FAR_MATE, HI))
    compute(FAR_PART)
    gather.share_last()
    gather.arrived((LEFT_MATE, HI), (RIGHT_MATE, LO))
    compute(LAST_PART)
    gather.sent()


def gather_qkv(x_rows, g, cos, sin, w_q, w_k, w_v, n_heads, piece):
    block, dim = x_rows.shape
    rows = 2 * NX * block
    width = n_heads * HD
    return pl.pallas_call(
        functools.partial(qkv_kernel, n_heads),
        out_shape=(jax.ShapeDtypeStruct((rows, width), BF16), jax.ShapeDtypeStruct((2, 2, piece, HD), BF16)),
        in_specs=[vmem_spec()] * 4 + [any_spec()] * 3,
        out_specs=(vmem_spec(), vmem_spec()),
        scratch_shapes=[pltpu.VMEM((rows, dim), BF16), pltpu.VMEM((dim, width + 2 * HD), BF16)] + GATHER_SEMS
        + [pltpu.SemaphoreType.DMA((3,))],
        compiler_params=params(0, 48), name='gather_qkv',
        cost_estimate=pl.CostEstimate(flops=2 * rows * dim * (width + 2 * HD), bytes_accessed=2 * dim * (width + 2 * HD), transcendentals=0),
    )(x_rows, g, cos, sin, w_q, w_k, w_v)


def add_rows(dst, a, b):
    step = min(16, dst.shape[0])

    @pl.loop(0, dst.shape[0] // step)
    def _(i):
        at = pl.ds(pl.multiple_of(i * step, step), step)
        dst[at, :] = (a[at, :].astype(F32) + b[at, :].astype(F32)).astype(BF16)


def finish_rows(out, res, parts):
    step = min(16, out.shape[0])

    @pl.loop(0, out.shape[0] // step)
    def _(i):
        at = pl.ds(pl.multiple_of(i * step, step), step)
        total = parts[0][at, :].astype(F32)
        for part in parts[1:]:
            total = total + part[at, :].astype(F32)
        out[at, :] = (res[at, :].astype(F32) + total.astype(BF16).astype(F32)).astype(BF16)


def mlp_kernel(y_hbm, g_ref, wg_hbm, wu_hbm, wd_hbm, z_hbm, full, wg, wu, wd, hid, give, got, passing, last,
               send_sem, recv_sem, w_sem, d_sem, mate_sems, row_sems, io_sem):
    block, dim = y_hbm.shape
    half = block // 2
    cols = wg.shape[1]
    step = 256
    n_steps = cols // step
    loads = []
    for n in range(n_steps):
        at = slice(n * step, (n + 1) * step)
        loads.append((pltpu.make_async_copy(wg_hbm.at[:, at], wg.at[:, at], w_sem.at[0, n]),
                      pltpu.make_async_copy(wu_hbm.at[:, at], wu.at[:, at], w_sem.at[1, n])))
    load_d = pltpu.make_async_copy(wd_hbm, wd, d_sem)
    gather = Gather(full, send_sem, recv_sem, half)
    n_rows = 2 * block
    head, tail = slice(0, half), slice(half, block)

    def gate_up(part, lo, hi):
        @pl.loop(lo, hi)
        def _(n):
            at = pl.ds(pl.multiple_of(n * step, step), step)
            a = full[part * n_rows:(part + 1) * n_rows, :]
            gate = jnp.dot(a, wg[:, at], preferred_element_type=F32)
            up = jnp.dot(a, wu[:, at], preferred_element_type=F32)
            hid[part, :, at] = (jax.nn.silu(gate) * up).astype(BF16)

    def down(part, mine, dst):
        wide = min(512, dim)

        @pl.loop(0, dim // wide)
        def _(n):
            at = pl.ds(pl.multiple_of(n * wide, wide), wide)
            a = hid[part, 0:block, :] if mine else hid[part, block:n_rows, :]
            dst[:, at] = jnp.dot(a, wd[:, at], preferred_element_type=F32).astype(BF16)

    kept = {FAR_PART: full.at[block:n_rows], FIRST_PART: full.at[2 * n_rows - block:2 * n_rows],
            LAST_PART: full.at[n_rows:n_rows + block], NEAR_PART: full.at[0:block]}
    traded, moved = {}, []

    def trade(part, buffer):
        down(part, False, give.at[buffer])
        traded[part] = pltpu.make_async_remote_copy(
            src_ref=give.at[buffer], dst_ref=got.at[part], send_sem=mate_sems.at[0, part], recv_sem=mate_sems.at[1, part],
            device_id=gather.mate, device_id_type=MESH)
        traded[part].start()

    def join(part):
        traded[part].wait_recv()
        add_rows(kept[part], kept[part], got.at[part])

    def move(src, dst, device):
        copy = pltpu.make_async_remote_copy(src_ref=src, dst_ref=dst, send_sem=row_sems.at[0, len(moved)],
                                            recv_sem=row_sems.at[1, len(moved)], device_id=device, device_id_type=MESH)
        copy.start()
        moved.append(copy)
        return copy

    fetch = pltpu.make_async_copy(y_hbm, give.at[0], io_sem)
    fetch.start()
    for pair in loads:
        for load in pair:
            load.start()
    load_d.start()
    fetch.wait()
    norm_into(give.at[0], g_ref, full, block)
    gather.enter()
    gather.start()
    gather.arrived((MATE, LO), (MATE, HI))
    split = (n_steps + 1) // 2
    for lo, hi in ((0, split), (split, n_steps)):
        for pair in loads[lo:hi]:
            for load in pair:
                load.wait()
        gate_up(NEAR_PART, lo, hi)
        if lo == 0:
            gather.relay()
    gather.arrived((LEFT_MATE, LO), (RIGHT_MATE, HI))
    gate_up(FIRST_PART, 0, n_steps - 1)
    gather.share_far()
    gate_up(FIRST_PART, n_steps - 1, n_steps)
    gather.arrived((FAR_MATE, LO), (FAR_MATE, HI))
    gate_up(FAR_PART, 0, n_steps)
    load_d.wait()
    trade(FAR_PART, 0)
    down(FAR_PART, True, kept[FAR_PART])
    gather.share_last()
    join(FAR_PART)
    pass_right = move(kept[FAR_PART].at[head], passing.at[0], gather.right)
    pass_left = move(kept[FAR_PART].at[tail], passing.at[1], gather.left)
    gather.arrived((LEFT_MATE, HI), (RIGHT_MATE, LO))
    gather.sent()
    trade(FIRST_PART, 1)
    down(FIRST_PART, True, kept[FIRST_PART])
    gate_up(LAST_PART, 0, split)
    join(FIRST_PART)
    moved_first = [move(kept[FIRST_PART].at[head], last.at[1, head], gather.left),
                   move(kept[FIRST_PART].at[tail], last.at[0, tail], gather.right)]
    gate_up(LAST_PART, split, n_steps)
    traded[FAR_PART].wait_send()
    trade(LAST_PART, 0)
    down(LAST_PART, True, kept[LAST_PART])
    traded[FIRST_PART].wait_send()
    trade(NEAR_PART, 1)
    join(LAST_PART)
    pass_left.wait_recv()
    add_rows(kept[LAST_PART].at[head], kept[LAST_PART].at[head], passing.at[1])
    pass_right.wait_recv()
    add_rows(kept[LAST_PART].at[tail], kept[LAST_PART].at[tail], passing.at[0])
    moved_last = [move(kept[LAST_PART].at[head], last.at[1, tail], gather.left),
                  move(kept[LAST_PART].at[tail], last.at[0, head], gather.right)]
    down(NEAR_PART, True, kept[NEAR_PART])
    traded[LAST_PART].wait_send()
    fetch.start()
    traded[NEAR_PART].wait_recv()
    fetch.wait()
    for copy in moved_first + moved_last:
        copy.wait_recv()
    done = full.at[3 * n_rows:3 * n_rows + block]
    finish_rows(done, give.at[0], [kept[NEAR_PART], got.at[NEAR_PART], last.at[0], last.at[1]])
    put = pltpu.make_async_copy(done, z_hbm, io_sem)
    put.start()
    traded[NEAR_PART].wait_send()
    for copy in moved:
        copy.wait_send()
    put.wait()


def mlp(y_rows, g, w_gate, w_up, w_down):
    block, dim = y_rows.shape
    rows = 2 * NX * block
    cols = w_gate.shape[1]
    sem = pltpu.SemaphoreType.DMA
    buffer = lambda *shape: pltpu.VMEM(shape, BF16)
    return pl.pallas_call(
        mlp_kernel,
        out_shape=jax.ShapeDtypeStruct((block, dim), BF16),
        in_specs=[any_spec(), vmem_spec()] + [any_spec()] * 3,
        out_specs=any_spec(),
        scratch_shapes=[buffer(rows, dim), buffer(dim, cols), buffer(dim, cols), buffer(cols, dim), buffer(NX, 2 * block, cols),
                        buffer(2, block, dim), buffer(NX, block, dim), buffer(2, block // 2, dim), buffer(2, block, dim)]
        + GATHER_SEMS + [sem((2, cols // 256)), sem, sem((2, NX)), sem((2, 6)), sem],
        compiler_params=params(1, 64), name='mlp',
        cost_estimate=pl.CostEstimate(flops=6 * rows * dim * cols, bytes_accessed=6 * dim * cols, transcendentals=rows * cols),
    )(y_rows, g, w_gate, w_up, w_down)


def scatter_kernel(h_ref, w_hbm, res_ref, out_ref, w, give, mine, got, passing, last, w_sem, give_sem, got_sem, send_sem, recv_sem):
    x, c, partner, right, left = tp_place()
    block, dim = res_ref.shape
    half = block // 2
    step = 512
    n_steps = dim // step
    loads = []
    for n in range(n_steps):
        at = slice(n * step, (n + 1) * step)
        loads.append(pltpu.make_async_copy(w_hbm.at[:, at], w.at[:, at], w_sem.at[n]))
        loads[-1].start()
    enter([partner, right, left])
    h0, h1 = slice(0, half), slice(half, block)

    def product(dx, core, dst, wait_w=False):
        start = pl.multiple_of((((x + dx) % NX) * 2 + core) * block, block)
        if wait_w:
            for load in loads:
                load.wait()

        @pl.loop(0, n_steps)
        def _(n):
            at = pl.ds(pl.multiple_of(n * step, step), step)
            dst[:, at] = jnp.dot(h_ref[pl.ds(start, block), :], w[:, at], preferred_element_type=F32).astype(BF16)

    def exchange(b, dx, wait_w=False):
        product(dx, 1 - c, give.at[b], wait_w)
        copy = pltpu.make_async_remote_copy(src_ref=give.at[b], dst_ref=got.at[b], send_sem=give_sem.at[b],
                                            recv_sem=got_sem.at[b], device_id=partner, device_id_type=MESH)
        copy.start()
        product(dx, c, mine.at[b])
        return copy

    started = []

    def send(src, dst, device):
        n = len(started)
        copy = pltpu.make_async_remote_copy(src_ref=src, dst_ref=dst, send_sem=send_sem.at[n], recv_sem=recv_sem.at[n],
                                            device_id=device, device_id_type=MESH)
        copy.start()
        started.append(copy)
        return copy

    pair = exchange(0, 2, True)
    pair.wait_recv()
    add_rows(mine.at[0], mine.at[0], got.at[0])
    pass_right = send(mine.at[0, h0], passing.at[0], right)
    pass_left = send(mine.at[0, h1], passing.at[1], left)
    pair_r = exchange(1, 1)
    pair_l = exchange(2, NX - 1)
    pair_r.wait_recv()
    add_rows(mine.at[1], mine.at[1], got.at[1])
    to_right_1 = send(mine.at[1, h1], last.at[0, h1], right)
    pair_l.wait_recv()
    add_rows(mine.at[2], mine.at[2], got.at[2])
    to_left_0 = send(mine.at[2, h0], last.at[1, h0], left)
    pair_o = exchange(3, 0)
    pass_right.wait_recv()
    add_rows(mine.at[1, h0], mine.at[1, h0], passing.at[0])
    to_right_0 = send(mine.at[1, h0], last.at[0, h0], right)
    pass_left.wait_recv()
    add_rows(mine.at[2, h1], mine.at[2, h1], passing.at[1])
    to_left_1 = send(mine.at[2, h1], last.at[1, h1], left)
    pair_o.wait_recv()
    for copy in (to_right_1, to_left_0, to_right_0, to_left_1):
        copy.wait_recv()
    finish_rows(out_ref, res_ref, [mine.at[3], got.at[3], last.at[0], last.at[1]])
    for copy in (pair, pair_r, pair_l, pair_o, *started):
        copy.wait_send()


def scatter_product(h, w, res, cid):
    rows, depth = h.shape
    block, dim = res.shape
    half = block // 2
    sem = pltpu.SemaphoreType.DMA
    return pl.pallas_call(
        scatter_kernel,
        out_shape=jax.ShapeDtypeStruct((block, dim), BF16),
        in_specs=[vmem_spec(), any_spec(), vmem_spec()],
        out_specs=vmem_spec(),
        scratch_shapes=[pltpu.VMEM((depth, dim), BF16)] + [pltpu.VMEM((4, block, dim), BF16)] * 3
        + [pltpu.VMEM((2, half, dim), BF16), pltpu.VMEM((2, block, dim), BF16),
           sem((max(1, dim // 512),)), sem((4,)), sem((4,)), sem((6,)), sem((6,))],
        compiler_params=params(cid, 48), name='scatter_product_%d' % cid,
        cost_estimate=pl.CostEstimate(flops=2 * rows * dim * depth, bytes_accessed=2 * dim * depth, transcendentals=0),
    )(h, w, res)


def attention_order():
    seq = [((0, 0), 0)]
    waits = {}

    def then(actions, *units):
        waits.setdefault(len(seq), []).extend(actions)
        seq.extend(units)

    first = lambda *s: [(p, 0) for p in s]
    both = lambda *s: [(p, w) for p in s for w in (0, 1)]
    then(['T1'], *first((1, 0), (3, 0)))
    then(['F0'], *first((0, 1), (0, 3)))
    then(['T2'], *first((2, 0)), ((0, 1), 1), ((0, 3), 1))
    then(['F1'], ((1, 0), 1), ((3, 0), 1))
    then(['F3'], *both((1, 1), (1, 3)))
    then(['F2'], *both((3, 1), (3, 3)))
    then(['E0'], ((2, 0), 1), *both((0, 2)))
    then(['E1', 'E3'], *both((1, 2), (3, 2), (2, 1), (2, 3)))
    then(['E2'], *both((2, 2)))
    return seq, waits


def pick(index, values):
    out = index * 0 + values[0]
    for i, v in enumerate(values[1:], 1):
        if v != values[i - 1]:
            out = jnp.where(index >= i, v, out)
    return out


def attention_kernel(n_heads, q_ref, kv_ref, o_ref, m_ref, l_ref, acc_ref, buf, send_sem, recv_sem):
    piece = kv_ref.shape[2]
    me = lax.axis_index('cp')
    y, z = me % NX, me // NX
    scale = HD ** -0.5 * math.log2(math.e)
    at_y = lambda d: {'cp': z * NX + (y + d) % NX}
    at_z = lambda d: {'cp': ((z + d) % NX) * NX + y}
    enter([at_y(1), at_y(3), at_z(1), at_z(3)])
    axes = ((at_y, at_z), (at_z, at_y))

    def slot(kind, da, db):
        dy, dz = (da, db) if kind == 0 else (db, da)
        return dz * NX + dy

    started, landing = [], {}

    def copy_of(kind, src, dst, axis, d, part, n):
        source = kv_ref.at[kind] if src == (0, 0) else buf.at[kind, slot(kind, *src)]
        target = buf.at[kind, slot(kind, *dst)]
        if part is not None:
            source, target = source.at[part], target.at[part]
        return pltpu.make_async_remote_copy(
            src_ref=source, dst_ref=target, send_sem=send_sem.at[n],
            recv_sem=recv_sem.at[kind, slot(kind, *dst), part or 0],
            device_id=axes[kind][axis](d), device_id_type=MESH)

    def send(kind, src, dst, axis, d, part=None):
        key = (kind, src, dst, axis, d, part, len(started))
        copy_of(*key).start()
        started.append(key)
        landing[kind, dst, part] = key

    def landed(*key):
        copy_of(*landing[key]).wait_recv()

    def arrived(kind, *names):
        for name in names:
            for part in ((0, 1) if 2 in name else (None,)):
                landed(kind, name, part)

    def along_b(kind, da):
        send(kind, (da, 0), (da, 3), 1, 1)
        send(kind, (da, 0), (da, 1), 1, 3)

    def act(name):
        step, da = name[0], int(name[1])
        for kind in range(2):
            if name == 'T1':
                arrived(kind, (1, 0), (3, 0))
                send(kind, (3, 0), (2, 0), 0, 1, 0)
                send(kind, (1, 0), (2, 0), 0, 3, 1)
                along_b(kind, 1)
                along_b(kind, 3)
            elif name == 'T2':
                arrived(kind, (2, 0))
                along_b(kind, 2)
            elif step == 'F':
                for db, d, part in ((3, 1, 0), (1, 3, 1)):
                    if da == 2:
                        landed(kind, (2, db), None)
                    else:
                        arrived(kind, (da, db))
                    send(kind, (da, db), (da, 2), 1, d, part)
            else:
                for part in (0, 1):
                    landed(kind, (da, 2), part)

    kinds = (0, 1)
    for kind in kinds:
        send(kind, (0, 0), (3, 0), 0, 1)
        send(kind, (0, 0), (1, 0), 0, 3)
    for kind in kinds:
        along_b(kind, 0)

    m_ref[...] = jnp.full_like(m_ref, -1e30)
    l_ref[...] = jnp.zeros_like(l_ref)
    acc_ref[...] = jnp.zeros_like(acc_ref)

    def unit(q_row, k, v, masked):
        rows = pl.ds(pl.multiple_of(q_row, piece), piece)
        heads = [slice(h * HD, (h + 1) * HD) for h in range(n_heads)]

        def score(cols):
            s = lax.dot_general(q_ref[rows, cols], k, (((1,), (1,)), ((), ())), preferred_element_type=F32) * scale
            if masked:
                row = lax.broadcasted_iota(jnp.int32, (piece, piece), 0)
                col = lax.broadcasted_iota(jnp.int32, (piece, piece), 1)
                s = jnp.where(row >= col, s, -1e30)
            return s

        def absorb(cols, s):
            m_old = m_ref[rows, cols]
            m_new = jnp.maximum(m_old, jnp.max(s, axis=1, keepdims=True))
            alpha = jnp.exp2(m_old - m_new)
            p = [jnp.exp2(s[:, i * HD:(i + 1) * HD] - m_new) for i in range(piece // HD)]
            psum = p[0]
            for part in p[1:]:
                psum = psum + part
            l_ref[rows, cols] = l_ref[rows, cols] * alpha + psum
            pb = jnp.concatenate([part.astype(BF16) for part in p], axis=1)
            pv = jnp.dot(pb, v, preferred_element_type=F32)
            acc_ref[rows, cols] = acc_ref[rows, cols] * alpha + pv
            m_ref[rows, cols] = m_new

        ahead = score(heads[0])
        for cols, after in zip(heads, heads[1:] + [None]):
            s, ahead = ahead, score(after) if after else None
            absorb(cols, s)

    @pl.loop(0, 2)
    def _(kind):
        unit(kind * piece, kv_ref[kind, 0], kv_ref[kind, 1], True)

    unit(piece, kv_ref[0, 0], kv_ref[0, 1], False)
    seq, waits = attention_order()
    marks = sorted(waits) + [len(seq)]

    @pl.loop(1, len(seq))
    def _(u):
        for mark in marks[:-1]:
            @pl.when(u == mark)
            def _():
                for name in waits[mark]:
                    act(name)

        dy = pick(u, [p[0] for p, _ in seq])
        dz = pick(u, [p[1] for p, _ in seq])
        which = pick(u, [w for _, w in seq])
        src = ((z + dz) % NX) * NX + (y + dy) % NX
        late = jnp.where(src > me, 1, 0)
        q_row = jnp.where(which == 0, 1, late) * piece
        kind = which * late
        at = dz * NX + dy
        unit(q_row, buf[kind, at, 0], buf[kind, at, 1], False)

    @pl.loop(0, 2)
    def _(part):
        rows = pl.ds(pl.multiple_of(part * piece, piece), piece)
        for h in range(n_heads):
            cols = slice(h * HD, (h + 1) * HD)
            total = jnp.sum(l_ref[rows, cols], axis=1, keepdims=True)
            o_ref[rows, cols] = (acc_ref[rows, cols] / total).astype(BF16)

    for key in started:
        copy_of(*key).wait_send()


def attention(q, kv):
    rows, width = q.shape
    piece = kv.shape[2]
    sem = pltpu.SemaphoreType.DMA
    return pl.pallas_call(
        functools.partial(attention_kernel, width // HD),
        out_shape=jax.ShapeDtypeStruct((rows, width), BF16),
        in_specs=[vmem_spec()] * 2,
        out_specs=vmem_spec(),
        scratch_shapes=[pltpu.VMEM((rows, width), F32)] * 3 + [pltpu.VMEM((2, NX * NX, 2, piece, HD), BF16),
                                                              sem((40,)), sem((2, NX * NX, 2))],
        compiler_params=params(2, 48), name='attention',
        cost_estimate=pl.CostEstimate(flops=18 * 10 ** 9, bytes_accessed=10 * 2 ** 20, transcendentals=35 * 10 ** 6),
    )(q, kv)


def solution(mesh):
    row_spec = P('dp', ('cp', 'tp'), None)
    head_cols = P(None, 'tp', None)
    cp_size = mesh.shape['cp']

    def local_layer(x, g_attn, w_q, w_k, w_v, w_o, g_mlp, w_gate, w_up, w_down):
        x_rows = x[0]
        block, dim = x_rows.shape
        rows = block * mesh.shape['tp']
        piece = rows // 2
        cp_index = lax.axis_index('cp')
        n_heads = w_q.shape[1]
        j = jnp.arange(rows, dtype=jnp.int32)
        positions = jnp.where(j < piece, cp_index * piece + j, (2 * cp_size - 1 - cp_index) * piece + j - piece)
        cos, sin = rope_tables(positions)
        q, kv = gather_qkv(x_rows, g_attn.reshape(1, dim), cos, sin, w_q.reshape(dim, n_heads * HD),
                           w_k.reshape(dim, HD), w_v.reshape(dim, HD), n_heads, piece)
        o = attention(q, kv)
        y_rows = scatter_product(o, w_o.reshape(n_heads * HD, dim), x_rows, 3)
        z_rows = mlp(y_rows, g_mlp.reshape(1, dim), w_gate, w_up, w_down)
        return z_rows[None]

    return jax.shard_map(local_layer, mesh=mesh,
                         in_specs=(row_spec, P(), head_cols, head_cols, head_cols, P('tp', None, None),
                                   P(), P(None, 'tp'), P(None, 'tp'), P('tp', None)),
                         out_specs=row_spec, check_vma=False)
```

```python
import functools
import math
import jax
import jax.numpy as jnp
from jax import lax
from jax.experimental import pallas as pl
from jax.experimental.pallas import tpu as pltpu
from jax.sharding import PartitionSpec as P

NORM_EPS = 1e-5
ROPE_THETA = 500000.0
HD = 128
NX = 4
MESH = pl.DeviceIdType.MESH
F32 = jnp.float32
BF16 = jnp.bfloat16


def params(cid, vmem_mib, **more):
    return pltpu.CompilerParams(collective_id=cid, has_side_effects=True, vmem_limit_bytes=min(vmem_mib * 2 ** 20, 67043328), **more)


def vmem_spec():
    return pl.BlockSpec(memory_space=pltpu.VMEM)


def hbm_spec():
    return pl.BlockSpec(memory_space=pltpu.HBM)


def rope_tables(positions):
    inv_freq = ROPE_THETA ** (-2.0 * jnp.arange(HD // 2, dtype=F32) / HD)
    angles = positions.astype(F32)[:, None] * inv_freq[None, :]
    c, s = jnp.cos(angles), jnp.sin(angles)
    return jnp.concatenate([c, c], axis=-1), jnp.concatenate([-s, s], axis=-1)


def enter(peers):
    barrier = pltpu.get_barrier_semaphore()
    for peer in peers:
        pl.semaphore_signal(barrier, inc=1, device_id=peer, device_id_type=MESH)
    pl.semaphore_wait(barrier, len(peers))


def tp_place():
    t = lax.axis_index('tp')
    x, c = t // 2, t % 2
    side = lambda d: {'tp': ((x + d) % NX) * 2 + c}
    return x, c, {'tp': x * 2 + 1 - c}, side(1), side(NX - 1)


OWN, MATE, LEFT, LEFT_MATE, RIGHT, RIGHT_MATE, FAR, FAR_MATE = range(8)
LO, HI = range(2)
NEAR_PART, FIRST_PART, LAST_PART, FAR_PART = range(4)
GATHER_PARTS = (((OWN, LO), (OWN, HI), (MATE, LO), (MATE, HI)),
                ((LEFT, LO), (RIGHT, HI), (LEFT_MATE, LO), (RIGHT_MATE, HI)),
                ((LEFT, HI), (RIGHT, LO), (LEFT_MATE, HI), (RIGHT_MATE, LO)),
                ((FAR, LO), (FAR, HI), (FAR_MATE, LO), (FAR_MATE, HI)))
GATHER_PLACE = {name: i for i, name in enumerate(n for part in GATHER_PARTS for n in part)}
N_PLACES = len(GATHER_PLACE)


def norm_into(x_ref, g_ref, which, full, rows):
    gain = g_ref[which:which + 1, :].astype(F32)
    step = min(16, rows)

    @pl.loop(0, rows // step)
    def _(i):
        where = pl.ds(pl.multiple_of(i * step, step), step)
        r = x_ref[where, :].astype(F32)
        mean_sq = jnp.mean(r * r, axis=-1, keepdims=True)
        full[where, :] = (r * lax.rsqrt(mean_sq + NORM_EPS) * gain).astype(BF16)


class Gather:
    def __init__(self, full, send_sem, recv_sem, half):
        self.full, self.send_sem, self.recv_sem, self.half = full, send_sem, recv_sem, half
        _, _, self.mate, self.right, self.left = tp_place()
        self.started, self.landing = [], {}

    def enter(self):
        enter([self.mate, self.right, self.left])

    def send(self, src, dst, h, device):
        rows = [pl.ds(GATHER_PLACE[slot, h] * self.half, self.half) for slot in (src, dst)]
        copy = pltpu.make_async_remote_copy(
            src_ref=self.full.at[rows[0]], dst_ref=self.full.at[rows[1]],
            send_sem=self.send_sem.at[len(self.started)], recv_sem=self.recv_sem.at[GATHER_PLACE[dst, h]],
            device_id=device, device_id_type=MESH)
        copy.start()
        self.started.append(copy)
        self.landing[dst, h] = copy

    def arrived(self, *names):
        for name in names:
            self.landing[name].wait_recv()

    def start(self):
        self.send(OWN, LEFT, LO, self.right)
        self.send(OWN, RIGHT, HI, self.left)
        for h in (LO, HI):
            self.send(OWN, MATE, h, self.mate)

    def relay(self):
        self.arrived((LEFT, LO))
        self.send(LEFT, FAR, LO, self.right)
        self.send(OWN, LEFT, HI, self.right)
        self.arrived((RIGHT, HI))
        self.send(RIGHT, FAR, HI, self.left)
        self.send(OWN, RIGHT, LO, self.left)
        self.send(LEFT, LEFT_MATE, LO, self.mate)
        self.send(RIGHT, RIGHT_MATE, HI, self.mate)

    def share_far(self):
        for h in (LO, HI):
            self.arrived((FAR, h))
            self.send(FAR, FAR_MATE, h, self.mate)

    def share_last(self):
        self.arrived((LEFT, HI))
        self.send(LEFT, LEFT_MATE, HI, self.mate)
        self.arrived((RIGHT, LO))
        self.send(RIGHT, RIGHT_MATE, LO, self.mate)

    def sent(self, *which):
        for copy in self.started:
            copy.wait_send()


def part_rows(part, block):
    t = lax.axis_index('tp')
    x, c = t // 2, t % 2
    rows = []
    for name, h in GATHER_PARTS[part]:
        dx, other = {OWN: 0, LEFT: NX - 1, RIGHT: 1, FAR: 2}[name // 2 * 2], name % 2
        core = 1 - c if other else c
        rows.append((((x + dx) % NX) * 2 + core) * block + h * (block // 2))
    return rows


N_SENDS = 14
GATHER_SEMS = [pltpu.SemaphoreType.DMA((N_SENDS,)), pltpu.SemaphoreType.DMA((N_PLACES,))]


def qkv_kernel(n_heads, x_hbm, g_ref, cos_ref, sin_ref, wq_hbm, wk_hbm, wv_hbm, q_ref, kv_ref, full, w, x_ref, send_sem, recv_sem, w_sem, x_sem):
    block = x_ref.shape[0]
    half = block // 2
    piece = kv_ref.shape[2]
    width = n_heads * HD
    loads = [pltpu.make_async_copy(wq_hbm, w.at[:, 0:width], w_sem.at[0]),
             pltpu.make_async_copy(wk_hbm, w.at[:, width:width + HD], w_sem.at[1]),
             pltpu.make_async_copy(wv_hbm, w.at[:, width + HD:width + 2 * HD], w_sem.at[2])]

    def rotate(v, cos, sin):
        f = v.astype(BF16).astype(F32)
        return (f * cos + pltpu.roll(f, HD // 2, 1) * sin).astype(BF16)

    def keys_values(part, rows, a):
        out = jnp.dot(a, w[:, width:], preferred_element_type=F32)
        for i, r in enumerate(rows):
            here = slice(i * half, (i + 1) * half)
            where = pl.ds(pl.multiple_of(r % piece, half), half)
            kv_ref[r // piece, 0, where, :] = rotate(out[here, :HD], cos_ref[pl.ds(r, half), :], sin_ref[pl.ds(r, half), :])
            kv_ref[r // piece, 1, where, :] = out[here, HD:].astype(BF16)

    def queries(part, rows, a):
        for start in range(0, width, 2 * HD):
            out = jnp.dot(a, w[:, start:start + 2 * HD], preferred_element_type=F32)
            for i, r in enumerate(rows):
                here = slice(i * half, (i + 1) * half)
                cos, sin = cos_ref[pl.ds(r, half), :], sin_ref[pl.ds(r, half), :]
                for k in (0, HD):
                    q_ref[pl.ds(r, half), start + k:start + k + HD] = rotate(out[here, k:k + HD], cos, sin)

    def compute(part):
        rows = [pl.multiple_of(r, half) for r in part_rows(part, block)]
        n = len(rows) * half
        a = full[part * n:(part + 1) * n, :]
        keys_values(part, rows, a)
        queries(part, rows, a)

    gather = Gather(full, send_sem, recv_sem, half)
    fetch = pltpu.make_async_copy(x_hbm, x_ref, x_sem)
    fetch.start()
    for load in loads:
        load.start()
    gather.enter()
    fetch.wait()
    norm_into(x_ref, g_ref, 0, full, block)
    gather.start()
    gather.arrived((MATE, LO), (MATE, HI))
    for load in loads:
        load.wait()
    compute(NEAR_PART)
    gather.relay()
    gather.arrived((LEFT_MATE, LO), (RIGHT_MATE, HI))
    compute(FIRST_PART)
    gather.share_far()
    gather.arrived((FAR_MATE, LO), (FAR_MATE, HI))
    compute(FAR_PART)
    gather.share_last()
    gather.arrived((LEFT_MATE, HI), (RIGHT_MATE, LO))
    compute(LAST_PART)
    gather.sent()


def gather_qkv(x_rows, g, cos, sin, w_q, w_k, w_v, n_heads, piece):
    block, dim = x_rows.shape
    rows = 2 * NX * block
    width = n_heads * HD
    return pl.pallas_call(
        functools.partial(qkv_kernel, n_heads),
        out_shape=(jax.ShapeDtypeStruct((rows, width), BF16), jax.ShapeDtypeStruct((2, 2, piece, HD), BF16)),
        in_specs=[hbm_spec()] + [vmem_spec()] * 3 + [hbm_spec()] * 3,
        out_specs=(vmem_spec(), vmem_spec()),
        scratch_shapes=[pltpu.VMEM((rows, dim), BF16), pltpu.VMEM((dim, width + 2 * HD), BF16), pltpu.VMEM((block, dim), BF16)]
        + GATHER_SEMS + [pltpu.SemaphoreType.DMA((3,)), pltpu.SemaphoreType.DMA],
        compiler_params=params(0, 48), name='gather_qkv',
        cost_estimate=pl.CostEstimate(flops=2 * rows * dim * (width + 2 * HD), bytes_accessed=2 * dim * (width + 2 * HD), transcendentals=0),
    )(x_rows, g, cos, sin, w_q, w_k, w_v)


def add_rows(dst, a, b):
    step = min(16, dst.shape[0])

    @pl.loop(0, dst.shape[0] // step)
    def _(i):
        at = pl.ds(pl.multiple_of(i * step, step), step)
        dst[at, :] = (a[at, :].astype(F32) + b[at, :].astype(F32)).astype(BF16)


def finish_rows(out, res, parts):
    step = min(16, out.shape[0])

    @pl.loop(0, out.shape[0] // step)
    def _(i):
        at = pl.ds(pl.multiple_of(i * step, step), step)
        total = parts[0][at, :].astype(F32)
        for part in parts[1:]:
            total = total + part[at, :].astype(F32)
        total = total.astype(BF16)
        out[at, :] = total if res is None else (res[at, :].astype(F32) + total.astype(F32)).astype(BF16)


def mlp_kernel(y_hbm, g_ref, wg_hbm, wu_hbm, wd_hbm, sum_ref, full, wg, wu, wd, hid, give, got, passing, last,
               send_sem, recv_sem, w_sem, d_sem, mate_sems, row_sems, io_sem):
    block, dim = y_hbm.shape
    half = block // 2
    cols = wg.shape[1]
    step = 256
    n_steps = cols // step
    loads = []
    for n in range(n_steps):
        at = slice(n * step, (n + 1) * step)
        loads.append((pltpu.make_async_copy(wg_hbm.at[:, at], wg.at[:, at], w_sem.at[0, n]),
                      pltpu.make_async_copy(wu_hbm.at[:, at], wu.at[:, at], w_sem.at[1, n])))
    load_d = pltpu.make_async_copy(wd_hbm, wd, d_sem)
    gather = Gather(full, send_sem, recv_sem, half)
    n_rows = 2 * block
    head, tail = slice(0, half), slice(half, block)

    def gate_up(part, lo, hi):
        def tile(n):
            at = pl.ds(pl.multiple_of(n * step, step), step)
            a = full[part * n_rows:(part + 1) * n_rows, :]
            gate = jnp.dot(a, wg[:, at], preferred_element_type=F32)
            up = jnp.dot(a, wu[:, at], preferred_element_type=F32)
            hid[part, :, at] = (jax.nn.silu(gate) * up).astype(BF16)

        @pl.loop(0, (hi - lo) // 2)
        def _(i):
            tile(lo + 2 * i)
            tile(lo + 2 * i + 1)

        if (hi - lo) % 2:
            tile(hi - 1)

    def down(part, first, *dst):
        wide = min(1024, dim)

        @pl.loop(0, dim // wide)
        def _(n):
            at = pl.ds(pl.multiple_of(n * wide, wide), wide)
            a = hid[part, first * block:(first + len(dst)) * block, :]
            out = jnp.dot(a, wd[:, at], preferred_element_type=F32).astype(BF16)
            for i, d in enumerate(dst):
                d[:, at] = out[i * block:(i + 1) * block, :]

    kept = {FAR_PART: full.at[block:n_rows], FIRST_PART: full.at[2 * n_rows - block:2 * n_rows],
            LAST_PART: full.at[n_rows:n_rows + block], NEAR_PART: full.at[0:block]}
    traded, moved = {}, []

    def trade(part, buffer):
        if part == FAR_PART:
            down(part, 1, give.at[buffer])
        else:
            down(part, 0, kept[part], give.at[buffer])
        traded[part] = pltpu.make_async_remote_copy(
            src_ref=give.at[buffer], dst_ref=got.at[part], send_sem=mate_sems.at[0, part], recv_sem=mate_sems.at[1, part],
            device_id=gather.mate, device_id_type=MESH)
        traded[part].start()

    def join(part):
        traded[part].wait_recv()
        add_rows(kept[part], kept[part], got.at[part])

    def move(src, dst, device):
        copy = pltpu.make_async_remote_copy(src_ref=src, dst_ref=dst, send_sem=row_sems.at[0, len(moved)],
                                            recv_sem=row_sems.at[1, len(moved)], device_id=device, device_id_type=MESH)
        copy.start()
        moved.append(copy)
        return copy

    fetch = pltpu.make_async_copy(y_hbm, give.at[0], io_sem)
    fetch.start()
    for pair in loads:
        for load in pair:
            load.start()
    load_d.start()
    gather.enter()
    fetch.wait()
    norm_into(give.at[0], g_ref, 1, full, block)
    gather.start()
    gather.arrived((MATE, LO), (MATE, HI))
    split = (n_steps + 1) // 2
    for lo, hi in ((0, split), (split, n_steps)):
        for pair in loads[lo:hi]:
            for load in pair:
                load.wait()
        gate_up(NEAR_PART, lo, hi)
        if lo == 0:
            gather.relay()
    gather.arrived((LEFT_MATE, LO), (RIGHT_MATE, HI))
    gate_up(FIRST_PART, 0, n_steps - 1)
    gather.share_far()
    gate_up(FIRST_PART, n_steps - 1, n_steps)
    gather.arrived((FAR_MATE, LO), (FAR_MATE, HI))
    gate_up(FAR_PART, 0, n_steps)
    load_d.wait()
    trade(FAR_PART, 0)
    down(FAR_PART, 0, kept[FAR_PART])
    gather.share_last()
    join(FAR_PART)
    pass_right = move(kept[FAR_PART].at[head], passing.at[0], gather.right)
    pass_left = move(kept[FAR_PART].at[tail], passing.at[1], gather.left)
    gather.arrived((LEFT_MATE, HI), (RIGHT_MATE, LO))
    gather.sent()
    trade(FIRST_PART, 1)
    gate_up(LAST_PART, 0, split)
    join(FIRST_PART)
    moved_first = [move(kept[FIRST_PART].at[head], last.at[1, head], gather.left),
                   move(kept[FIRST_PART].at[tail], last.at[0, tail], gather.right)]
    gate_up(LAST_PART, split, n_steps)
    traded[FAR_PART].wait_send()
    trade(LAST_PART, 0)
    traded[FIRST_PART].wait_send()
    trade(NEAR_PART, 1)
    join(LAST_PART)
    pass_left.wait_recv()
    add_rows(kept[LAST_PART].at[head], kept[LAST_PART].at[head], passing.at[1])
    pass_right.wait_recv()
    add_rows(kept[LAST_PART].at[tail], kept[LAST_PART].at[tail], passing.at[0])
    moved_last = [move(kept[LAST_PART].at[head], last.at[1, tail], gather.left),
                  move(kept[LAST_PART].at[tail], last.at[0, head], gather.right)]
    traded[LAST_PART].wait_send()
    traded[NEAR_PART].wait_recv()
    for copy in moved_first + moved_last:
        copy.wait_recv()
    finish_rows(sum_ref, None, [kept[NEAR_PART], got.at[NEAR_PART], last.at[0], last.at[1]])
    traded[NEAR_PART].wait_send()
    for copy in moved:
        copy.wait_send()


def mlp(y_rows, g, w_gate, w_up, w_down):
    block, dim = y_rows.shape
    rows = 2 * NX * block
    cols = w_gate.shape[1]
    sem = pltpu.SemaphoreType.DMA
    buffer = lambda *shape: pltpu.VMEM(shape, BF16)
    return pl.pallas_call(
        mlp_kernel,
        out_shape=jax.ShapeDtypeStruct((block, dim), BF16),
        in_specs=[hbm_spec(), vmem_spec()] + [hbm_spec()] * 3,
        out_specs=vmem_spec(),
        scratch_shapes=[buffer(rows, dim), buffer(dim, cols), buffer(dim, cols), buffer(cols, dim), buffer(NX, 2 * block, cols),
                        buffer(2, block, dim), buffer(NX, block, dim), buffer(2, block // 2, dim), buffer(2, block, dim)]
        + GATHER_SEMS + [sem((2, cols // 256)), sem, sem((2, NX)), sem((2, 6)), sem],
        compiler_params=params(1, 64), name='mlp',
        cost_estimate=pl.CostEstimate(flops=6 * rows * dim * cols, bytes_accessed=6 * dim * cols, transcendentals=rows * cols),
    )(y_rows, g, w_gate, w_up, w_down)


def scatter_kernel(h_ref, w_hbm, res_ref, out_ref, w, give, mine, got, passing, last, w_sem, give_sem, got_sem, send_sem, recv_sem):
    x, c, partner, right, left = tp_place()
    block, dim = res_ref.shape
    half = block // 2
    step = 512
    n_steps = dim // step
    loads = []
    for n in range(n_steps):
        at = slice(n * step, (n + 1) * step)
        loads.append(pltpu.make_async_copy(w_hbm.at[:, at], w.at[:, at], w_sem.at[n]))
        loads[-1].start()
    enter([partner, right, left])
    h0, h1 = slice(0, half), slice(half, block)

    def product(dx, core, dst, wait_w=False):
        start = pl.multiple_of((((x + dx) % NX) * 2 + core) * block, block)
        if wait_w:
            for load in loads:
                load.wait()

        @pl.loop(0, n_steps)
        def _(n):
            at = pl.ds(pl.multiple_of(n * step, step), step)
            dst[:, at] = jnp.dot(h_ref[pl.ds(start, block), :], w[:, at], preferred_element_type=F32).astype(BF16)

    def exchange(b, dx, wait_w=False):
        product(dx, 1 - c, give.at[b], wait_w)
        copy = pltpu.make_async_remote_copy(src_ref=give.at[b], dst_ref=got.at[b], send_sem=give_sem.at[b],
                                            recv_sem=got_sem.at[b], device_id=partner, device_id_type=MESH)
        copy.start()
        product(dx, c, mine.at[b])
        return copy

    started = []

    def send(src, dst, device):
        n = len(started)
        copy = pltpu.make_async_remote_copy(src_ref=src, dst_ref=dst, send_sem=send_sem.at[n], recv_sem=recv_sem.at[n],
                                            device_id=device, device_id_type=MESH)
        copy.start()
        started.append(copy)
        return copy

    pair = exchange(0, 2, True)
    pair.wait_recv()
    add_rows(mine.at[0], mine.at[0], got.at[0])
    pass_right = send(mine.at[0, h0], passing.at[0], right)
    pass_left = send(mine.at[0, h1], passing.at[1], left)
    pair_r = exchange(1, 1)
    pair_l = exchange(2, NX - 1)
    pair_r.wait_recv()
    add_rows(mine.at[1], mine.at[1], got.at[1])
    to_right_1 = send(mine.at[1, h1], last.at[0, h1], right)
    pair_l.wait_recv()
    add_rows(mine.at[2], mine.at[2], got.at[2])
    to_left_0 = send(mine.at[2, h0], last.at[1, h0], left)
    pair_o = exchange(3, 0)
    pass_right.wait_recv()
    add_rows(mine.at[1, h0], mine.at[1, h0], passing.at[0])
    to_right_0 = send(mine.at[1, h0], last.at[0, h0], right)
    pass_left.wait_recv()
    add_rows(mine.at[2, h1], mine.at[2, h1], passing.at[1])
    to_left_1 = send(mine.at[2, h1], last.at[1, h1], left)
    pair_o.wait_recv()
    for copy in (to_right_1, to_left_0, to_right_0, to_left_1):
        copy.wait_recv()
    finish_rows(out_ref, res_ref, [mine.at[3], got.at[3], last.at[0], last.at[1]])
    for copy in (pair, pair_r, pair_l, pair_o, *started):
        copy.wait_send()


def scatter_product(h, w, res, cid):
    rows, depth = h.shape
    block, dim = res.shape
    half = block // 2
    sem = pltpu.SemaphoreType.DMA
    return pl.pallas_call(
        scatter_kernel,
        out_shape=jax.ShapeDtypeStruct((block, dim), BF16),
        in_specs=[vmem_spec(), hbm_spec(), vmem_spec()],
        out_specs=vmem_spec(),
        scratch_shapes=[pltpu.VMEM((depth, dim), BF16)] + [pltpu.VMEM((4, block, dim), BF16)] * 3
        + [pltpu.VMEM((2, half, dim), BF16), pltpu.VMEM((2, block, dim), BF16),
           sem((max(1, dim // 512),)), sem((4,)), sem((4,)), sem((6,)), sem((6,))],
        compiler_params=params(cid, 48), name='scatter_product_%d' % cid,
        cost_estimate=pl.CostEstimate(flops=2 * rows * dim * depth, bytes_accessed=2 * dim * depth, transcendentals=0),
    )(h, w, res)


def attention_order():
    seq = [((0, 0), 0)]
    waits = {}

    def then(actions, *units):
        waits.setdefault(len(seq), []).extend(actions)
        seq.extend(units)

    first = lambda *s: [(p, 0) for p in s]
    both = lambda *s: [(p, w) for p in s for w in (0, 1)]
    then(['T1'], *first((1, 0), (3, 0)))
    then(['F0'], *first((0, 1), (0, 3)))
    then(['T2'], *first((2, 0)), ((0, 1), 1), ((0, 3), 1))
    then(['F1'], ((1, 0), 1), ((3, 0), 1))
    then(['F3'], *both((1, 1), (1, 3)))
    then(['F2'], *both((3, 1), (3, 3)))
    then(['E0'], ((2, 0), 1), *both((0, 2)))
    then(['E1', 'E3'], *both((1, 2), (3, 2), (2, 1), (2, 3)))
    then(['E2'], *both((2, 2)))
    return seq, waits


def pick(index, values):
    out = index * 0 + values[0]
    for i, v in enumerate(values[1:], 1):
        if v != values[i - 1]:
            out = jnp.where(index >= i, v, out)
    return out


def attention_kernel(n_heads, q_ref, kv_ref, o_ref, m_ref, l_ref, acc_ref, buf, send_sem, recv_sem):
    piece = kv_ref.shape[2]
    me = lax.axis_index('cp')
    y, z = me % NX, me // NX
    scale = HD ** -0.5 * math.log2(math.e)
    at_y = lambda d: {'cp': z * NX + (y + d) % NX}
    at_z = lambda d: {'cp': ((z + d) % NX) * NX + y}
    enter([at_y(1), at_y(3), at_z(1), at_z(3)])
    axes = ((at_y, at_z), (at_z, at_y))

    def slot(kind, da, db):
        dy, dz = (da, db) if kind == 0 else (db, da)
        return dz * NX + dy

    started, landing = [], {}

    def copy_of(kind, src, dst, axis, d, part, n):
        source = kv_ref.at[kind] if src == (0, 0) else buf.at[kind, slot(kind, *src)]
        target = buf.at[kind, slot(kind, *dst)]
        if part is not None:
            source, target = source.at[part], target.at[part]
        return pltpu.make_async_remote_copy(
            src_ref=source, dst_ref=target, send_sem=send_sem.at[n],
            recv_sem=recv_sem.at[kind, slot(kind, *dst), part or 0],
            device_id=axes[kind][axis](d), device_id_type=MESH)

    def send(kind, src, dst, axis, d, part=None):
        key = (kind, src, dst, axis, d, part, len(started))
        copy_of(*key).start()
        started.append(key)
        landing[kind, dst, part] = key

    def landed(*key):
        copy_of(*landing[key]).wait_recv()

    def arrived(kind, *names):
        for name in names:
            for part in ((0, 1) if 2 in name else (None,)):
                landed(kind, name, part)

    def along_b(kind, da):
        send(kind, (da, 0), (da, 3), 1, 1)
        send(kind, (da, 0), (da, 1), 1, 3)

    def act(name):
        step, da = name[0], int(name[1])
        for kind in range(2):
            if name == 'T1':
                arrived(kind, (1, 0), (3, 0))
                send(kind, (3, 0), (2, 0), 0, 1, 0)
                send(kind, (1, 0), (2, 0), 0, 3, 1)
                along_b(kind, 1)
                along_b(kind, 3)
            elif name == 'T2':
                arrived(kind, (2, 0))
                along_b(kind, 2)
            elif step == 'F':
                for db, d, part in ((3, 1, 0), (1, 3, 1)):
                    if da == 2:
                        landed(kind, (2, db), None)
                    else:
                        arrived(kind, (da, db))
                    send(kind, (da, db), (da, 2), 1, d, part)
            else:
                for part in (0, 1):
                    landed(kind, (da, 2), part)

    kinds = (0, 1)
    for kind in kinds:
        send(kind, (0, 0), (3, 0), 0, 1)
        send(kind, (0, 0), (1, 0), 0, 3)
    for kind in kinds:
        along_b(kind, 0)

    m_ref[...] = jnp.full_like(m_ref, -1e30)
    l_ref[...] = jnp.zeros_like(l_ref)
    acc_ref[...] = jnp.zeros_like(acc_ref)

    def unit(q_row, k, v, masked):
        rows = pl.ds(pl.multiple_of(q_row, piece), piece)
        heads = [slice(h * HD, (h + 1) * HD) for h in range(n_heads)]

        def score(cols):
            s = lax.dot_general(q_ref[rows, cols], k, (((1,), (1,)), ((), ())), preferred_element_type=F32)
            if masked:
                row = lax.broadcasted_iota(jnp.int32, (piece, piece), 0)
                col = lax.broadcasted_iota(jnp.int32, (piece, piece), 1)
                s = jnp.where(row >= col, s, -1e30)
            return s

        def absorb(cols, s):
            m_old = m_ref[rows, cols]
            m_new = jnp.maximum(m_old, jnp.max(s, axis=1, keepdims=True) * scale)
            alpha = jnp.exp2(m_old - m_new)
            p = [jnp.exp2(s[:, i * HD:(i + 1) * HD] * scale - m_new) for i in range(piece // HD)]
            psum = p[0]
            for part in p[1:]:
                psum = psum + part
            l_ref[rows, cols] = l_ref[rows, cols] * alpha + psum
            pb = jnp.concatenate([part.astype(BF16) for part in p], axis=1)
            pv = jnp.dot(pb, v, preferred_element_type=F32)
            acc_ref[rows, cols] = acc_ref[rows, cols] * alpha + pv
            m_ref[rows, cols] = m_new

        ahead = score(heads[0])
        for cols, after in zip(heads, heads[1:] + [None]):
            s, ahead = ahead, score(after) if after else None
            absorb(cols, s)

    @pl.loop(0, 2)
    def _(kind):
        unit(kind * piece, kv_ref[kind, 0], kv_ref[kind, 1], True)

    unit(piece, kv_ref[0, 0], kv_ref[0, 1], False)
    seq, waits = attention_order()
    marks = sorted(waits) + [len(seq)]

    @pl.loop(1, len(seq))
    def _(u):
        for mark in marks[:-1]:
            @pl.when(u == mark)
            def _():
                for name in waits[mark]:
                    act(name)

        dy = pick(u, [p[0] for p, _ in seq])
        dz = pick(u, [p[1] for p, _ in seq])
        which = pick(u, [w for _, w in seq])
        src = ((z + dz) % NX) * NX + (y + dy) % NX
        late = jnp.where(src > me, 1, 0)
        q_row = jnp.where(which == 0, 1, late) * piece
        kind = which * late
        at = dz * NX + dy
        unit(q_row, buf[kind, at, 0], buf[kind, at, 1], False)

    @pl.loop(0, 2)
    def _(part):
        rows = pl.ds(pl.multiple_of(part * piece, piece), piece)
        for h in range(n_heads):
            cols = slice(h * HD, (h + 1) * HD)
            total = jnp.sum(l_ref[rows, cols], axis=1, keepdims=True)
            o_ref[rows, cols] = (acc_ref[rows, cols] / total).astype(BF16)

    for key in started:
        copy_of(*key).wait_send()


def attention(q, kv):
    rows, width = q.shape
    piece = kv.shape[2]
    sem = pltpu.SemaphoreType.DMA
    return pl.pallas_call(
        functools.partial(attention_kernel, width // HD),
        out_shape=jax.ShapeDtypeStruct((rows, width), BF16),
        in_specs=[vmem_spec()] * 2,
        out_specs=vmem_spec(),
        scratch_shapes=[pltpu.VMEM((rows, width), F32)] * 3 + [pltpu.VMEM((2, NX * NX, 2, piece, HD), BF16),
                                                              sem((40,)), sem((2, NX * NX, 2))],
        compiler_params=params(2, 48), name='attention',
        cost_estimate=pl.CostEstimate(flops=18 * 10 ** 9, bytes_accessed=10 * 2 ** 20, transcendentals=35 * 10 ** 6),
    )(q, kv)


def solution(mesh):
    row_spec = P('dp', ('cp', 'tp'), None)
    head_cols = P(None, 'tp', None)
    cp_size = mesh.shape['cp']

    def local_layer(x, g_attn, w_q, w_k, w_v, w_o, g_mlp, w_gate, w_up, w_down):
        x_rows = x[0]
        block, dim = x_rows.shape
        rows = block * mesh.shape['tp']
        piece = rows // 2
        cp_index = lax.axis_index('cp')
        n_heads = w_q.shape[1]
        j = jnp.arange(rows, dtype=jnp.int32)
        positions = jnp.where(j < piece, cp_index * piece + j, (2 * cp_size - 1 - cp_index) * piece + j - piece)
        cos, sin = rope_tables(positions)
        gains = jnp.stack([g_attn, g_mlp])
        in_hbm = [pltpu.with_memory_space_constraint(v, pltpu.HBM) for v in (x_rows, w_k.reshape(dim, HD), w_v.reshape(dim, HD))]
        q, kv = gather_qkv(in_hbm[0], gains, cos, sin, w_q.reshape(dim, n_heads * HD), *in_hbm[1:], n_heads, piece)
        o = attention(q, kv)
        y_rows = scatter_product(o, w_o.reshape(n_heads * HD, dim), x_rows, 3)
        d_rows = mlp(y_rows, gains, w_gate, w_up, w_down)
        return (y_rows.astype(F32) + d_rows.astype(F32)).astype(BF16)[None]

    return jax.shard_map(local_layer, mesh=mesh,
                         in_specs=(row_spec, P(), head_cols, head_cols, head_cols, P('tp', None, None),
                                   P(), P(None, 'tp'), P(None, 'tp'), P('tp', None)),
                         out_specs=row_spec, check_vma=False)
```

```python
import functools
import math
import jax
import jax.numpy as jnp
from jax import lax
from jax.experimental import pallas as pl
from jax.experimental.pallas import tpu as pltpu
from jax.sharding import PartitionSpec as P

NORM_EPS = 1e-5
ROPE_THETA = 500000.0
HD = 128
NX = 4
MESH = pl.DeviceIdType.MESH
F32 = jnp.float32
BF16 = jnp.bfloat16


def params(cid, vmem_mib, **more):
    return pltpu.CompilerParams(collective_id=cid, has_side_effects=True, vmem_limit_bytes=min(vmem_mib * 2 ** 20, 67043328), **more)


def vmem_spec():
    return pl.BlockSpec(memory_space=pltpu.VMEM)


def hbm_spec():
    return pl.BlockSpec(memory_space=pltpu.HBM)


def rope_tables(positions):
    inv_freq = ROPE_THETA ** (-2.0 * jnp.arange(HD // 2, dtype=F32) / HD)
    angles = positions.astype(F32)[:, None] * inv_freq[None, :]
    c, s = jnp.cos(angles), jnp.sin(angles)
    return jnp.concatenate([c, c], axis=-1), jnp.concatenate([-s, s], axis=-1)


def enter(peers):
    barrier = pltpu.get_barrier_semaphore()
    for peer in peers:
        pl.semaphore_signal(barrier, inc=1, device_id=peer, device_id_type=MESH)
    pl.semaphore_wait(barrier, len(peers))


def tp_place():
    t = lax.axis_index('tp')
    x, c = t // 2, t % 2
    side = lambda d: {'tp': ((x + d) % NX) * 2 + c}
    return x, c, {'tp': x * 2 + 1 - c}, side(1), side(NX - 1)


OWN, MATE, LEFT, LEFT_MATE, RIGHT, RIGHT_MATE, FAR, FAR_MATE = range(8)
LO, HI = range(2)
NEAR_PART, FIRST_PART, LAST_PART, FAR_PART = range(4)
GATHER_PARTS = (((OWN, LO), (OWN, HI), (MATE, LO), (MATE, HI)),
                ((LEFT, LO), (RIGHT, HI), (LEFT_MATE, LO), (RIGHT_MATE, HI)),
                ((LEFT, HI), (RIGHT, LO), (LEFT_MATE, HI), (RIGHT_MATE, LO)),
                ((FAR, LO), (FAR, HI), (FAR_MATE, LO), (FAR_MATE, HI)))
GATHER_PLACE = {name: i for i, name in enumerate(n for part in GATHER_PARTS for n in part)}
N_PLACES = len(GATHER_PLACE)


def norm_into(x_ref, g_ref, full, rows):
    gain = jnp.concatenate([g_ref[i:i + 1, :] for i in range(g_ref.shape[0])], axis=1).astype(F32)
    step = min(16, rows)

    @pl.loop(0, rows // step)
    def _(i):
        where = pl.ds(pl.multiple_of(i * step, step), step)
        r = x_ref[where, :].astype(F32)
        mean_sq = jnp.mean(r * r, axis=-1, keepdims=True)
        full[where, :] = (r * lax.rsqrt(mean_sq + NORM_EPS) * gain).astype(BF16)


class Gather:
    def __init__(self, full, send_sem, recv_sem, half):
        self.full, self.send_sem, self.recv_sem, self.half = full, send_sem, recv_sem, half
        _, _, self.mate, self.right, self.left = tp_place()
        self.started, self.landing = [], {}

    def enter(self):
        enter([self.mate, self.right, self.left])

    def send(self, src, dst, h, device):
        rows = [pl.ds(GATHER_PLACE[slot, h] * self.half, self.half) for slot in (src, dst)]
        copy = pltpu.make_async_remote_copy(
            src_ref=self.full.at[rows[0]], dst_ref=self.full.at[rows[1]],
            send_sem=self.send_sem.at[len(self.started)], recv_sem=self.recv_sem.at[GATHER_PLACE[dst, h]],
            device_id=device, device_id_type=MESH)
        copy.start()
        self.started.append(copy)
        self.landing[dst, h] = copy

    def arrived(self, *names):
        for name in names:
            self.landing[name].wait_recv()

    def rest(self):
        self.send(OWN, LEFT, HI, self.right)
        self.send(OWN, RIGHT, LO, self.left)

    def start(self):
        self.send(OWN, LEFT, LO, self.right)
        self.send(OWN, RIGHT, HI, self.left)
        for h in (LO, HI):
            self.send(OWN, MATE, h, self.mate)

    def relay(self):
        self.arrived((LEFT, LO))
        self.send(LEFT, FAR, LO, self.right)
        self.arrived((RIGHT, HI))
        self.send(RIGHT, FAR, HI, self.left)
        self.send(LEFT, LEFT_MATE, LO, self.mate)
        self.send(RIGHT, RIGHT_MATE, HI, self.mate)

    def share_far(self):
        for h in (LO, HI):
            self.arrived((FAR, h))
            self.send(FAR, FAR_MATE, h, self.mate)

    def share_last(self):
        self.arrived((LEFT, HI))
        self.send(LEFT, LEFT_MATE, HI, self.mate)
        self.arrived((RIGHT, LO))
        self.send(RIGHT, RIGHT_MATE, LO, self.mate)

    def sent(self, *which):
        for copy in self.started:
            copy.wait_send()


def part_rows(part, block):
    t = lax.axis_index('tp')
    x, c = t // 2, t % 2
    rows = []
    for name, h in GATHER_PARTS[part]:
        dx, other = {OWN: 0, LEFT: NX - 1, RIGHT: 1, FAR: 2}[name // 2 * 2], name % 2
        core = 1 - c if other else c
        rows.append((((x + dx) % NX) * 2 + core) * block + h * (block // 2))
    return rows


N_SENDS = 14
GATHER_SEMS = [pltpu.SemaphoreType.DMA((N_SENDS,)), pltpu.SemaphoreType.DMA((N_PLACES,))]


def qkv_kernel(n_heads, x_hbm, g_ref, cos_ref, sin_ref, wq_hbm, wk_hbm, wv_hbm, q_ref, kv_ref, full, w, x_ref, send_sem, recv_sem, w_sem, x_sem):
    block = x_ref.shape[0]
    half = block // 2
    piece = kv_ref.shape[2]
    width = n_heads * HD
    loads = [pltpu.make_async_copy(wq_hbm, w.at[:, 0:width], w_sem.at[0]),
             pltpu.make_async_copy(wk_hbm, w.at[:, width:width + HD], w_sem.at[1]),
             pltpu.make_async_copy(wv_hbm, w.at[:, width + HD:width + 2 * HD], w_sem.at[2])]

    def rotate(v, cos, sin):
        f = v.astype(BF16).astype(F32)
        return (f * cos + pltpu.roll(f, HD // 2, 1) * sin).astype(BF16)

    def keys_values(part, rows, a):
        out = jnp.dot(a, w[:, width:], preferred_element_type=F32)
        for i, r in enumerate(rows):
            here = slice(i * half, (i + 1) * half)
            where = pl.ds(pl.multiple_of(r % piece, half), half)
            kv_ref[r // piece, 0, where, :] = rotate(out[here, :HD], cos_ref[pl.ds(r, half), :], sin_ref[pl.ds(r, half), :])
            kv_ref[r // piece, 1, where, :] = out[here, HD:].astype(BF16)

    def queries(part, rows, a):
        for start in range(0, width, 2 * HD):
            out = jnp.dot(a, w[:, start:start + 2 * HD], preferred_element_type=F32)
            for i, r in enumerate(rows):
                here = slice(i * half, (i + 1) * half)
                cos, sin = cos_ref[pl.ds(r, half), :], sin_ref[pl.ds(r, half), :]
                for k in (0, HD):
                    q_ref[pl.ds(r, half), start + k:start + k + HD] = rotate(out[here, k:k + HD], cos, sin)

    def compute(part):
        rows = [pl.multiple_of(r, half) for r in part_rows(part, block)]
        n = len(rows) * half
        a = full[part * n:(part + 1) * n, :]
        keys_values(part, rows, a)
        queries(part, rows, a)

    gather = Gather(full, send_sem, recv_sem, half)
    fetch = pltpu.make_async_copy(x_hbm, x_ref, x_sem)
    fetch.start()
    for load in loads:
        load.start()
    gather.enter()
    fetch.wait()
    norm_into(x_ref, g_ref, full, block)
    gather.start()
    gather.rest()
    gather.arrived((MATE, LO), (MATE, HI))
    for load in loads:
        load.wait()
    compute(NEAR_PART)
    gather.relay()
    gather.arrived((LEFT_MATE, LO), (RIGHT_MATE, HI))
    compute(FIRST_PART)
    gather.share_last()
    gather.arrived((LEFT_MATE, HI), (RIGHT_MATE, LO))
    compute(LAST_PART)
    gather.share_far()
    gather.arrived((FAR_MATE, LO), (FAR_MATE, HI))
    compute(FAR_PART)
    gather.sent()


def gather_qkv(x_rows, g, cos, sin, w_q, w_k, w_v, n_heads, piece):
    block, dim = x_rows.shape
    rows = 2 * NX * block
    width = n_heads * HD
    return pl.pallas_call(
        functools.partial(qkv_kernel, n_heads),
        out_shape=(jax.ShapeDtypeStruct((rows, width), BF16), jax.ShapeDtypeStruct((2, 2, piece, HD), BF16)),
        in_specs=[hbm_spec()] + [vmem_spec()] * 3 + [hbm_spec()] * 3,
        out_specs=(vmem_spec(), vmem_spec()),
        scratch_shapes=[pltpu.VMEM((rows, dim), BF16), pltpu.VMEM((dim, width + 2 * HD), BF16), pltpu.VMEM((block, dim), BF16)]
        + GATHER_SEMS + [pltpu.SemaphoreType.DMA((3,)), pltpu.SemaphoreType.DMA],
        compiler_params=params(0, 48), name='gather_qkv',
        cost_estimate=pl.CostEstimate(flops=2 * rows * dim * (width + 2 * HD), bytes_accessed=2 * dim * (width + 2 * HD), transcendentals=0),
    )(x_rows, g, cos, sin, w_q, w_k, w_v)


def add_rows(dst, a, b):
    step = min(16, dst.shape[0])

    @pl.loop(0, dst.shape[0] // step)
    def _(i):
        at = pl.ds(pl.multiple_of(i * step, step), step)
        dst[at, :] = (a[at, :].astype(F32) + b[at, :].astype(F32)).astype(BF16)


def finish_rows(out, res, parts):
    step = min(16, out.shape[0])

    @pl.loop(0, out.shape[0] // step)
    def _(i):
        at = pl.ds(pl.multiple_of(i * step, step), step)
        total = parts[0][at, :].astype(F32)
        for part in parts[1:]:
            total = total + part[at, :].astype(F32)
        total = total.astype(BF16)
        out[at, :] = total if res is None else (res[at, :].astype(F32) + total.astype(F32)).astype(BF16)


def mlp_kernel(y_hbm, g_ref, wg_hbm, wu_hbm, wd_hbm, sum_ref, full, wg, wu, wd, hid, give, got, passing, last,
               send_sem, recv_sem, w_sem, d_sem, mate_sems, row_sems, io_sem):
    block, dim = y_hbm.shape
    half = block // 2
    cols = wg.shape[1]
    step = 256
    n_steps = cols // step
    loads = []
    for n in range(n_steps):
        at = slice(n * step, (n + 1) * step)
        loads.append((pltpu.make_async_copy(wg_hbm.at[:, at], wg.at[:, at], w_sem.at[0, n]),
                      pltpu.make_async_copy(wu_hbm.at[:, at], wu.at[:, at], w_sem.at[1, n])))
    load_d = pltpu.make_async_copy(wd_hbm, wd, d_sem)
    gather = Gather(full, send_sem, recv_sem, half)
    n_rows = 2 * block
    head, tail = slice(0, half), slice(half, block)

    def gate_up(part, lo, hi):
        def tile(n):
            at = pl.ds(pl.multiple_of(n * step, step), step)
            a = full[part * n_rows:(part + 1) * n_rows, :]
            gate = jnp.dot(a, wg[:, at], preferred_element_type=F32)
            up = jnp.dot(a, wu[:, at], preferred_element_type=F32)
            hid[part, :, at] = (jax.nn.silu(gate) * up).astype(BF16)

        @pl.loop(0, (hi - lo) // 2)
        def _(i):
            tile(lo + 2 * i)
            tile(lo + 2 * i + 1)

        if (hi - lo) % 2:
            tile(hi - 1)

    def down(part, first, *dst):
        wide = min(1024, dim)

        @pl.loop(0, dim // wide)
        def _(n):
            at = pl.ds(pl.multiple_of(n * wide, wide), wide)
            a = hid[part, first * block:(first + len(dst)) * block, :]
            out = jnp.dot(a, wd[:, at], preferred_element_type=F32).astype(BF16)
            for i, d in enumerate(dst):
                d[:, at] = out[i * block:(i + 1) * block, :]

    kept = {FAR_PART: full.at[block:n_rows], FIRST_PART: full.at[2 * n_rows - block:2 * n_rows],
            LAST_PART: full.at[n_rows:n_rows + block], NEAR_PART: full.at[0:block]}
    traded, moved = {}, []

    def trade(part, buffer):
        if part == FAR_PART:
            down(part, 1, give.at[buffer])
        else:
            down(part, 0, kept[part], give.at[buffer])
        traded[part] = pltpu.make_async_remote_copy(
            src_ref=give.at[buffer], dst_ref=got.at[part], send_sem=mate_sems.at[0, part], recv_sem=mate_sems.at[1, part],
            device_id=gather.mate, device_id_type=MESH)
        traded[part].start()

    def join(part):
        traded[part].wait_recv()
        add_rows(kept[part], kept[part], got.at[part])

    def move(src, dst, device):
        copy = pltpu.make_async_remote_copy(src_ref=src, dst_ref=dst, send_sem=row_sems.at[0, len(moved)],
                                            recv_sem=row_sems.at[1, len(moved)], device_id=device, device_id_type=MESH)
        copy.start()
        moved.append(copy)
        return copy

    fetch = pltpu.make_async_copy(y_hbm, give.at[0], io_sem)
    fetch.start()
    for pair in loads:
        for load in pair:
            load.start()
    load_d.start()
    gather.enter()
    fetch.wait()
    norm_into(give.at[0], g_ref, full, block)
    gather.start()
    gather.arrived((MATE, LO), (MATE, HI))
    split = (n_steps + 1) // 2
    for lo, hi in ((0, split), (split, n_steps)):
        for pair in loads[lo:hi]:
            for load in pair:
                load.wait()
        gate_up(NEAR_PART, lo, hi)
        if lo == 0:
            gather.relay()
            gather.rest()
    gather.arrived((LEFT_MATE, LO), (RIGHT_MATE, HI))
    gate_up(FIRST_PART, 0, n_steps - 1)
    gather.share_far()
    gate_up(FIRST_PART, n_steps - 1, n_steps)
    gather.arrived((FAR_MATE, LO), (FAR_MATE, HI))
    gate_up(FAR_PART, 0, n_steps)
    load_d.wait()
    trade(FAR_PART, 0)
    down(FAR_PART, 0, kept[FAR_PART])
    gather.share_last()
    join(FAR_PART)
    pass_right = move(kept[FAR_PART].at[head], passing.at[0], gather.right)
    pass_left = move(kept[FAR_PART].at[tail], passing.at[1], gather.left)
    gather.arrived((LEFT_MATE, HI), (RIGHT_MATE, LO))
    gather.sent()
    trade(FIRST_PART, 1)
    gate_up(LAST_PART, 0, split)
    join(FIRST_PART)
    moved_first = [move(kept[FIRST_PART].at[head], last.at[1, head], gather.left),
                   move(kept[FIRST_PART].at[tail], last.at[0, tail], gather.right)]
    gate_up(LAST_PART, split, n_steps)
    traded[FAR_PART].wait_send()
    trade(LAST_PART, 0)
    traded[FIRST_PART].wait_send()
    trade(NEAR_PART, 1)
    join(LAST_PART)
    pass_left.wait_recv()
    add_rows(kept[LAST_PART].at[head], kept[LAST_PART].at[head], passing.at[1])
    pass_right.wait_recv()
    add_rows(kept[LAST_PART].at[tail], kept[LAST_PART].at[tail], passing.at[0])
    moved_last = [move(kept[LAST_PART].at[head], last.at[1, tail], gather.left),
                  move(kept[LAST_PART].at[tail], last.at[0, head], gather.right)]
    traded[LAST_PART].wait_send()
    traded[NEAR_PART].wait_recv()
    for copy in moved_first + moved_last:
        copy.wait_recv()
    finish_rows(sum_ref, None, [kept[NEAR_PART], got.at[NEAR_PART], last.at[0], last.at[1]])
    traded[NEAR_PART].wait_send()
    for copy in moved:
        copy.wait_send()


def mlp(y_rows, g, w_gate, w_up, w_down):
    block, dim = y_rows.shape
    rows = 2 * NX * block
    cols = w_gate.shape[1]
    sem = pltpu.SemaphoreType.DMA
    buffer = lambda *shape: pltpu.VMEM(shape, BF16)
    return pl.pallas_call(
        mlp_kernel,
        out_shape=jax.ShapeDtypeStruct((block, dim), BF16),
        in_specs=[hbm_spec(), vmem_spec()] + [hbm_spec()] * 3,
        out_specs=vmem_spec(),
        scratch_shapes=[buffer(rows, dim), buffer(dim, cols), buffer(dim, cols), buffer(cols, dim), buffer(NX, 2 * block, cols),
                        buffer(2, block, dim), buffer(NX, block, dim), buffer(2, block // 2, dim), buffer(2, block, dim)]
        + GATHER_SEMS + [sem((2, cols // 256)), sem, sem((2, NX)), sem((2, 6)), sem],
        compiler_params=params(1, 64), name='mlp',
        cost_estimate=pl.CostEstimate(flops=6 * rows * dim * cols, bytes_accessed=6 * dim * cols, transcendentals=rows * cols),
    )(y_rows, g, w_gate, w_up, w_down)


def scatter_kernel(h_ref, w_hbm, res_ref, out_ref, w, give, mine, got, passing, last, w_sem, give_sem, got_sem, send_sem, recv_sem):
    x, c, partner, right, left = tp_place()
    block, dim = res_ref.shape
    half = block // 2
    step = 512
    n_steps = dim // step
    loads = []
    for n in range(n_steps):
        at = slice(n * step, (n + 1) * step)
        loads.append(pltpu.make_async_copy(w_hbm.at[:, at], w.at[:, at], w_sem.at[n]))
        loads[-1].start()
    enter([partner, right, left])
    h0, h1 = slice(0, half), slice(half, block)

    def product(dx, core, dst, wait_w=False):
        start = pl.multiple_of((((x + dx) % NX) * 2 + core) * block, block)
        if wait_w:
            for load in loads:
                load.wait()

        @pl.loop(0, n_steps)
        def _(n):
            at = pl.ds(pl.multiple_of(n * step, step), step)
            dst[:, at] = jnp.dot(h_ref[pl.ds(start, block), :], w[:, at], preferred_element_type=F32).astype(BF16)

    def exchange(b, dx, wait_w=False):
        product(dx, 1 - c, give.at[b], wait_w)
        copy = pltpu.make_async_remote_copy(src_ref=give.at[b], dst_ref=got.at[b], send_sem=give_sem.at[b],
                                            recv_sem=got_sem.at[b], device_id=partner, device_id_type=MESH)
        copy.start()
        product(dx, c, mine.at[b])
        return copy

    started = []

    def send(src, dst, device):
        n = len(started)
        copy = pltpu.make_async_remote_copy(src_ref=src, dst_ref=dst, send_sem=send_sem.at[n], recv_sem=recv_sem.at[n],
                                            device_id=device, device_id_type=MESH)
        copy.start()
        started.append(copy)
        return copy

    pair = exchange(0, 2, True)
    pair.wait_recv()
    add_rows(mine.at[0], mine.at[0], got.at[0])
    pass_right = send(mine.at[0, h0], passing.at[0], right)
    pass_left = send(mine.at[0, h1], passing.at[1], left)
    pair_r = exchange(1, 1)
    pair_l = exchange(2, NX - 1)
    pair_r.wait_recv()
    add_rows(mine.at[1], mine.at[1], got.at[1])
    to_right_1 = send(mine.at[1, h1], last.at[0, h1], right)
    pair_l.wait_recv()
    add_rows(mine.at[2], mine.at[2], got.at[2])
    to_left_0 = send(mine.at[2, h0], last.at[1, h0], left)
    pair_o = exchange(3, 0)
    pass_right.wait_recv()
    add_rows(mine.at[1, h0], mine.at[1, h0], passing.at[0])
    to_right_0 = send(mine.at[1, h0], last.at[0, h0], right)
    pass_left.wait_recv()
    add_rows(mine.at[2, h1], mine.at[2, h1], passing.at[1])
    to_left_1 = send(mine.at[2, h1], last.at[1, h1], left)
    pair_o.wait_recv()
    for copy in (to_right_1, to_left_0, to_right_0, to_left_1):
        copy.wait_recv()
    finish_rows(out_ref, res_ref, [mine.at[3], got.at[3], last.at[0], last.at[1]])
    for copy in (pair, pair_r, pair_l, pair_o, *started):
        copy.wait_send()


def scatter_product(h, w, res, cid):
    rows, depth = h.shape
    block, dim = res.shape
    half = block // 2
    sem = pltpu.SemaphoreType.DMA
    return pl.pallas_call(
        scatter_kernel,
        out_shape=jax.ShapeDtypeStruct((block, dim), BF16),
        in_specs=[vmem_spec(), hbm_spec(), vmem_spec()],
        out_specs=vmem_spec(),
        scratch_shapes=[pltpu.VMEM((depth, dim), BF16)] + [pltpu.VMEM((4, block, dim), BF16)] * 3
        + [pltpu.VMEM((2, half, dim), BF16), pltpu.VMEM((2, block, dim), BF16),
           sem((max(1, dim // 512),)), sem((4,)), sem((4,)), sem((6,)), sem((6,))],
        compiler_params=params(cid, 48), name='scatter_product_%d' % cid,
        cost_estimate=pl.CostEstimate(flops=2 * rows * dim * depth, bytes_accessed=2 * dim * depth, transcendentals=0),
    )(h, w, res)


O, R, F, L = range(NX)
EARLY, LATE = range(2)


def attention_order():
    first = lambda dy, dz: ((dy, dz), EARLY)
    second = lambda dy, dz: ((dy, dz), LATE)
    plan = [
        ('near', EARLY, R), ('spread', EARLY, L), ('pass', EARLY, O), first(O, R), first(O, L), first(R, O),
        first(L, O), ('near', LATE, R), ('spread', LATE, L), ('pass', LATE, O), second(O, R), second(O, L),
        ('spread', EARLY, F), second(R, O), first(F, O), ('pass', EARLY, R), first(R, R), ('pass', LATE, R),
        second(R, R), first(R, L), ('pass', EARLY, L), second(L, O), first(L, R), ('pass', LATE, L),
        ('end', EARLY, O), first(O, F), second(R, L), ('spread', LATE, F), ('end', LATE, O), second(O, F),
        ('end', LATE, R), second(F, O), second(L, R), ('pass', EARLY, F), ('end', LATE, L), first(F, R),
        second(F, R), ('end', EARLY, R), first(R, F), first(F, L), ('end', EARLY, L), ('pass', LATE, F),
        second(R, F), ('end', EARLY, F), first(F, F), second(F, L), ('end', LATE, F), second(F, F), first(L, F),
        second(L, F), first(L, L), second(L, L),
    ]
    seq, waits = [first(O, O)], {}
    for item in plan:
        if isinstance(item[0], str):
            waits.setdefault(len(seq), []).append(item)
        else:
            seq.append(item)
    return seq, waits


def pick(index, values):
    out = index * 0 + values[0]
    for i, v in enumerate(values[1:], 1):
        if v != values[i - 1]:
            out = jnp.where(index >= i, v, out)
    return out


def attention_kernel(n_heads, q_ref, kv_ref, o_ref, m_ref, l_ref, acc_ref, buf, send_sem, recv_sem):
    piece = kv_ref.shape[2]
    me = lax.axis_index('cp')
    y, z = me % NX, me // NX
    scale = HD ** -0.5 * math.log2(math.e)
    at_y = lambda d: {'cp': z * NX + (y + d) % NX}
    at_z = lambda d: {'cp': ((z + d) % NX) * NX + y}
    enter([at_y(1), at_y(3), at_z(1), at_z(3)])
    axes = ((at_y, at_z), (at_z, at_y))

    def slot(kind, da, db):
        dy, dz = (da, db) if kind == 0 else (db, da)
        return dz * NX + dy

    started, landing = [], {}

    def copy_of(kind, src, dst, axis, d, part, n):
        source = kv_ref.at[kind] if src == (0, 0) else buf.at[kind, slot(kind, *src)]
        target = buf.at[kind, slot(kind, *dst)]
        if part is not None:
            source, target = source.at[part], target.at[part]
        return pltpu.make_async_remote_copy(
            src_ref=source, dst_ref=target, send_sem=send_sem.at[n],
            recv_sem=recv_sem.at[kind, slot(kind, *dst), part or 0],
            device_id=axes[kind][axis](d), device_id_type=MESH)

    def send(kind, src, dst, axis, d, part=None):
        key = (kind, src, dst, axis, d, part, len(started))
        copy_of(*key).start()
        started.append(key)
        landing[kind, dst, part] = key

    def landed(*key):
        copy_of(*landing[key]).wait_recv()

    def spread(kind, da):
        send(kind, (da, O), (da, L), 1, R)
        send(kind, (da, O), (da, R), 1, L)

    def act(step, kind, da):
        if step == 'near':
            landed(kind, (R, O), None)
            landed(kind, (L, O), None)
            send(kind, (L, O), (F, O), 0, R, 0)
            send(kind, (R, O), (F, O), 0, L, 1)
            spread(kind, R)
        elif step == 'spread':
            if da == F:
                for part in (0, 1):
                    landed(kind, (F, O), part)
            spread(kind, da)
        elif step == 'pass':
            landed(kind, (da, L), None)
            send(kind, (da, L), (da, F), 1, R, 0)
            landed(kind, (da, R), None)
            send(kind, (da, R), (da, F), 1, L, 1)
        else:
            for part in (0, 1):
                landed(kind, (da, F), part)

    for kind in (EARLY, LATE):
        send(kind, (O, O), (L, O), 0, R)
        send(kind, (O, O), (R, O), 0, L)
        spread(kind, O)

    m_ref[...] = jnp.full_like(m_ref, -1e30)
    l_ref[...] = jnp.zeros_like(l_ref)
    acc_ref[...] = jnp.zeros_like(acc_ref)

    def unit(q_row, k, v, masked):
        rows = pl.ds(pl.multiple_of(q_row, piece), piece)
        heads = [slice(h * HD, (h + 1) * HD) for h in range(n_heads)]

        def score(cols):
            s = lax.dot_general(q_ref[rows, cols], k, (((1,), (1,)), ((), ())), preferred_element_type=F32)
            if masked:
                row = lax.broadcasted_iota(jnp.int32, (piece, piece), 0)
                col = lax.broadcasted_iota(jnp.int32, (piece, piece), 1)
                s = jnp.where(row >= col, s, -1e30)
            return s

        def absorb(cols, s):
            m_old = m_ref[rows, cols]
            m_new = jnp.maximum(m_old, jnp.max(s, axis=1, keepdims=True) * scale)
            alpha = jnp.exp2(m_old - m_new)
            p = [jnp.exp2(s[:, i * HD:(i + 1) * HD] * scale - m_new) for i in range(piece // HD)]
            psum = p[0]
            for part in p[1:]:
                psum = psum + part
            l_ref[rows, cols] = l_ref[rows, cols] * alpha + psum
            pb = jnp.concatenate([part.astype(BF16) for part in p], axis=1)
            pv = jnp.dot(pb, v, preferred_element_type=F32)
            acc_ref[rows, cols] = acc_ref[rows, cols] * alpha + pv
            m_ref[rows, cols] = m_new

        ahead = score(heads[0])
        for cols, after in zip(heads, heads[1:] + [None]):
            s, ahead = ahead, score(after) if after else None
            absorb(cols, s)

    @pl.loop(0, 2)
    def _(kind):
        unit(kind * piece, kv_ref[kind, 0], kv_ref[kind, 1], True)

    unit(piece, kv_ref[0, 0], kv_ref[0, 1], False)
    seq, waits = attention_order()
    marks = sorted(waits) + [len(seq)]

    @pl.loop(1, len(seq))
    def _(u):
        for mark in marks[:-1]:
            @pl.when(u == mark)
            def _():
                for step in waits[mark]:
                    act(*step)

        dy = pick(u, [p[0] for p, _ in seq])
        dz = pick(u, [p[1] for p, _ in seq])
        which = pick(u, [w for _, w in seq])
        src = ((z + dz) % NX) * NX + (y + dy) % NX
        late = jnp.where(src > me, 1, 0)
        q_row = jnp.where(which == 0, 1, late) * piece
        kind = which * late
        at = dz * NX + dy
        unit(q_row, buf[kind, at, 0], buf[kind, at, 1], False)

    @pl.loop(0, 2)
    def _(part):
        rows = pl.ds(pl.multiple_of(part * piece, piece), piece)
        for h in range(n_heads):
            cols = slice(h * HD, (h + 1) * HD)
            total = jnp.sum(l_ref[rows, cols], axis=1, keepdims=True)
            o_ref[rows, cols] = (acc_ref[rows, cols] / total).astype(BF16)

    for key in started:
        copy_of(*key).wait_send()


def attention(q, kv):
    rows, width = q.shape
    piece = kv.shape[2]
    sem = pltpu.SemaphoreType.DMA
    return pl.pallas_call(
        functools.partial(attention_kernel, width // HD),
        out_shape=jax.ShapeDtypeStruct((rows, width), BF16),
        in_specs=[vmem_spec()] * 2,
        out_specs=vmem_spec(),
        scratch_shapes=[pltpu.VMEM((rows, width), F32)] * 3 + [pltpu.VMEM((2, NX * NX, 2, piece, HD), BF16),
                                                              sem((40,)), sem((2, NX * NX, 2))],
        compiler_params=params(2, 48), name='attention',
        cost_estimate=pl.CostEstimate(flops=18 * 10 ** 9, bytes_accessed=10 * 2 ** 20, transcendentals=35 * 10 ** 6),
    )(q, kv)


def solution(mesh):
    row_spec = P('dp', ('cp', 'tp'), None)
    head_cols = P(None, 'tp', None)
    cp_size = mesh.shape['cp']

    def local_layer(x, g_attn, w_q, w_k, w_v, w_o, g_mlp, w_gate, w_up, w_down):
        x_rows = x[0]
        block, dim = x_rows.shape
        rows = block * mesh.shape['tp']
        piece = rows // 2
        cp_index = lax.axis_index('cp')
        n_heads = w_q.shape[1]
        j = jnp.arange(rows, dtype=jnp.int32)
        positions = jnp.where(j < piece, cp_index * piece + j, (2 * cp_size - 1 - cp_index) * piece + j - piece)
        cos, sin = rope_tables(positions)
        in_hbm = [pltpu.with_memory_space_constraint(v, pltpu.HBM) for v in (x_rows, w_k.reshape(dim, HD), w_v.reshape(dim, HD))]
        q, kv = gather_qkv(in_hbm[0], g_attn.reshape(dim // HD, HD), cos, sin, w_q.reshape(dim, n_heads * HD), *in_hbm[1:], n_heads, piece)
        o = attention(q, kv)
        y_rows = scatter_product(o, w_o.reshape(n_heads * HD, dim), x_rows, 3)
        d_rows = mlp(y_rows, g_mlp.reshape(dim // HD, HD), w_gate, w_up, w_down)
        return (y_rows.astype(F32) + d_rows.astype(F32)).astype(BF16)[None]

    return jax.shard_map(local_layer, mesh=mesh,
                         in_specs=(row_spec, P(), head_cols, head_cols, head_cols, P('tp', None, None),
                                   P(), P(None, 'tp'), P(None, 'tp'), P('tp', None)),
                         out_specs=row_spec, check_vma=False)
```

```python
import functools
import math
import jax
import jax.numpy as jnp
from jax import lax
from jax.experimental import pallas as pl
from jax.experimental.pallas import tpu as pltpu
from jax.sharding import PartitionSpec as P

NORM_EPS = 1e-5
ROPE_THETA = 500000.0
HD = 128
NX = 4
MESH = pl.DeviceIdType.MESH
F32 = jnp.float32
BF16 = jnp.bfloat16


def params(cid, vmem_mib, **more):
    return pltpu.CompilerParams(collective_id=cid, has_side_effects=True, vmem_limit_bytes=min(vmem_mib * 2 ** 20, 67043328), **more)


def vmem_spec():
    return pl.BlockSpec(memory_space=pltpu.VMEM)


def hbm_spec():
    return pl.BlockSpec(memory_space=pltpu.HBM)


def rope_tables(positions):
    inv_freq = ROPE_THETA ** (-2.0 * jnp.arange(HD // 2, dtype=F32) / HD)
    angles = positions.astype(F32)[:, None] * inv_freq[None, :]
    c, s = jnp.cos(angles), jnp.sin(angles)
    return jnp.concatenate([c, c], axis=-1), jnp.concatenate([-s, s], axis=-1)


def enter(peers):
    barrier = pltpu.get_barrier_semaphore()
    for peer in peers:
        pl.semaphore_signal(barrier, inc=1, device_id=peer, device_id_type=MESH)
    pl.semaphore_wait(barrier, len(peers))


def tp_place():
    t = lax.axis_index('tp')
    x, c = t // 2, t % 2
    side = lambda d: {'tp': ((x + d) % NX) * 2 + c}
    return x, c, {'tp': x * 2 + 1 - c}, side(1), side(NX - 1)


OWN, MATE, LEFT, LEFT_MATE, RIGHT, RIGHT_MATE, FAR, FAR_MATE = range(8)
LO, HI = range(2)
NEAR_PART, FIRST_PART, LAST_PART, FAR_PART = range(4)
GATHER_PARTS = (((OWN, LO), (OWN, HI), (MATE, LO), (MATE, HI)),
                ((LEFT, LO), (RIGHT, HI), (LEFT_MATE, LO), (RIGHT_MATE, HI)),
                ((LEFT, HI), (RIGHT, LO), (LEFT_MATE, HI), (RIGHT_MATE, LO)),
                ((FAR, LO), (FAR, HI), (FAR_MATE, LO), (FAR_MATE, HI)))
GATHER_PLACE = {name: i for i, name in enumerate(n for part in GATHER_PARTS for n in part)}
N_PLACES = len(GATHER_PLACE)


def norm_into(x_ref, g_ref, full, rows):
    gain = jnp.concatenate([g_ref[i:i + 1, :] for i in range(g_ref.shape[0])], axis=1).astype(F32)
    step = min(16, rows)

    @pl.loop(0, rows // step)
    def _(i):
        where = pl.ds(pl.multiple_of(i * step, step), step)
        r = x_ref[where, :].astype(F32)
        mean_sq = jnp.mean(r * r, axis=-1, keepdims=True)
        full[where, :] = (r * lax.rsqrt(mean_sq + NORM_EPS) * gain).astype(BF16)


class Gather:
    def __init__(self, full, send_sem, recv_sem, half):
        self.full, self.send_sem, self.recv_sem, self.half = full, send_sem, recv_sem, half
        _, _, self.mate, self.right, self.left = tp_place()
        self.started, self.landing = [], {}

    def enter(self):
        enter([self.mate, self.right, self.left])

    def send(self, src, dst, h, device):
        rows = [pl.ds(GATHER_PLACE[slot, h] * self.half, self.half) for slot in (src, dst)]
        copy = pltpu.make_async_remote_copy(
            src_ref=self.full.at[rows[0]], dst_ref=self.full.at[rows[1]],
            send_sem=self.send_sem.at[len(self.started)], recv_sem=self.recv_sem.at[GATHER_PLACE[dst, h]],
            device_id=device, device_id_type=MESH)
        copy.start()
        self.started.append(copy)
        self.landing[dst, h] = copy

    def arrived(self, *names):
        for name in names:
            self.landing[name].wait_recv()

    def rest(self):
        self.send(OWN, LEFT, HI, self.right)
        self.send(OWN, RIGHT, LO, self.left)

    def start(self):
        self.send(OWN, LEFT, LO, self.right)
        self.send(OWN, RIGHT, HI, self.left)
        for h in (LO, HI):
            self.send(OWN, MATE, h, self.mate)

    def relay(self):
        self.arrived((LEFT, LO))
        self.send(LEFT, FAR, LO, self.right)
        self.arrived((RIGHT, HI))
        self.send(RIGHT, FAR, HI, self.left)
        self.send(LEFT, LEFT_MATE, LO, self.mate)
        self.send(RIGHT, RIGHT_MATE, HI, self.mate)

    def share_far(self):
        for h in (LO, HI):
            self.arrived((FAR, h))
            self.send(FAR, FAR_MATE, h, self.mate)

    def share_last(self):
        self.arrived((LEFT, HI))
        self.send(LEFT, LEFT_MATE, HI, self.mate)
        self.arrived((RIGHT, LO))
        self.send(RIGHT, RIGHT_MATE, LO, self.mate)

    def sent(self, *which):
        for copy in self.started:
            copy.wait_send()


def part_rows(part, block):
    t = lax.axis_index('tp')
    x, c = t // 2, t % 2
    rows = []
    for name, h in GATHER_PARTS[part]:
        dx, other = {OWN: 0, LEFT: NX - 1, RIGHT: 1, FAR: 2}[name // 2 * 2], name % 2
        core = 1 - c if other else c
        rows.append((((x + dx) % NX) * 2 + core) * block + h * (block // 2))
    return rows


N_SENDS = 14
GATHER_SEMS = [pltpu.SemaphoreType.DMA((N_SENDS,)), pltpu.SemaphoreType.DMA((N_PLACES,))]


def qkv_kernel(n_heads, x_hbm, g_ref, cos_ref, sin_ref, wq_hbm, wk_hbm, wv_hbm, q_ref, kv_ref, full, w, wq3, x_ref, send_sem, recv_sem, w_sem, x_sem):
    block = x_ref.shape[0]
    half = block // 2
    piece = kv_ref.shape[2]
    width = n_heads * HD
    loads = [pltpu.make_async_copy(wq_hbm, wq3, w_sem.at[0]),
             pltpu.make_async_copy(wk_hbm, w.at[:, width:width + HD], w_sem.at[1]),
             pltpu.make_async_copy(wv_hbm, w.at[:, width + HD:width + 2 * HD], w_sem.at[2])]

    def rotate(v, cos, sin):
        f = v.astype(BF16).astype(F32)
        return (f * cos + pltpu.roll(f, HD // 2, 1) * sin).astype(BF16)

    def keys_values(part, rows, a):
        out = jnp.dot(a, w[:, width:], preferred_element_type=F32)
        for i, r in enumerate(rows):
            here = slice(i * half, (i + 1) * half)
            where = pl.ds(pl.multiple_of(r % piece, half), half)
            kv_ref[r // piece, 0, where, :] = rotate(out[here, :HD], cos_ref[pl.ds(r, half), :], sin_ref[pl.ds(r, half), :])
            kv_ref[r // piece, 1, where, :] = out[here, HD:].astype(BF16)

    def queries(part, rows, a):
        for start in range(0, width, 2 * HD):
            out = jnp.dot(a, w[:, start:start + 2 * HD], preferred_element_type=F32)
            for i, r in enumerate(rows):
                here = slice(i * half, (i + 1) * half)
                cos, sin = cos_ref[pl.ds(r, half), :], sin_ref[pl.ds(r, half), :]
                for k in (0, HD):
                    q_ref[pl.ds(r, half), start + k:start + k + HD] = rotate(out[here, k:k + HD], cos, sin)

    def compute(part):
        rows = [pl.multiple_of(r, half) for r in part_rows(part, block)]
        n = len(rows) * half
        a = full[part * n:(part + 1) * n, :]
        keys_values(part, rows, a)
        queries(part, rows, a)

    gather = Gather(full, send_sem, recv_sem, half)
    fetch = pltpu.make_async_copy(x_hbm, x_ref, x_sem)
    fetch.start()
    for load in loads:
        load.start()
    gather.enter()
    fetch.wait()
    norm_into(x_ref, g_ref, full, block)
    gather.start()
    gather.rest()
    gather.arrived((MATE, LO), (MATE, HI))
    for load in loads:
        load.wait()
    some = min(256, w.shape[0])

    @pl.loop(0, w.shape[0] // some)
    def _(i):
        at = pl.ds(pl.multiple_of(i * some, some), some)
        w[at, 0:width] = wq3[at].reshape(some, width)

    compute(NEAR_PART)
    gather.relay()
    gather.arrived((LEFT_MATE, LO), (RIGHT_MATE, HI))
    compute(FIRST_PART)
    gather.share_last()
    gather.arrived((LEFT_MATE, HI), (RIGHT_MATE, LO))
    compute(LAST_PART)
    gather.share_far()
    gather.arrived((FAR_MATE, LO), (FAR_MATE, HI))
    compute(FAR_PART)
    gather.sent()


def gather_qkv(x_rows, g, cos, sin, w_q, w_k, w_v, n_heads, piece):
    block, dim = x_rows.shape
    rows = 2 * NX * block
    width = n_heads * HD
    return pl.pallas_call(
        functools.partial(qkv_kernel, n_heads),
        out_shape=(jax.ShapeDtypeStruct((rows, width), BF16), jax.ShapeDtypeStruct((2, 2, piece, HD), BF16)),
        in_specs=[hbm_spec()] + [vmem_spec()] * 3 + [hbm_spec()] * 3,
        out_specs=(vmem_spec(), vmem_spec()),
        scratch_shapes=[pltpu.VMEM((rows, dim), BF16), pltpu.VMEM((dim, width + 2 * HD), BF16), pltpu.VMEM((dim, n_heads, HD), BF16),
                        pltpu.VMEM((block, dim), BF16)]
        + GATHER_SEMS + [pltpu.SemaphoreType.DMA((3,)), pltpu.SemaphoreType.DMA],
        compiler_params=params(0, 48), name='gather_qkv',
        cost_estimate=pl.CostEstimate(flops=2 * rows * dim * (width + 2 * HD), bytes_accessed=2 * dim * (width + 2 * HD), transcendentals=0),
    )(x_rows, g, cos, sin, w_q, w_k, w_v)


def add_rows(dst, a, b):
    step = min(16, dst.shape[0])

    @pl.loop(0, dst.shape[0] // step)
    def _(i):
        at = pl.ds(pl.multiple_of(i * step, step), step)
        dst[at, :] = (a[at, :].astype(F32) + b[at, :].astype(F32)).astype(BF16)


def finish_rows(out, res, parts):
    step = min(16, out.shape[0])

    @pl.loop(0, out.shape[0] // step)
    def _(i):
        at = pl.ds(pl.multiple_of(i * step, step), step)
        total = parts[0][at, :].astype(F32)
        for part in parts[1:]:
            total = total + part[at, :].astype(F32)
        total = total.astype(BF16)
        out[at, :] = total if res is None else (res[at, :].astype(F32) + total.astype(F32)).astype(BF16)


def mlp_kernel(y_hbm, g_ref, wg_hbm, wu_hbm, wd_hbm, sum_ref, full, wg, wu, wd, hid, give, got, passing, last,
               send_sem, recv_sem, w_sem, d_sem, mate_sems, row_sems, io_sem):
    block, dim = y_hbm.shape
    half = block // 2
    cols = wg.shape[1]
    step = 256
    n_steps = cols // step
    loads = []
    for n in range(n_steps):
        at = slice(n * step, (n + 1) * step)
        loads.append((pltpu.make_async_copy(wg_hbm.at[:, at], wg.at[:, at], w_sem.at[0, n]),
                      pltpu.make_async_copy(wu_hbm.at[:, at], wu.at[:, at], w_sem.at[1, n])))
    load_d = pltpu.make_async_copy(wd_hbm, wd, d_sem)
    gather = Gather(full, send_sem, recv_sem, half)
    n_rows = 2 * block
    head, tail = slice(0, half), slice(half, block)

    def gate_up(part, lo, hi):
        def tile(n):
            at = pl.ds(pl.multiple_of(n * step, step), step)
            a = full[part * n_rows:(part + 1) * n_rows, :]
            gate = jnp.dot(a, wg[:, at], preferred_element_type=F32)
            up = jnp.dot(a, wu[:, at], preferred_element_type=F32)
            hid[part, :, at] = (jax.nn.silu(gate) * up).astype(BF16)

        @pl.loop(0, (hi - lo) // 2)
        def _(i):
            tile(lo + 2 * i)
            tile(lo + 2 * i + 1)

        if (hi - lo) % 2:
            tile(hi - 1)

    def down(part, first, *dst):
        wide = min(1024, dim)

        @pl.loop(0, dim // wide)
        def _(n):
            at = pl.ds(pl.multiple_of(n * wide, wide), wide)
            a = hid[part, first * block:(first + len(dst)) * block, :]
            out = jnp.dot(a, wd[:, at], preferred_element_type=F32).astype(BF16)
            for i, d in enumerate(dst):
                d[:, at] = out[i * block:(i + 1) * block, :]

    kept = {FAR_PART: full.at[block:n_rows], FIRST_PART: full.at[2 * n_rows - block:2 * n_rows],
            LAST_PART: full.at[n_rows:n_rows + block], NEAR_PART: full.at[0:block]}
    traded, moved = {}, []

    def trade(part, buffer):
        if part == FAR_PART:
            down(part, 1, give.at[buffer])
        else:
            down(part, 0, kept[part], give.at[buffer])
        traded[part] = pltpu.make_async_remote_copy(
            src_ref=give.at[buffer], dst_ref=got.at[part], send_sem=mate_sems.at[0, part], recv_sem=mate_sems.at[1, part],
            device_id=gather.mate, device_id_type=MESH)
        traded[part].start()

    def join(part):
        traded[part].wait_recv()
        add_rows(kept[part], kept[part], got.at[part])

    def move(src, dst, device):
        copy = pltpu.make_async_remote_copy(src_ref=src, dst_ref=dst, send_sem=row_sems.at[0, len(moved)],
                                            recv_sem=row_sems.at[1, len(moved)], device_id=device, device_id_type=MESH)
        copy.start()
        moved.append(copy)
        return copy

    fetch = pltpu.make_async_copy(y_hbm, give.at[0], io_sem)
    fetch.start()
    for pair in loads:
        for load in pair:
            load.start()
    load_d.start()
    gather.enter()
    fetch.wait()
    norm_into(give.at[0], g_ref, full, block)
    gather.start()
    gather.arrived((MATE, LO), (MATE, HI))
    split = (n_steps + 1) // 2
    for lo, hi in ((0, split), (split, n_steps)):
        for pair in loads[lo:hi]:
            for load in pair:
                load.wait()
        gate_up(NEAR_PART, lo, hi)
        if lo == 0:
            gather.relay()
            gather.rest()
    gather.arrived((LEFT_MATE, LO), (RIGHT_MATE, HI))
    gate_up(FIRST_PART, 0, n_steps)
    load_d.wait()
    trade(FIRST_PART, 1)
    gather.share_far()
    join(FIRST_PART)
    moved_first = [move(kept[FIRST_PART].at[head], last.at[1, head], gather.left),
                   move(kept[FIRST_PART].at[tail], last.at[0, tail], gather.right)]
    gather.arrived((FAR_MATE, LO), (FAR_MATE, HI))
    gate_up(FAR_PART, 0, n_steps)
    trade(FAR_PART, 0)
    down(FAR_PART, 0, kept[FAR_PART])
    gather.share_last()
    join(FAR_PART)
    pass_right = move(kept[FAR_PART].at[head], passing.at[0], gather.right)
    pass_left = move(kept[FAR_PART].at[tail], passing.at[1], gather.left)
    gather.arrived((LEFT_MATE, HI), (RIGHT_MATE, LO))
    gather.sent()
    gate_up(LAST_PART, 0, n_steps)
    traded[FAR_PART].wait_send()
    trade(LAST_PART, 0)
    traded[FIRST_PART].wait_send()
    trade(NEAR_PART, 1)
    join(LAST_PART)
    pass_left.wait_recv()
    add_rows(kept[LAST_PART].at[head], kept[LAST_PART].at[head], passing.at[1])
    pass_right.wait_recv()
    add_rows(kept[LAST_PART].at[tail], kept[LAST_PART].at[tail], passing.at[0])
    moved_last = [move(kept[LAST_PART].at[head], last.at[1, tail], gather.left),
                  move(kept[LAST_PART].at[tail], last.at[0, head], gather.right)]
    traded[LAST_PART].wait_send()
    traded[NEAR_PART].wait_recv()
    for copy in moved_first + moved_last:
        copy.wait_recv()
    finish_rows(sum_ref, None, [kept[NEAR_PART], got.at[NEAR_PART], last.at[0], last.at[1]])
    traded[NEAR_PART].wait_send()
    for copy in moved:
        copy.wait_send()


def mlp(y_rows, g, w_gate, w_up, w_down):
    block, dim = y_rows.shape
    rows = 2 * NX * block
    cols = w_gate.shape[1]
    sem = pltpu.SemaphoreType.DMA
    buffer = lambda *shape: pltpu.VMEM(shape, BF16)
    return pl.pallas_call(
        mlp_kernel,
        out_shape=jax.ShapeDtypeStruct((block, dim), BF16),
        in_specs=[hbm_spec(), vmem_spec()] + [hbm_spec()] * 3,
        out_specs=vmem_spec(),
        scratch_shapes=[buffer(rows, dim), buffer(dim, cols), buffer(dim, cols), buffer(cols, dim), buffer(NX, 2 * block, cols),
                        buffer(2, block, dim), buffer(NX, block, dim), buffer(2, block // 2, dim), buffer(2, block, dim)]
        + GATHER_SEMS + [sem((2, cols // 256)), sem, sem((2, NX)), sem((2, 6)), sem],
        compiler_params=params(1, 64), name='mlp',
        cost_estimate=pl.CostEstimate(flops=6 * rows * dim * cols, bytes_accessed=6 * dim * cols, transcendentals=rows * cols),
    )(y_rows, g, w_gate, w_up, w_down)


def scatter_kernel(h_ref, w_hbm, res_ref, out_ref, w, give, mine, got, passing, last, w_sem, give_sem, got_sem, send_sem, recv_sem):
    x, c, partner, right, left = tp_place()
    block, dim = res_ref.shape
    half = block // 2
    step = 512
    n_steps = dim // step
    loads = []
    for n in range(n_steps):
        at = slice(n * step, (n + 1) * step)
        loads.append(pltpu.make_async_copy(w_hbm.at[:, at], w.at[:, at], w_sem.at[n]))
        loads[-1].start()
    enter([partner, right, left])
    h0, h1 = slice(0, half), slice(half, block)

    def product(dx, core, dst, wait_w=False):
        start = pl.multiple_of((((x + dx) % NX) * 2 + core) * block, block)
        if wait_w:
            for load in loads:
                load.wait()

        @pl.loop(0, n_steps)
        def _(n):
            at = pl.ds(pl.multiple_of(n * step, step), step)
            dst[:, at] = jnp.dot(h_ref[pl.ds(start, block), :], w[:, at], preferred_element_type=F32).astype(BF16)

    def exchange(b, dx, wait_w=False):
        product(dx, 1 - c, give.at[b], wait_w)
        copy = pltpu.make_async_remote_copy(src_ref=give.at[b], dst_ref=got.at[b], send_sem=give_sem.at[b],
                                            recv_sem=got_sem.at[b], device_id=partner, device_id_type=MESH)
        copy.start()
        product(dx, c, mine.at[b])
        return copy

    started = []

    def send(src, dst, device):
        n = len(started)
        copy = pltpu.make_async_remote_copy(src_ref=src, dst_ref=dst, send_sem=send_sem.at[n], recv_sem=recv_sem.at[n],
                                            device_id=device, device_id_type=MESH)
        copy.start()
        started.append(copy)
        return copy

    pair = exchange(0, 2, True)
    pair.wait_recv()
    add_rows(mine.at[0], mine.at[0], got.at[0])
    pass_right = send(mine.at[0, h0], passing.at[0], right)
    pass_left = send(mine.at[0, h1], passing.at[1], left)
    pair_r = exchange(1, 1)
    pair_l = exchange(2, NX - 1)
    pair_r.wait_recv()
    add_rows(mine.at[1], mine.at[1], got.at[1])
    to_right_1 = send(mine.at[1, h1], last.at[0, h1], right)
    pair_l.wait_recv()
    add_rows(mine.at[2], mine.at[2], got.at[2])
    to_left_0 = send(mine.at[2, h0], last.at[1, h0], left)
    pair_o = exchange(3, 0)
    pass_right.wait_recv()
    add_rows(mine.at[1, h0], mine.at[1, h0], passing.at[0])
    to_right_0 = send(mine.at[1, h0], last.at[0, h0], right)
    pass_left.wait_recv()
    add_rows(mine.at[2, h1], mine.at[2, h1], passing.at[1])
    to_left_1 = send(mine.at[2, h1], last.at[1, h1], left)
    pair_o.wait_recv()
    for copy in (to_right_1, to_left_0, to_right_0, to_left_1):
        copy.wait_recv()
    finish_rows(out_ref, res_ref, [mine.at[3], got.at[3], last.at[0], last.at[1]])
    for copy in (pair, pair_r, pair_l, pair_o, *started):
        copy.wait_send()


def scatter_product(h, w, res, cid):
    rows, depth = h.shape
    block, dim = res.shape
    half = block // 2
    sem = pltpu.SemaphoreType.DMA
    return pl.pallas_call(
        scatter_kernel,
        out_shape=jax.ShapeDtypeStruct((block, dim), BF16),
        in_specs=[vmem_spec(), hbm_spec(), vmem_spec()],
        out_specs=vmem_spec(),
        scratch_shapes=[pltpu.VMEM((depth, dim), BF16)] + [pltpu.VMEM((4, block, dim), BF16)] * 3
        + [pltpu.VMEM((2, half, dim), BF16), pltpu.VMEM((2, block, dim), BF16),
           sem((max(1, dim // 512),)), sem((4,)), sem((4,)), sem((6,)), sem((6,))],
        compiler_params=params(cid, 48), name='scatter_product_%d' % cid,
        cost_estimate=pl.CostEstimate(flops=2 * rows * dim * depth, bytes_accessed=2 * dim * depth, transcendentals=0),
    )(h, w, res)


O, R, F, L = range(NX)
EARLY, LATE = range(2)


def attention_order():
    first = lambda dy, dz: ((dy, dz), EARLY)
    second = lambda dy, dz: ((dy, dz), LATE)
    plan = [
        ('near', EARLY, R), ('spread', EARLY, L), ('pass', EARLY, O), first(O, R), first(O, L), first(R, O),
        first(L, O), ('near', LATE, R), ('spread', LATE, L), ('pass', LATE, O), second(O, R), second(O, L),
        ('spread', EARLY, F), second(R, O), first(F, O), ('pass', EARLY, R), first(R, R), ('pass', LATE, R),
        second(R, R), first(R, L), ('pass', EARLY, L), second(L, O), first(L, R), ('pass', LATE, L),
        ('end', EARLY, O), first(O, F), second(R, L), ('spread', LATE, F), ('end', LATE, O), second(O, F),
        ('end', LATE, R), second(F, O), second(L, R), ('pass', EARLY, F), ('end', LATE, L), first(F, R),
        second(F, R), ('end', EARLY, R), first(R, F), first(F, L), ('end', EARLY, L), ('pass', LATE, F),
        second(R, F), ('end', EARLY, F), first(F, F), second(F, L), ('end', LATE, F), second(F, F), first(L, F),
        second(L, F), first(L, L), second(L, L),
    ]
    seq, waits = [first(O, O)], {}
    for item in plan:
        if isinstance(item[0], str):
            waits.setdefault(len(seq), []).append(item)
        else:
            seq.append(item)
    return seq, waits


def pick(index, values):
    out = index * 0 + values[0]
    for i, v in enumerate(values[1:], 1):
        if v != values[i - 1]:
            out = jnp.where(index >= i, v, out)
    return out


def attention_kernel(n_heads, q_ref, kv_ref, o_ref, m_ref, l_ref, acc_ref, buf, send_sem, recv_sem):
    piece = kv_ref.shape[2]
    me = lax.axis_index('cp')
    y, z = me % NX, me // NX
    scale = HD ** -0.5 * math.log2(math.e)
    at_y = lambda d: {'cp': z * NX + (y + d) % NX}
    at_z = lambda d: {'cp': ((z + d) % NX) * NX + y}
    enter([at_y(1), at_y(3), at_z(1), at_z(3)])
    axes = ((at_y, at_z), (at_z, at_y))

    def slot(kind, da, db):
        dy, dz = (da, db) if kind == 0 else (db, da)
        return dz * NX + dy

    started, landing = [], {}

    def copy_of(kind, src, dst, axis, d, part, n):
        source = kv_ref.at[kind] if src == (0, 0) else buf.at[kind, slot(kind, *src)]
        target = buf.at[kind, slot(kind, *dst)]
        if part is not None:
            source, target = source.at[part], target.at[part]
        return pltpu.make_async_remote_copy(
            src_ref=source, dst_ref=target, send_sem=send_sem.at[n],
            recv_sem=recv_sem.at[kind, slot(kind, *dst), part or 0],
            device_id=axes[kind][axis](d), device_id_type=MESH)

    def send(kind, src, dst, axis, d, part=None):
        key = (kind, src, dst, axis, d, part, len(started))
        copy_of(*key).start()
        started.append(key)
        landing[kind, dst, part] = key

    def landed(*key):
        copy_of(*landing[key]).wait_recv()

    def spread(kind, da):
        send(kind, (da, O), (da, L), 1, R)
        send(kind, (da, O), (da, R), 1, L)

    def act(step, kind, da):
        if step == 'near':
            landed(kind, (R, O), None)
            landed(kind, (L, O), None)
            send(kind, (L, O), (F, O), 0, R, 0)
            send(kind, (R, O), (F, O), 0, L, 1)
            spread(kind, R)
        elif step == 'spread':
            if da == F:
                for part in (0, 1):
                    landed(kind, (F, O), part)
            spread(kind, da)
        elif step == 'pass':
            landed(kind, (da, L), None)
            send(kind, (da, L), (da, F), 1, R, 0)
            landed(kind, (da, R), None)
            send(kind, (da, R), (da, F), 1, L, 1)
        else:
            for part in (0, 1):
                landed(kind, (da, F), part)

    for kind in (EARLY, LATE):
        send(kind, (O, O), (L, O), 0, R)
        send(kind, (O, O), (R, O), 0, L)
        spread(kind, O)

    m_ref[...] = jnp.full_like(m_ref, -1e30)
    l_ref[...] = jnp.zeros_like(l_ref)
    acc_ref[...] = jnp.zeros_like(acc_ref)

    def unit(q_row, k, v, masked):
        rows = pl.ds(pl.multiple_of(q_row, piece), piece)
        heads = [slice(h * HD, (h + 1) * HD) for h in range(n_heads)]

        def score(cols):
            s = lax.dot_general(q_ref[rows, cols], k, (((1,), (1,)), ((), ())), preferred_element_type=F32)
            if masked:
                row = lax.broadcasted_iota(jnp.int32, (piece, piece), 0)
                col = lax.broadcasted_iota(jnp.int32, (piece, piece), 1)
                s = jnp.where(row >= col, s, -1e30)
            return s

        def absorb(cols, s):
            m_old = m_ref[rows, cols]
            m_new = jnp.maximum(m_old, jnp.max(s, axis=1, keepdims=True) * scale)
            alpha = jnp.exp2(m_old - m_new)
            p = [jnp.exp2(s[:, i * HD:(i + 1) * HD] * scale - m_new) for i in range(piece // HD)]
            psum = p[0]
            for part in p[1:]:
                psum = psum + part
            l_ref[rows, cols] = l_ref[rows, cols] * alpha + psum
            pb = jnp.concatenate([part.astype(BF16) for part in p], axis=1)
            pv = jnp.dot(pb, v, preferred_element_type=F32)
            acc_ref[rows, cols] = acc_ref[rows, cols] * alpha + pv
            m_ref[rows, cols] = m_new

        ahead = score(heads[0])
        for cols, after in zip(heads, heads[1:] + [None]):
            s, ahead = ahead, score(after) if after else None
            absorb(cols, s)

    @pl.loop(0, 2)
    def _(kind):
        unit(kind * piece, kv_ref[kind, 0], kv_ref[kind, 1], True)

    unit(piece, kv_ref[0, 0], kv_ref[0, 1], False)
    seq, waits = attention_order()
    marks = sorted(waits) + [len(seq)]

    @pl.loop(1, len(seq))
    def _(u):
        for mark in marks[:-1]:
            @pl.when(u == mark)
            def _():
                for step in waits[mark]:
                    act(*step)

        dy = pick(u, [p[0] for p, _ in seq])
        dz = pick(u, [p[1] for p, _ in seq])
        which = pick(u, [w for _, w in seq])
        src = ((z + dz) % NX) * NX + (y + dy) % NX
        late = jnp.where(src > me, 1, 0)
        q_row = jnp.where(which == 0, 1, late) * piece
        kind = which * late
        at = dz * NX + dy
        unit(q_row, buf[kind, at, 0], buf[kind, at, 1], False)

    @pl.loop(0, 2)
    def _(part):
        rows = pl.ds(pl.multiple_of(part * piece, piece), piece)
        for h in range(n_heads):
            cols = slice(h * HD, (h + 1) * HD)
            total = jnp.sum(l_ref[rows, cols], axis=1, keepdims=True)
            o_ref[rows, cols] = (acc_ref[rows, cols] / total).astype(BF16)

    for key in started:
        copy_of(*key).wait_send()


def attention(q, kv):
    rows, width = q.shape
    piece = kv.shape[2]
    sem = pltpu.SemaphoreType.DMA
    return pl.pallas_call(
        functools.partial(attention_kernel, width // HD),
        out_shape=jax.ShapeDtypeStruct((rows, width), BF16),
        in_specs=[vmem_spec()] * 2,
        out_specs=vmem_spec(),
        scratch_shapes=[pltpu.VMEM((rows, width), F32)] * 3 + [pltpu.VMEM((2, NX * NX, 2, piece, HD), BF16),
                                                              sem((40,)), sem((2, NX * NX, 2))],
        compiler_params=params(2, 48), name='attention',
        cost_estimate=pl.CostEstimate(flops=18 * 10 ** 9, bytes_accessed=10 * 2 ** 20, transcendentals=35 * 10 ** 6),
    )(q, kv)


def solution(mesh):
    row_spec = P('dp', ('cp', 'tp'), None)
    head_cols = P(None, 'tp', None)
    cp_size = mesh.shape['cp']

    def local_layer(x, g_attn, w_q, w_k, w_v, w_o, g_mlp, w_gate, w_up, w_down):
        x_rows = x[0]
        block, dim = x_rows.shape
        rows = block * mesh.shape['tp']
        piece = rows // 2
        cp_index = lax.axis_index('cp')
        n_heads = w_q.shape[1]
        j = jnp.arange(rows, dtype=jnp.int32)
        positions = jnp.where(j < piece, cp_index * piece + j, (2 * cp_size - 1 - cp_index) * piece + j - piece)
        cos, sin = rope_tables(positions)
        in_hbm = [pltpu.with_memory_space_constraint(v, pltpu.HBM) for v in (x_rows, w_q, w_k.reshape(dim, HD), w_v.reshape(dim, HD))]
        q, kv = gather_qkv(in_hbm[0], g_attn.reshape(dim // HD, HD), cos, sin, *in_hbm[1:], n_heads, piece)
        o = attention(q, kv)
        y_rows = scatter_product(o, w_o.reshape(n_heads * HD, dim), x_rows, 3)
        d_rows = mlp(y_rows, g_mlp.reshape(dim // HD, HD), w_gate, w_up, w_down)
        return (y_rows.astype(F32) + d_rows.astype(F32)).astype(BF16)[None]

    return jax.shard_map(local_layer, mesh=mesh,
                         in_specs=(row_spec, P(), head_cols, head_cols, head_cols, P('tp', None, None),
                                   P(), P(None, 'tp'), P(None, 'tp'), P('tp', None)),
                         out_specs=row_spec, check_vma=False)
```

```python
import functools
import math
import jax
import jax.numpy as jnp
from jax import lax
from jax.experimental import pallas as pl
from jax.experimental.pallas import tpu as pltpu
from jax.sharding import PartitionSpec as P

NORM_EPS = 1e-5
ROPE_THETA = 500000.0
HD = 128
NX = 4
MESH = pl.DeviceIdType.MESH
F32 = jnp.float32
BF16 = jnp.bfloat16


def params(cid, vmem_mib, **more):
    return pltpu.CompilerParams(collective_id=cid, has_side_effects=True, vmem_limit_bytes=min(vmem_mib * 2 ** 20, 67043328), **more)


def vmem_spec():
    return pl.BlockSpec(memory_space=pltpu.VMEM)


def hbm_spec():
    return pl.BlockSpec(memory_space=pltpu.HBM)


def rope_tables(positions):
    inv_freq = ROPE_THETA ** (-2.0 * jnp.arange(HD // 2, dtype=F32) / HD)
    angles = positions.astype(F32)[:, None] * inv_freq[None, :]
    c, s = jnp.cos(angles), jnp.sin(angles)
    return jnp.concatenate([c, c], axis=-1), jnp.concatenate([-s, s], axis=-1)


def enter(peers):
    barrier = pltpu.get_barrier_semaphore()
    for peer in peers:
        pl.semaphore_signal(barrier, inc=1, device_id=peer, device_id_type=MESH)
    pl.semaphore_wait(barrier, len(peers))


def tp_place():
    t = lax.axis_index('tp')
    x, c = t // 2, t % 2
    side = lambda d: {'tp': ((x + d) % NX) * 2 + c}
    return x, c, {'tp': x * 2 + 1 - c}, side(1), side(NX - 1)


OWN, MATE, LEFT, LEFT_MATE, RIGHT, RIGHT_MATE, FAR, FAR_MATE = range(8)
LO, HI = range(2)
NEAR_PART, FIRST_PART, LAST_PART, FAR_PART = range(4)
GATHER_PARTS = (((OWN, LO), (OWN, HI), (MATE, LO), (MATE, HI)),
                ((LEFT, LO), (RIGHT, HI), (LEFT_MATE, LO), (RIGHT_MATE, HI)),
                ((LEFT, HI), (RIGHT, LO), (LEFT_MATE, HI), (RIGHT_MATE, LO)),
                ((FAR, LO), (FAR, HI), (FAR_MATE, LO), (FAR_MATE, HI)))
GATHER_PLACE = {name: i for i, name in enumerate(n for part in GATHER_PARTS for n in part)}
N_PLACES = len(GATHER_PLACE)


def norm_into(x_ref, g_ref, full, rows):
    gain = jnp.concatenate([g_ref[i:i + 1, :] for i in range(g_ref.shape[0])], axis=1).astype(F32)
    step = min(16, rows)

    @pl.loop(0, rows // step)
    def _(i):
        where = pl.ds(pl.multiple_of(i * step, step), step)
        r = x_ref[where, :].astype(F32)
        mean_sq = jnp.mean(r * r, axis=-1, keepdims=True)
        full[where, :] = (r * lax.rsqrt(mean_sq + NORM_EPS) * gain).astype(BF16)


class Gather:
    def __init__(self, full, send_sem, recv_sem, half):
        self.full, self.send_sem, self.recv_sem, self.half = full, send_sem, recv_sem, half
        _, _, self.mate, self.right, self.left = tp_place()
        self.started, self.landing = [], {}

    def enter(self):
        enter([self.mate, self.right, self.left])

    def send(self, src, dst, h, device):
        rows = [pl.ds(GATHER_PLACE[slot, h] * self.half, self.half) for slot in (src, dst)]
        copy = pltpu.make_async_remote_copy(
            src_ref=self.full.at[rows[0]], dst_ref=self.full.at[rows[1]],
            send_sem=self.send_sem.at[len(self.started)], recv_sem=self.recv_sem.at[GATHER_PLACE[dst, h]],
            device_id=device, device_id_type=MESH)
        copy.start()
        self.started.append(copy)
        self.landing[dst, h] = copy

    def arrived(self, *names):
        for name in names:
            self.landing[name].wait_recv()

    def rest(self):
        self.send(OWN, LEFT, HI, self.right)
        self.send(OWN, RIGHT, LO, self.left)

    def start(self):
        self.send(OWN, LEFT, LO, self.right)
        self.send(OWN, RIGHT, HI, self.left)
        for h in (LO, HI):
            self.send(OWN, MATE, h, self.mate)

    def relay(self):
        self.arrived((LEFT, LO))
        self.send(LEFT, FAR, LO, self.right)
        self.arrived((RIGHT, HI))
        self.send(RIGHT, FAR, HI, self.left)
        self.send(LEFT, LEFT_MATE, LO, self.mate)
        self.send(RIGHT, RIGHT_MATE, HI, self.mate)

    def share_far(self):
        for h in (LO, HI):
            self.arrived((FAR, h))
            self.send(FAR, FAR_MATE, h, self.mate)

    def share_last(self):
        self.arrived((LEFT, HI))
        self.send(LEFT, LEFT_MATE, HI, self.mate)
        self.arrived((RIGHT, LO))
        self.send(RIGHT, RIGHT_MATE, LO, self.mate)

    def sent(self, *which):
        for copy in self.started:
            copy.wait_send()


def part_rows(part, block):
    t = lax.axis_index('tp')
    x, c = t // 2, t % 2
    rows = []
    for name, h in GATHER_PARTS[part]:
        dx, other = {OWN: 0, LEFT: NX - 1, RIGHT: 1, FAR: 2}[name // 2 * 2], name % 2
        core = 1 - c if other else c
        rows.append((((x + dx) % NX) * 2 + core) * block + h * (block // 2))
    return rows


N_SENDS = 14
GATHER_SEMS = [pltpu.SemaphoreType.DMA((N_SENDS,)), pltpu.SemaphoreType.DMA((N_PLACES,))]


def qkv_kernel(n_heads, x_hbm, g_ref, cos_ref, sin_ref, wq_hbm, wk_hbm, wv_hbm, q_ref, kv_ref, full, w, wq3, x_ref, send_sem, recv_sem, w_sem, x_sem):
    block = x_ref.shape[0]
    half = block // 2
    piece = kv_ref.shape[2]
    width = n_heads * HD
    loads = [pltpu.make_async_copy(wq_hbm, wq3, w_sem.at[0]),
             pltpu.make_async_copy(wk_hbm, w.at[:, width:width + HD], w_sem.at[1]),
             pltpu.make_async_copy(wv_hbm, w.at[:, width + HD:width + 2 * HD], w_sem.at[2])]

    def rotate(v, cos, sin):
        f = v.astype(BF16).astype(F32)
        return (f * cos + pltpu.roll(f, HD // 2, 1) * sin).astype(BF16)

    def keys_values(part, rows, a):
        out = jnp.dot(a, w[:, width:], preferred_element_type=F32)
        for i, r in enumerate(rows):
            here = slice(i * half, (i + 1) * half)
            where = pl.ds(pl.multiple_of(r % piece, half), half)
            kv_ref[r // piece, 0, where, :] = rotate(out[here, :HD], cos_ref[pl.ds(r, half), :], sin_ref[pl.ds(r, half), :])
            kv_ref[r // piece, 1, where, :] = out[here, HD:].astype(BF16)

    def queries(part, rows, a):
        for start in range(0, width, 2 * HD):
            out = jnp.dot(a, w[:, start:start + 2 * HD], preferred_element_type=F32)
            for i, r in enumerate(rows):
                here = slice(i * half, (i + 1) * half)
                cos, sin = cos_ref[pl.ds(r, half), :], sin_ref[pl.ds(r, half), :]
                for k in (0, HD):
                    q_ref[pl.ds(r, half), start + k:start + k + HD] = rotate(out[here, k:k + HD], cos, sin)

    def compute(part):
        rows = [pl.multiple_of(r, half) for r in part_rows(part, block)]
        n = len(rows) * half
        a = full[part * n:(part + 1) * n, :]
        keys_values(part, rows, a)
        queries(part, rows, a)

    gather = Gather(full, send_sem, recv_sem, half)
    fetch = pltpu.make_async_copy(x_hbm, x_ref, x_sem)
    fetch.start()
    for load in loads:
        load.start()
    gather.enter()
    fetch.wait()
    norm_into(x_ref, g_ref, full, block)
    gather.start()
    gather.rest()
    gather.arrived((MATE, LO), (MATE, HI))
    for load in loads:
        load.wait()
    some = min(256, w.shape[0])

    @pl.loop(0, w.shape[0] // some)
    def _(i):
        at = pl.ds(pl.multiple_of(i * some, some), some)
        w[at, 0:width] = wq3[at].reshape(some, width)

    compute(NEAR_PART)
    gather.relay()
    gather.arrived((LEFT_MATE, LO), (RIGHT_MATE, HI))
    compute(FIRST_PART)
    gather.share_last()
    gather.arrived((LEFT_MATE, HI), (RIGHT_MATE, LO))
    compute(LAST_PART)
    gather.share_far()
    gather.arrived((FAR_MATE, LO), (FAR_MATE, HI))
    compute(FAR_PART)
    gather.sent()


def gather_qkv(x_rows, g, cos, sin, w_q, w_k, w_v, n_heads, piece):
    block, dim = x_rows.shape
    rows = 2 * NX * block
    width = n_heads * HD
    return pl.pallas_call(
        functools.partial(qkv_kernel, n_heads),
        out_shape=(jax.ShapeDtypeStruct((rows, width), BF16), jax.ShapeDtypeStruct((2, 2, piece, HD), BF16)),
        in_specs=[hbm_spec()] + [vmem_spec()] * 3 + [hbm_spec()] * 3,
        out_specs=(vmem_spec(), vmem_spec()),
        scratch_shapes=[pltpu.VMEM((rows, dim), BF16), pltpu.VMEM((dim, width + 2 * HD), BF16), pltpu.VMEM((dim, n_heads, HD), BF16),
                        pltpu.VMEM((block, dim), BF16)]
        + GATHER_SEMS + [pltpu.SemaphoreType.DMA((3,)), pltpu.SemaphoreType.DMA],
        compiler_params=params(0, 48), name='gather_qkv',
        cost_estimate=pl.CostEstimate(flops=2 * rows * dim * (width + 2 * HD), bytes_accessed=2 * dim * (width + 2 * HD), transcendentals=0),
    )(x_rows, g, cos, sin, w_q, w_k, w_v)


def add_rows(dst, a, b):
    step = min(16, dst.shape[0])

    @pl.loop(0, dst.shape[0] // step)
    def _(i):
        at = pl.ds(pl.multiple_of(i * step, step), step)
        dst[at, :] = (a[at, :].astype(F32) + b[at, :].astype(F32)).astype(BF16)


def finish_rows(out, res, parts):
    step = min(16, out.shape[0])

    @pl.loop(0, out.shape[0] // step)
    def _(i):
        at = pl.ds(pl.multiple_of(i * step, step), step)
        total = parts[0][at, :].astype(F32)
        for part in parts[1:]:
            total = total + part[at, :].astype(F32)
        total = total.astype(BF16)
        out[at, :] = total if res is None else (res[at, :].astype(F32) + total.astype(F32)).astype(BF16)


def mlp_kernel(y_hbm, g_ref, wg_hbm, wu_hbm, wd_hbm, sum_ref, full, wg, wu, wd, hid, give, got, passing, last,
               send_sem, recv_sem, w_sem, d_sem, mate_sems, row_sems, io_sem):
    block, dim = y_hbm.shape
    half = block // 2
    cols = wg.shape[1]
    step = 256
    n_steps = cols // step

    def loads(n):
        at = pl.ds(pl.multiple_of(n * step, step), step)
        return (pltpu.make_async_copy(wg_hbm.at[:, at], wg.at[:, at], w_sem.at[0, n]),
                pltpu.make_async_copy(wu_hbm.at[:, at], wu.at[:, at], w_sem.at[1, n]))

    load_d = pltpu.make_async_copy(wd_hbm, wd, d_sem)
    gather = Gather(full, send_sem, recv_sem, half)
    n_rows = 2 * block
    head, tail = slice(0, half), slice(half, block)

    def gate_up(part, lo, hi):
        def tile(n):
            at = pl.ds(pl.multiple_of(n * step, step), step)
            if part == NEAR_PART:
                for load in loads(n):
                    load.wait()
            a = full[part * n_rows:(part + 1) * n_rows, :]
            gate = jnp.dot(a, wg[:, at], preferred_element_type=F32)
            up = jnp.dot(a, wu[:, at], preferred_element_type=F32)
            hid[part, :, at] = (jax.nn.silu(gate) * up).astype(BF16)

        @pl.loop(0, (hi - lo) // 2)
        def _(i):
            tile(lo + 2 * i)
            tile(lo + 2 * i + 1)

        if (hi - lo) % 2:
            tile(hi - 1)

    def down(part, first, *dst):
        wide = min(1024, dim)

        @pl.loop(0, dim // wide)
        def _(n):
            at = pl.ds(pl.multiple_of(n * wide, wide), wide)
            a = hid[part, first * block:(first + len(dst)) * block, :]
            out = jnp.dot(a, wd[:, at], preferred_element_type=F32).astype(BF16)
            for i, d in enumerate(dst):
                d[:, at] = out[i * block:(i + 1) * block, :]

    kept = {FAR_PART: full.at[block:n_rows], FIRST_PART: full.at[2 * n_rows - block:2 * n_rows],
            LAST_PART: full.at[n_rows:n_rows + block], NEAR_PART: full.at[0:block]}
    traded, moved = {}, []

    def trade(part, buffer):
        if part in (FAR_PART, NEAR_PART):
            down(part, 1, give.at[buffer])
        else:
            down(part, 0, kept[part], give.at[buffer])
        traded[part] = pltpu.make_async_remote_copy(
            src_ref=give.at[buffer], dst_ref=got.at[part], send_sem=mate_sems.at[0, part], recv_sem=mate_sems.at[1, part],
            device_id=gather.mate, device_id_type=MESH)
        traded[part].start()

    def join(part):
        traded[part].wait_recv()
        add_rows(kept[part], kept[part], got.at[part])

    def move(src, dst, device):
        copy = pltpu.make_async_remote_copy(src_ref=src, dst_ref=dst, send_sem=row_sems.at[0, len(moved)],
                                            recv_sem=row_sems.at[1, len(moved)], device_id=device, device_id_type=MESH)
        copy.start()
        moved.append(copy)
        return copy

    fetch = pltpu.make_async_copy(y_hbm, give.at[0], io_sem)
    fetch.start()
    for n in range(n_steps):
        for load in loads(n):
            load.start()
    load_d.start()
    gather.enter()
    fetch.wait()
    norm_into(give.at[0], g_ref, full, block)
    gather.start()
    gather.arrived((MATE, LO), (MATE, HI))
    gate_up(NEAR_PART, 0, n_steps - 1)
    gather.relay()
    gather.rest()
    gate_up(NEAR_PART, n_steps - 1, n_steps)
    gather.arrived((LEFT_MATE, LO), (RIGHT_MATE, HI))
    gate_up(FIRST_PART, 0, n_steps)
    load_d.wait()
    trade(FIRST_PART, 1)
    gather.share_far()
    join(FIRST_PART)
    moved_first = [move(kept[FIRST_PART].at[head], last.at[1, head], gather.left),
                   move(kept[FIRST_PART].at[tail], last.at[0, tail], gather.right)]
    gather.arrived((FAR_MATE, LO), (FAR_MATE, HI))
    gate_up(FAR_PART, 0, n_steps)
    trade(FAR_PART, 0)
    down(FAR_PART, 0, kept[FAR_PART])
    gather.share_last()
    join(FAR_PART)
    pass_right = move(kept[FAR_PART].at[head], passing.at[0], gather.right)
    pass_left = move(kept[FAR_PART].at[tail], passing.at[1], gather.left)
    gather.arrived((LEFT_MATE, HI), (RIGHT_MATE, LO))
    gather.sent()
    gate_up(LAST_PART, 0, n_steps)
    traded[FAR_PART].wait_send()
    trade(LAST_PART, 0)
    traded[FIRST_PART].wait_send()
    trade(NEAR_PART, 1)
    join(LAST_PART)
    pass_left.wait_recv()
    add_rows(kept[LAST_PART].at[head], kept[LAST_PART].at[head], passing.at[1])
    pass_right.wait_recv()
    add_rows(kept[LAST_PART].at[tail], kept[LAST_PART].at[tail], passing.at[0])
    moved_last = [move(kept[LAST_PART].at[head], last.at[1, tail], gather.left),
                  move(kept[LAST_PART].at[tail], last.at[0, head], gather.right)]
    down(NEAR_PART, 0, kept[NEAR_PART])
    traded[LAST_PART].wait_send()
    traded[NEAR_PART].wait_recv()
    for copy in moved_first + moved_last:
        copy.wait_recv()
    finish_rows(sum_ref, None, [kept[NEAR_PART], got.at[NEAR_PART], last.at[0], last.at[1]])
    traded[NEAR_PART].wait_send()
    for copy in moved:
        copy.wait_send()


def mlp(y_rows, g, w_gate, w_up, w_down):
    block, dim = y_rows.shape
    rows = 2 * NX * block
    cols = w_gate.shape[1]
    sem = pltpu.SemaphoreType.DMA
    buffer = lambda *shape: pltpu.VMEM(shape, BF16)
    return pl.pallas_call(
        mlp_kernel,
        out_shape=jax.ShapeDtypeStruct((block, dim), BF16),
        in_specs=[hbm_spec(), vmem_spec()] + [hbm_spec()] * 3,
        out_specs=vmem_spec(),
        scratch_shapes=[buffer(rows, dim), buffer(dim, cols), buffer(dim, cols), buffer(cols, dim), buffer(NX, 2 * block, cols),
                        buffer(2, block, dim), buffer(NX, block, dim), buffer(2, block // 2, dim), buffer(2, block, dim)]
        + GATHER_SEMS + [sem((2, cols // 256)), sem, sem((2, NX)), sem((2, 6)), sem],
        compiler_params=params(1, 64), name='mlp',
        cost_estimate=pl.CostEstimate(flops=6 * rows * dim * cols, bytes_accessed=6 * dim * cols, transcendentals=rows * cols),
    )(y_rows, g, w_gate, w_up, w_down)


def scatter_kernel(h_ref, w_hbm, res_ref, out_ref, w, give, mine, got, passing, last, w_sem, give_sem, got_sem, send_sem, recv_sem):
    x, c, partner, right, left = tp_place()
    block, dim = res_ref.shape
    half = block // 2
    step = 512
    n_steps = dim // step
    loads = []
    for n in range(n_steps):
        at = slice(n * step, (n + 1) * step)
        loads.append(pltpu.make_async_copy(w_hbm.at[:, at], w.at[:, at], w_sem.at[n]))
        loads[-1].start()
    enter([partner, right, left])
    h0, h1 = slice(0, half), slice(half, block)

    def product(dx, core, dst, wait_w=False):
        start = pl.multiple_of((((x + dx) % NX) * 2 + core) * block, block)
        if wait_w:
            for load in loads:
                load.wait()

        @pl.loop(0, n_steps)
        def _(n):
            at = pl.ds(pl.multiple_of(n * step, step), step)
            dst[:, at] = jnp.dot(h_ref[pl.ds(start, block), :], w[:, at], preferred_element_type=F32).astype(BF16)

    def exchange(b, dx, wait_w=False):
        product(dx, 1 - c, give.at[b], wait_w)
        copy = pltpu.make_async_remote_copy(src_ref=give.at[b], dst_ref=got.at[b], send_sem=give_sem.at[b],
                                            recv_sem=got_sem.at[b], device_id=partner, device_id_type=MESH)
        copy.start()
        product(dx, c, mine.at[b])
        return copy

    started = []

    def send(src, dst, device):
        n = len(started)
        copy = pltpu.make_async_remote_copy(src_ref=src, dst_ref=dst, send_sem=send_sem.at[n], recv_sem=recv_sem.at[n],
                                            device_id=device, device_id_type=MESH)
        copy.start()
        started.append(copy)
        return copy

    pair = exchange(0, 2, True)
    pair.wait_recv()
    add_rows(mine.at[0], mine.at[0], got.at[0])
    pass_right = send(mine.at[0, h0], passing.at[0], right)
    pass_left = send(mine.at[0, h1], passing.at[1], left)
    pair_r = exchange(1, 1)
    pair_l = exchange(2, NX - 1)
    pair_r.wait_recv()
    add_rows(mine.at[1], mine.at[1], got.at[1])
    to_right_1 = send(mine.at[1, h1], last.at[0, h1], right)
    pair_l.wait_recv()
    add_rows(mine.at[2], mine.at[2], got.at[2])
    to_left_0 = send(mine.at[2, h0], last.at[1, h0], left)
    pair_o = exchange(3, 0)
    pass_right.wait_recv()
    add_rows(mine.at[1, h0], mine.at[1, h0], passing.at[0])
    to_right_0 = send(mine.at[1, h0], last.at[0, h0], right)
    pass_left.wait_recv()
    add_rows(mine.at[2, h1], mine.at[2, h1], passing.at[1])
    to_left_1 = send(mine.at[2, h1], last.at[1, h1], left)
    pair_o.wait_recv()
    for copy in (to_right_1, to_left_0, to_right_0, to_left_1):
        copy.wait_recv()
    finish_rows(out_ref, res_ref, [mine.at[3], got.at[3], last.at[0], last.at[1]])
    for copy in (pair, pair_r, pair_l, pair_o, *started):
        copy.wait_send()


def scatter_product(h, w, res, cid):
    rows, depth = h.shape
    block, dim = res.shape
    half = block // 2
    sem = pltpu.SemaphoreType.DMA
    return pl.pallas_call(
        scatter_kernel,
        out_shape=jax.ShapeDtypeStruct((block, dim), BF16),
        in_specs=[vmem_spec(), hbm_spec(), vmem_spec()],
        out_specs=vmem_spec(),
        scratch_shapes=[pltpu.VMEM((depth, dim), BF16)] + [pltpu.VMEM((4, block, dim), BF16)] * 3
        + [pltpu.VMEM((2, half, dim), BF16), pltpu.VMEM((2, block, dim), BF16),
           sem((max(1, dim // 512),)), sem((4,)), sem((4,)), sem((6,)), sem((6,))],
        compiler_params=params(cid, 48), name='scatter_product_%d' % cid,
        cost_estimate=pl.CostEstimate(flops=2 * rows * dim * depth, bytes_accessed=2 * dim * depth, transcendentals=0),
    )(h, w, res)


O, R, F, L = range(NX)
EARLY, LATE = range(2)


def attention_order():
    first = lambda dy, dz: ((dy, dz), EARLY)
    second = lambda dy, dz: ((dy, dz), LATE)
    plan = [
        ('near', EARLY, R), ('spread', EARLY, L), ('pass', EARLY, O), first(O, R), first(O, L), first(R, O),
        first(L, O), ('near', LATE, R), ('spread', LATE, L), ('pass', LATE, O), second(O, R), second(O, L),
        ('spread', EARLY, F), second(R, O), first(F, O), ('pass', EARLY, R), first(R, R), ('pass', LATE, R),
        second(R, R), first(R, L), ('pass', EARLY, L), second(L, O), first(L, R), ('pass', LATE, L),
        ('end', EARLY, O), first(O, F), second(R, L), ('spread', LATE, F), ('end', LATE, O), second(O, F),
        ('end', LATE, R), second(F, O), second(L, R), ('pass', EARLY, F), ('end', LATE, L), first(F, R),
        second(F, R), ('end', EARLY, R), first(R, F), first(F, L), ('end', EARLY, L), ('pass', LATE, F),
        second(R, F), ('end', EARLY, F), first(F, F), second(F, L), ('end', LATE, F), second(F, F), first(L, F),
        second(L, F), first(L, L), second(L, L),
    ]
    seq, waits = [first(O, O)], {}
    for item in plan:
        if isinstance(item[0], str):
            waits.setdefault(len(seq), []).append(item)
        else:
            seq.append(item)
    return seq, waits


def pick(index, values):
    out = index * 0 + values[0]
    for i, v in enumerate(values[1:], 1):
        if v != values[i - 1]:
            out = jnp.where(index >= i, v, out)
    return out


def attention_kernel(n_heads, q_ref, kv_ref, o_ref, m_ref, l_ref, acc_ref, buf, send_sem, recv_sem):
    piece = kv_ref.shape[2]
    me = lax.axis_index('cp')
    y, z = me % NX, me // NX
    scale = HD ** -0.5 * math.log2(math.e)
    at_y = lambda d: {'cp': z * NX + (y + d) % NX}
    at_z = lambda d: {'cp': ((z + d) % NX) * NX + y}
    enter([at_y(1), at_y(3), at_z(1), at_z(3)])
    axes = ((at_y, at_z), (at_z, at_y))

    def slot(kind, da, db):
        dy, dz = (da, db) if kind == 0 else (db, da)
        return dz * NX + dy

    started, landing = [], {}

    def copy_of(kind, src, dst, axis, d, part, n):
        source = kv_ref.at[kind] if src == (0, 0) else buf.at[kind, slot(kind, *src)]
        target = buf.at[kind, slot(kind, *dst)]
        if part is not None:
            source, target = source.at[part], target.at[part]
        return pltpu.make_async_remote_copy(
            src_ref=source, dst_ref=target, send_sem=send_sem.at[n],
            recv_sem=recv_sem.at[kind, slot(kind, *dst), part or 0],
            device_id=axes[kind][axis](d), device_id_type=MESH)

    def send(kind, src, dst, axis, d, part=None):
        key = (kind, src, dst, axis, d, part, len(started))
        copy_of(*key).start()
        started.append(key)
        landing[kind, dst, part] = key

    def landed(*key):
        copy_of(*landing[key]).wait_recv()

    def spread(kind, da):
        send(kind, (da, O), (da, L), 1, R)
        send(kind, (da, O), (da, R), 1, L)

    def act(step, kind, da):
        if step == 'near':
            landed(kind, (R, O), None)
            landed(kind, (L, O), None)
            send(kind, (L, O), (F, O), 0, R, 0)
            send(kind, (R, O), (F, O), 0, L, 1)
            spread(kind, R)
        elif step == 'spread':
            if da == F:
                for part in (0, 1):
                    landed(kind, (F, O), part)
            spread(kind, da)
        elif step == 'pass':
            landed(kind, (da, L), None)
            send(kind, (da, L), (da, F), 1, R, 0)
            landed(kind, (da, R), None)
            send(kind, (da, R), (da, F), 1, L, 1)
        else:
            for part in (0, 1):
                landed(kind, (da, F), part)

    for kind in (EARLY, LATE):
        send(kind, (O, O), (L, O), 0, R)
        send(kind, (O, O), (R, O), 0, L)
        spread(kind, O)

    m_ref[...] = jnp.full_like(m_ref, -1e30)
    l_ref[...] = jnp.zeros_like(l_ref)
    acc_ref[...] = jnp.zeros_like(acc_ref)

    def unit(q_row, k, v, masked):
        rows = pl.ds(pl.multiple_of(q_row, piece), piece)
        heads = [slice(h * HD, (h + 1) * HD) for h in range(n_heads)]

        def score(cols):
            s = lax.dot_general(q_ref[rows, cols], k, (((1,), (1,)), ((), ())), preferred_element_type=F32)
            if masked:
                row = lax.broadcasted_iota(jnp.int32, (piece, piece), 0)
                col = lax.broadcasted_iota(jnp.int32, (piece, piece), 1)
                s = jnp.where(row >= col, s, -1e30)
            return s

        def absorb(cols, s):
            m_old = m_ref[rows, cols]
            m_new = jnp.maximum(m_old, jnp.max(s, axis=1, keepdims=True) * scale)
            alpha = jnp.exp2(m_old - m_new)
            p = [jnp.exp2(s[:, i * HD:(i + 1) * HD] * scale - m_new) for i in range(piece // HD)]
            psum = p[0]
            for part in p[1:]:
                psum = psum + part
            l_ref[rows, cols] = l_ref[rows, cols] * alpha + psum
            pb = jnp.concatenate([part.astype(BF16) for part in p], axis=1)
            pv = jnp.dot(pb, v, preferred_element_type=F32)
            acc_ref[rows, cols] = acc_ref[rows, cols] * alpha + pv
            m_ref[rows, cols] = m_new

        ahead = score(heads[0])
        for cols, after in zip(heads, heads[1:] + [None]):
            s, ahead = ahead, score(after) if after else None
            absorb(cols, s)

    @pl.loop(0, 2)
    def _(kind):
        unit(kind * piece, kv_ref[kind, 0], kv_ref[kind, 1], True)

    unit(piece, kv_ref[0, 0], kv_ref[0, 1], False)
    seq, waits = attention_order()
    marks = sorted(waits) + [len(seq)]

    @pl.loop(1, len(seq))
    def _(u):
        for mark in marks[:-1]:
            @pl.when(u == mark)
            def _():
                for step in waits[mark]:
                    act(*step)

        dy = pick(u, [p[0] for p, _ in seq])
        dz = pick(u, [p[1] for p, _ in seq])
        which = pick(u, [w for _, w in seq])
        src = ((z + dz) % NX) * NX + (y + dy) % NX
        late = jnp.where(src > me, 1, 0)
        q_row = jnp.where(which == 0, 1, late) * piece
        kind = which * late
        at = dz * NX + dy
        unit(q_row, buf[kind, at, 0], buf[kind, at, 1], False)

    @pl.loop(0, 2)
    def _(part):
        rows = pl.ds(pl.multiple_of(part * piece, piece), piece)
        for h in range(n_heads):
            cols = slice(h * HD, (h + 1) * HD)
            total = jnp.sum(l_ref[rows, cols], axis=1, keepdims=True)
            o_ref[rows, cols] = (acc_ref[rows, cols] / total).astype(BF16)

    for key in started:
        copy_of(*key).wait_send()


def attention(q, kv):
    rows, width = q.shape
    piece = kv.shape[2]
    sem = pltpu.SemaphoreType.DMA
    return pl.pallas_call(
        functools.partial(attention_kernel, width // HD),
        out_shape=jax.ShapeDtypeStruct((rows, width), BF16),
        in_specs=[vmem_spec()] * 2,
        out_specs=vmem_spec(),
        scratch_shapes=[pltpu.VMEM((rows, width), F32)] * 3 + [pltpu.VMEM((2, NX * NX, 2, piece, HD), BF16),
                                                              sem((40,)), sem((2, NX * NX, 2))],
        compiler_params=params(2, 48), name='attention',
        cost_estimate=pl.CostEstimate(flops=18 * 10 ** 9, bytes_accessed=10 * 2 ** 20, transcendentals=35 * 10 ** 6),
    )(q, kv)


def solution(mesh):
    row_spec = P('dp', ('cp', 'tp'), None)
    head_cols = P(None, 'tp', None)
    cp_size = mesh.shape['cp']

    def local_layer(x, g_attn, w_q, w_k, w_v, w_o, g_mlp, w_gate, w_up, w_down):
        x_rows = x[0]
        block, dim = x_rows.shape
        rows = block * mesh.shape['tp']
        piece = rows // 2
        cp_index = lax.axis_index('cp')
        n_heads = w_q.shape[1]
        j = jnp.arange(rows, dtype=jnp.int32)
        positions = jnp.where(j < piece, cp_index * piece + j, (2 * cp_size - 1 - cp_index) * piece + j - piece)
        cos, sin = rope_tables(positions)
        in_hbm = [pltpu.with_memory_space_constraint(v, pltpu.HBM) for v in (x_rows, w_q, w_k.reshape(dim, HD), w_v.reshape(dim, HD))]
        q, kv = gather_qkv(in_hbm[0], g_attn.reshape(dim // HD, HD), cos, sin, *in_hbm[1:], n_heads, piece)
        o = attention(q, kv)
        y_rows = scatter_product(o, w_o.reshape(n_heads * HD, dim), x_rows, 3)
        d_rows = mlp(y_rows, g_mlp.reshape(dim // HD, HD), w_gate, w_up, w_down)
        return (y_rows.astype(F32) + d_rows.astype(F32)).astype(BF16)[None]

    return jax.shard_map(local_layer, mesh=mesh,
                         in_specs=(row_spec, P(), head_cols, head_cols, head_cols, P('tp', None, None),
                                   P(), P(None, 'tp'), P(None, 'tp'), P('tp', None)),
                         out_specs=row_spec, check_vma=False)
```

```python
import functools
import math
import jax
import jax.numpy as jnp
from jax import lax
from jax.experimental import pallas as pl
from jax.experimental.pallas import tpu as pltpu
from jax.sharding import PartitionSpec as P

NORM_EPS = 1e-5
ROPE_THETA = 500000.0
HD = 128
NX = 4
MESH = pl.DeviceIdType.MESH
F32 = jnp.float32
BF16 = jnp.bfloat16


def params(cid, vmem_mib, **more):
    return pltpu.CompilerParams(collective_id=cid, has_side_effects=True, vmem_limit_bytes=min(vmem_mib * 2 ** 20, 67043328), **more)


def vmem_spec():
    return pl.BlockSpec(memory_space=pltpu.VMEM)


def hbm_spec():
    return pl.BlockSpec(memory_space=pltpu.HBM)


def rope_tables(positions):
    inv_freq = ROPE_THETA ** (-2.0 * jnp.arange(HD // 2, dtype=F32) / HD)
    angles = positions.astype(F32)[:, None] * inv_freq[None, :]
    c, s = jnp.cos(angles), jnp.sin(angles)
    return jnp.concatenate([c, c], axis=-1), jnp.concatenate([-s, s], axis=-1)


def knock(peers):
    for peer in peers:
        pl.semaphore_signal(pltpu.get_barrier_semaphore(), inc=1, device_id=peer, device_id_type=MESH)


def answered(peers):
    pl.semaphore_wait(pltpu.get_barrier_semaphore(), len(peers))


def tp_place():
    t = lax.axis_index('tp')
    x, c = t // 2, t % 2
    side = lambda d: {'tp': ((x + d) % NX) * 2 + c}
    return x, c, {'tp': x * 2 + 1 - c}, side(1), side(NX - 1)


OWN, MATE, LEFT, LEFT_MATE, RIGHT, RIGHT_MATE, FAR, FAR_MATE = range(8)
LO, HI = range(2)
NEAR_PART, FIRST_PART, LAST_PART, FAR_PART = range(4)
GATHER_PARTS = (((OWN, LO), (OWN, HI), (MATE, LO), (MATE, HI)),
                ((LEFT, LO), (RIGHT, HI), (LEFT_MATE, LO), (RIGHT_MATE, HI)),
                ((LEFT, HI), (RIGHT, LO), (LEFT_MATE, HI), (RIGHT_MATE, LO)),
                ((FAR, LO), (FAR, HI), (FAR_MATE, LO), (FAR_MATE, HI)))
GATHER_PLACE = {name: i for i, name in enumerate(n for part in GATHER_PARTS for n in part)}
N_PLACES = len(GATHER_PLACE)


def norm_into(x_ref, g_ref, full, rows):
    gain = jnp.concatenate([g_ref[i:i + 1, :] for i in range(g_ref.shape[0])], axis=1).astype(F32)
    step = min(16, rows)

    @pl.loop(0, rows // step)
    def _(i):
        where = pl.ds(pl.multiple_of(i * step, step), step)
        r = x_ref[where, :].astype(F32)
        mean_sq = jnp.mean(r * r, axis=-1, keepdims=True)
        full[where, :] = (r * lax.rsqrt(mean_sq + NORM_EPS) * gain).astype(BF16)


class Gather:
    def __init__(self, full, send_sem, recv_sem, half):
        self.full, self.send_sem, self.recv_sem, self.half = full, send_sem, recv_sem, half
        _, _, self.mate, self.right, self.left = tp_place()
        self.started, self.landing = [], {}

    def enter(self, barrier):
        barrier([self.mate, self.right, self.left])

    def send(self, src, dst, h, device):
        rows = [pl.ds(GATHER_PLACE[slot, h] * self.half, self.half) for slot in (src, dst)]
        copy = pltpu.make_async_remote_copy(
            src_ref=self.full.at[rows[0]], dst_ref=self.full.at[rows[1]],
            send_sem=self.send_sem.at[len(self.started)], recv_sem=self.recv_sem.at[GATHER_PLACE[dst, h]],
            device_id=device, device_id_type=MESH)
        copy.start()
        self.started.append(copy)
        self.landing[dst, h] = copy

    def arrived(self, *names):
        for name in names:
            self.landing[name].wait_recv()

    def rest(self):
        self.send(OWN, LEFT, HI, self.right)
        self.send(OWN, RIGHT, LO, self.left)

    def start(self):
        self.send(OWN, LEFT, LO, self.right)
        self.send(OWN, RIGHT, HI, self.left)
        for h in (LO, HI):
            self.send(OWN, MATE, h, self.mate)

    def relay(self):
        self.arrived((LEFT, LO))
        self.send(LEFT, FAR, LO, self.right)
        self.arrived((RIGHT, HI))
        self.send(RIGHT, FAR, HI, self.left)
        self.send(LEFT, LEFT_MATE, LO, self.mate)
        self.send(RIGHT, RIGHT_MATE, HI, self.mate)

    def share_far(self):
        for h in (LO, HI):
            self.arrived((FAR, h))
            self.send(FAR, FAR_MATE, h, self.mate)

    def share_last(self):
        self.arrived((LEFT, HI))
        self.send(LEFT, LEFT_MATE, HI, self.mate)
        self.arrived((RIGHT, LO))
        self.send(RIGHT, RIGHT_MATE, LO, self.mate)

    def sent(self, *which):
        for copy in self.started:
            copy.wait_send()


def part_rows(part, block):
    t = lax.axis_index('tp')
    x, c = t // 2, t % 2
    rows = []
    for name, h in GATHER_PARTS[part]:
        dx, other = {OWN: 0, LEFT: NX - 1, RIGHT: 1, FAR: 2}[name // 2 * 2], name % 2
        core = 1 - c if other else c
        rows.append((((x + dx) % NX) * 2 + core) * block + h * (block // 2))
    return rows


N_SENDS = 14
GATHER_SEMS = [pltpu.SemaphoreType.DMA((N_SENDS,)), pltpu.SemaphoreType.DMA((N_PLACES,))]


def qkv_kernel(n_heads, x_hbm, g_ref, cos_ref, sin_ref, wq_hbm, wk_hbm, wv_hbm, q_ref, kv_ref, full, w, wq3, x_ref, send_sem, recv_sem, w_sem, x_sem):
    block = x_ref.shape[0]
    half = block // 2
    piece = kv_ref.shape[2]
    width = n_heads * HD
    loads = [pltpu.make_async_copy(wq_hbm, wq3, w_sem.at[0]),
             pltpu.make_async_copy(wk_hbm, w.at[:, width:width + HD], w_sem.at[1]),
             pltpu.make_async_copy(wv_hbm, w.at[:, width + HD:width + 2 * HD], w_sem.at[2])]

    def rotate(v, cos, sin):
        f = v.astype(BF16).astype(F32)
        return (f * cos + pltpu.roll(f, HD // 2, 1) * sin).astype(BF16)

    def keys_values(part, rows, a):
        out = jnp.dot(a, w[:, width:], preferred_element_type=F32)
        for i, r in enumerate(rows):
            here = slice(i * half, (i + 1) * half)
            where = pl.ds(pl.multiple_of(r % piece, half), half)
            kv_ref[r // piece, 0, where, :] = rotate(out[here, :HD], cos_ref[pl.ds(r, half), :], sin_ref[pl.ds(r, half), :])
            kv_ref[r // piece, 1, where, :] = out[here, HD:].astype(BF16)

    def queries(part, rows, a):
        for start in range(0, width, 2 * HD):
            out = jnp.dot(a, w[:, start:start + 2 * HD], preferred_element_type=F32)
            for i, r in enumerate(rows):
                here = slice(i * half, (i + 1) * half)
                cos, sin = cos_ref[pl.ds(r, half), :], sin_ref[pl.ds(r, half), :]
                for k in (0, HD):
                    q_ref[pl.ds(r, half), start + k:start + k + HD] = rotate(out[here, k:k + HD], cos, sin)

    def compute(part):
        rows = [pl.multiple_of(r, half) for r in part_rows(part, block)]
        n = len(rows) * half
        a = full[part * n:(part + 1) * n, :]
        keys_values(part, rows, a)
        queries(part, rows, a)

    gather = Gather(full, send_sem, recv_sem, half)
    fetch = pltpu.make_async_copy(x_hbm, x_ref, x_sem)
    fetch.start()
    for load in loads:
        load.start()
    gather.enter(knock)
    fetch.wait()
    norm_into(x_ref, g_ref, full, block)
    gather.enter(answered)
    gather.start()
    gather.rest()
    gather.arrived((MATE, LO), (MATE, HI))
    for load in loads:
        load.wait()
    some = min(256, w.shape[0])

    @pl.loop(0, w.shape[0] // some)
    def _(i):
        at = pl.ds(pl.multiple_of(i * some, some), some)
        w[at, 0:width] = wq3[at].reshape(some, width)

    compute(NEAR_PART)
    gather.relay()
    gather.arrived((LEFT_MATE, LO), (RIGHT_MATE, HI))
    compute(FIRST_PART)
    gather.share_last()
    gather.arrived((LEFT_MATE, HI), (RIGHT_MATE, LO))
    compute(LAST_PART)
    gather.share_far()
    gather.arrived((FAR_MATE, LO), (FAR_MATE, HI))
    compute(FAR_PART)
    gather.sent()


def gather_qkv(x_rows, g, cos, sin, w_q, w_k, w_v, n_heads, piece):
    block, dim = x_rows.shape
    rows = 2 * NX * block
    width = n_heads * HD
    return pl.pallas_call(
        functools.partial(qkv_kernel, n_heads),
        out_shape=(jax.ShapeDtypeStruct((rows, width), BF16), jax.ShapeDtypeStruct((2, 2, piece, HD), BF16)),
        in_specs=[hbm_spec()] + [vmem_spec()] * 3 + [hbm_spec()] * 3,
        out_specs=(vmem_spec(), vmem_spec()),
        scratch_shapes=[pltpu.VMEM((rows, dim), BF16), pltpu.VMEM((dim, width + 2 * HD), BF16), pltpu.VMEM((dim, n_heads, HD), BF16),
                        pltpu.VMEM((block, dim), BF16)]
        + GATHER_SEMS + [pltpu.SemaphoreType.DMA((3,)), pltpu.SemaphoreType.DMA],
        compiler_params=params(0, 48), name='gather_qkv',
        cost_estimate=pl.CostEstimate(flops=2 * rows * dim * (width + 2 * HD), bytes_accessed=2 * dim * (width + 2 * HD), transcendentals=0),
    )(x_rows, g, cos, sin, w_q, w_k, w_v)


def add_rows(dst, a, b):
    step = min(16, dst.shape[0])

    @pl.loop(0, dst.shape[0] // step)
    def _(i):
        at = pl.ds(pl.multiple_of(i * step, step), step)
        dst[at, :] = a[at, :] + b[at, :]


def finish_rows(out, res, parts):
    step = min(16, out.shape[0])

    @pl.loop(0, out.shape[0] // step)
    def _(i):
        at = pl.ds(pl.multiple_of(i * step, step), step)
        total = parts[0][at, :].astype(F32)
        for part in parts[1:]:
            total = total + part[at, :].astype(F32)
        total = total.astype(BF16)
        out[at, :] = total if res is None else (res[at, :].astype(F32) + total.astype(F32)).astype(BF16)


def mlp_kernel(y_hbm, g_ref, wg_hbm, wu_hbm, wd_hbm, sum_ref, full, wg, wu, wd, hid, give, got, passing, last,
               send_sem, recv_sem, w_sem, d_sem, mate_sems, row_sems, io_sem):
    block, dim = y_hbm.shape
    half = block // 2
    cols = wg.shape[1]
    step = 256
    n_steps = cols // step

    def loads(n):
        at = pl.ds(pl.multiple_of(n * step, step), step)
        return (pltpu.make_async_copy(wg_hbm.at[:, at], wg.at[:, at], w_sem.at[0, n]),
                pltpu.make_async_copy(wu_hbm.at[:, at], wu.at[:, at], w_sem.at[1, n]))

    load_d = pltpu.make_async_copy(wd_hbm, wd, d_sem)
    gather = Gather(full, send_sem, recv_sem, half)
    n_rows = 2 * block
    head, tail = slice(0, half), slice(half, block)

    def gate_up(part, lo, hi):
        def tile(n):
            at = pl.ds(pl.multiple_of(n * step, step), step)
            if part == NEAR_PART:
                for load in loads(n):
                    load.wait()
            a = full[part * n_rows:(part + 1) * n_rows, :]
            gate = jnp.dot(a, wg[:, at], preferred_element_type=F32)
            up = jnp.dot(a, wu[:, at], preferred_element_type=F32)
            hid[part, :, at] = (jax.nn.silu(gate) * up).astype(BF16)

        @pl.loop(0, (hi - lo) // 2)
        def _(i):
            tile(lo + 2 * i)
            tile(lo + 2 * i + 1)

        if (hi - lo) % 2:
            tile(hi - 1)

    def down(part, first, *dst):
        wide = min(1024, dim)

        @pl.loop(0, dim // wide)
        def _(n):
            at = pl.ds(pl.multiple_of(n * wide, wide), wide)
            a = hid[part, first * block:(first + len(dst)) * block, :]
            out = jnp.dot(a, wd[:, at], preferred_element_type=F32).astype(BF16)
            for i, d in enumerate(dst):
                d[:, at] = out[i * block:(i + 1) * block, :]

    kept = {FAR_PART: full.at[block:n_rows], FIRST_PART: full.at[2 * n_rows - block:2 * n_rows],
            LAST_PART: full.at[n_rows:n_rows + block], NEAR_PART: full.at[0:block]}
    traded, moved = {}, []

    def trade(part, buffer):
        if part in (FAR_PART, NEAR_PART):
            down(part, 1, give.at[buffer])
        else:
            down(part, 0, kept[part], give.at[buffer])
        traded[part] = pltpu.make_async_remote_copy(
            src_ref=give.at[buffer], dst_ref=got.at[part], send_sem=mate_sems.at[0, part], recv_sem=mate_sems.at[1, part],
            device_id=gather.mate, device_id_type=MESH)
        traded[part].start()

    def join(part):
        traded[part].wait_recv()
        add_rows(kept[part], kept[part], got.at[part])

    def move(src, dst, device):
        copy = pltpu.make_async_remote_copy(src_ref=src, dst_ref=dst, send_sem=row_sems.at[0, len(moved)],
                                            recv_sem=row_sems.at[1, len(moved)], device_id=device, device_id_type=MESH)
        copy.start()
        moved.append(copy)
        return copy

    fetch = pltpu.make_async_copy(y_hbm, give.at[0], io_sem)
    fetch.start()
    for n in range(n_steps):
        for load in loads(n):
            load.start()
    load_d.start()
    gather.enter(knock)
    fetch.wait()
    norm_into(give.at[0], g_ref, full, block)
    gather.enter(answered)
    gather.start()
    gather.arrived((MATE, LO), (MATE, HI))
    gate_up(NEAR_PART, 0, n_steps - 1)
    gather.relay()
    gather.rest()
    gate_up(NEAR_PART, n_steps - 1, n_steps)
    gather.arrived((LEFT_MATE, LO), (RIGHT_MATE, HI))
    gate_up(FIRST_PART, 0, n_steps)
    load_d.wait()
    trade(FIRST_PART, 1)
    gather.share_far()
    join(FIRST_PART)
    moved_first = [move(kept[FIRST_PART].at[head], last.at[1, head], gather.left),
                   move(kept[FIRST_PART].at[tail], last.at[0, tail], gather.right)]
    gather.arrived((FAR_MATE, LO), (FAR_MATE, HI))
    gate_up(FAR_PART, 0, n_steps)
    trade(FAR_PART, 0)
    down(FAR_PART, 0, kept[FAR_PART])
    gather.share_last()
    join(FAR_PART)
    pass_right = move(kept[FAR_PART].at[head], passing.at[0], gather.right)
    pass_left = move(kept[FAR_PART].at[tail], passing.at[1], gather.left)
    gather.arrived((LEFT_MATE, HI), (RIGHT_MATE, LO))
    gather.sent()
    gate_up(LAST_PART, 0, n_steps)
    traded[FAR_PART].wait_send()
    trade(LAST_PART, 0)
    traded[FIRST_PART].wait_send()
    trade(NEAR_PART, 1)
    join(LAST_PART)
    pass_left.wait_recv()
    add_rows(kept[LAST_PART].at[head], kept[LAST_PART].at[head], passing.at[1])
    pass_right.wait_recv()
    add_rows(kept[LAST_PART].at[tail], kept[LAST_PART].at[tail], passing.at[0])
    moved_last = [move(kept[LAST_PART].at[head], last.at[1, tail], gather.left),
                  move(kept[LAST_PART].at[tail], last.at[0, head], gather.right)]
    down(NEAR_PART, 0, kept[NEAR_PART])
    traded[LAST_PART].wait_send()
    traded[NEAR_PART].wait_recv()
    for copy in moved_first + moved_last:
        copy.wait_recv()
    finish_rows(sum_ref, None, [kept[NEAR_PART], got.at[NEAR_PART], last.at[0], last.at[1]])
    traded[NEAR_PART].wait_send()
    for copy in moved:
        copy.wait_send()


def mlp(y_rows, g, w_gate, w_up, w_down):
    block, dim = y_rows.shape
    rows = 2 * NX * block
    cols = w_gate.shape[1]
    sem = pltpu.SemaphoreType.DMA
    buffer = lambda *shape: pltpu.VMEM(shape, BF16)
    return pl.pallas_call(
        mlp_kernel,
        out_shape=jax.ShapeDtypeStruct((block, dim), BF16),
        in_specs=[hbm_spec(), vmem_spec()] + [hbm_spec()] * 3,
        out_specs=vmem_spec(),
        scratch_shapes=[buffer(rows, dim), buffer(dim, cols), buffer(dim, cols), buffer(cols, dim), buffer(NX, 2 * block, cols),
                        buffer(2, block, dim), buffer(NX, block, dim), buffer(2, block // 2, dim), buffer(2, block, dim)]
        + GATHER_SEMS + [sem((2, cols // 256)), sem, sem((2, NX)), sem((2, 6)), sem],
        compiler_params=params(1, 64), name='mlp',
        cost_estimate=pl.CostEstimate(flops=6 * rows * dim * cols, bytes_accessed=6 * dim * cols, transcendentals=rows * cols),
    )(y_rows, g, w_gate, w_up, w_down)


def scatter_kernel(h_ref, w_hbm, res_ref, out_ref, w, give, mine, got, passing, last, w_sem, give_sem, got_sem, send_sem, recv_sem):
    x, c, partner, right, left = tp_place()
    block, dim = res_ref.shape
    half = block // 2
    step = 512
    n_steps = dim // step
    loads = []
    for n in range(n_steps):
        at = slice(n * step, (n + 1) * step)
        loads.append(pltpu.make_async_copy(w_hbm.at[:, at], w.at[:, at], w_sem.at[n]))
        loads[-1].start()
    knock([partner, right, left])
    h0, h1 = slice(0, half), slice(half, block)

    def product(dx, core, dst, wait_w=False):
        start = pl.multiple_of((((x + dx) % NX) * 2 + core) * block, block)
        if wait_w:
            for load in loads:
                load.wait()

        @pl.loop(0, n_steps)
        def _(n):
            at = pl.ds(pl.multiple_of(n * step, step), step)
            dst[:, at] = jnp.dot(h_ref[pl.ds(start, block), :], w[:, at], preferred_element_type=F32).astype(BF16)

    def exchange(b, dx, wait_w=False):
        product(dx, 1 - c, give.at[b], wait_w)
        if wait_w:
            answered([partner, right, left])
        copy = pltpu.make_async_remote_copy(src_ref=give.at[b], dst_ref=got.at[b], send_sem=give_sem.at[b],
                                            recv_sem=got_sem.at[b], device_id=partner, device_id_type=MESH)
        copy.start()
        product(dx, c, mine.at[b])
        return copy

    started = []

    def send(src, dst, device):
        n = len(started)
        copy = pltpu.make_async_remote_copy(src_ref=src, dst_ref=dst, send_sem=send_sem.at[n], recv_sem=recv_sem.at[n],
                                            device_id=device, device_id_type=MESH)
        copy.start()
        started.append(copy)
        return copy

    pair = exchange(0, 2, True)
    pair.wait_recv()
    add_rows(mine.at[0], mine.at[0], got.at[0])
    pass_right = send(mine.at[0, h0], passing.at[0], right)
    pass_left = send(mine.at[0, h1], passing.at[1], left)
    pair_r = exchange(1, 1)
    pair_l = exchange(2, NX - 1)
    pair_r.wait_recv()
    add_rows(mine.at[1], mine.at[1], got.at[1])
    to_right_1 = send(mine.at[1, h1], last.at[0, h1], right)
    pair_l.wait_recv()
    add_rows(mine.at[2], mine.at[2], got.at[2])
    to_left_0 = send(mine.at[2, h0], last.at[1, h0], left)
    pair_o = exchange(3, 0)
    pass_right.wait_recv()
    add_rows(mine.at[1, h0], mine.at[1, h0], passing.at[0])
    to_right_0 = send(mine.at[1, h0], last.at[0, h0], right)
    pass_left.wait_recv()
    add_rows(mine.at[2, h1], mine.at[2, h1], passing.at[1])
    to_left_1 = send(mine.at[2, h1], last.at[1, h1], left)
    pair_o.wait_recv()
    for copy in (to_right_1, to_left_0, to_right_0, to_left_1):
        copy.wait_recv()
    finish_rows(out_ref, res_ref, [mine.at[3], got.at[3], last.at[0], last.at[1]])
    for copy in (pair, pair_r, pair_l, pair_o, *started):
        copy.wait_send()


def scatter_product(h, w, res, cid):
    rows, depth = h.shape
    block, dim = res.shape
    half = block // 2
    sem = pltpu.SemaphoreType.DMA
    return pl.pallas_call(
        scatter_kernel,
        out_shape=jax.ShapeDtypeStruct((block, dim), BF16),
        in_specs=[vmem_spec(), hbm_spec(), vmem_spec()],
        out_specs=vmem_spec(),
        scratch_shapes=[pltpu.VMEM((depth, dim), BF16)] + [pltpu.VMEM((4, block, dim), BF16)] * 3
        + [pltpu.VMEM((2, half, dim), BF16), pltpu.VMEM((2, block, dim), BF16),
           sem((max(1, dim // 512),)), sem((4,)), sem((4,)), sem((6,)), sem((6,))],
        compiler_params=params(cid, 48), name='scatter_product_%d' % cid,
        cost_estimate=pl.CostEstimate(flops=2 * rows * dim * depth, bytes_accessed=2 * dim * depth, transcendentals=0),
    )(h, w, res)


O, R, F, L = range(NX)
EARLY, LATE = range(2)


def attention_order():
    first = lambda dy, dz: ((dy, dz), EARLY)
    second = lambda dy, dz: ((dy, dz), LATE)
    plan = [
        ('near', EARLY, R), ('spread', EARLY, L), ('pass', EARLY, O), first(O, R), first(O, L), first(R, O),
        first(L, O), ('near', LATE, R), ('spread', LATE, L), ('pass', LATE, O), second(O, R), second(O, L),
        ('spread', EARLY, F), second(R, O), first(F, O), ('pass', EARLY, R), first(R, R), ('pass', LATE, R),
        second(R, R), first(R, L), ('pass', EARLY, L), second(L, O), first(L, R), ('pass', LATE, L),
        ('end', EARLY, O), first(O, F), second(R, L), ('spread', LATE, F), ('end', LATE, O), second(O, F),
        ('end', LATE, R), second(F, O), second(L, R), ('pass', EARLY, F), ('end', LATE, L), first(F, R),
        second(F, R), ('end', EARLY, R), first(R, F), first(F, L), ('end', EARLY, L), ('pass', LATE, F),
        second(R, F), ('end', EARLY, F), first(F, F), second(F, L), ('end', LATE, F), second(F, F), first(L, F),
        second(L, F), first(L, L), second(L, L),
    ]
    seq, waits = [first(O, O)], {}
    for item in plan:
        if isinstance(item[0], str):
            waits.setdefault(len(seq), []).append(item)
        else:
            seq.append(item)
    return seq, waits


def pick(index, values):
    out = index * 0 + values[0]
    for i, v in enumerate(values[1:], 1):
        if v != values[i - 1]:
            out = jnp.where(index >= i, v, out)
    return out


def attention_kernel(n_heads, q_ref, kv_ref, o_ref, m_ref, l_ref, acc_ref, buf, send_sem, recv_sem):
    piece = kv_ref.shape[2]
    me = lax.axis_index('cp')
    y, z = me % NX, me // NX
    scale = HD ** -0.5 * math.log2(math.e)
    at_y = lambda d: {'cp': z * NX + (y + d) % NX}
    at_z = lambda d: {'cp': ((z + d) % NX) * NX + y}
    peers = [at_y(R), at_y(L), at_z(R), at_z(L)]
    knock(peers)
    axes = ((at_y, at_z), (at_z, at_y))

    def slot(kind, da, db):
        dy, dz = (da, db) if kind == 0 else (db, da)
        return dz * NX + dy

    started, landing = [], {}

    def copy_of(kind, src, dst, axis, d, part, n):
        source = kv_ref.at[kind] if src == (0, 0) else buf.at[kind, slot(kind, *src)]
        target = buf.at[kind, slot(kind, *dst)]
        if part is not None:
            source, target = source.at[part], target.at[part]
        return pltpu.make_async_remote_copy(
            src_ref=source, dst_ref=target, send_sem=send_sem.at[n],
            recv_sem=recv_sem.at[kind, slot(kind, *dst), part or 0],
            device_id=axes[kind][axis](d), device_id_type=MESH)

    def send(kind, src, dst, axis, d, part=None):
        key = (kind, src, dst, axis, d, part, len(started))
        copy_of(*key).start()
        started.append(key)
        landing[kind, dst, part] = key

    def landed(*key):
        copy_of(*landing[key]).wait_recv()

    def spread(kind, da):
        send(kind, (da, O), (da, L), 1, R)
        send(kind, (da, O), (da, R), 1, L)

    def act(step, kind, da):
        if step == 'near':
            landed(kind, (R, O), None)
            landed(kind, (L, O), None)
            send(kind, (L, O), (F, O), 0, R, 0)
            send(kind, (R, O), (F, O), 0, L, 1)
            spread(kind, R)
        elif step == 'spread':
            if da == F:
                for part in (0, 1):
                    landed(kind, (F, O), part)
            spread(kind, da)
        elif step == 'pass':
            landed(kind, (da, L), None)
            send(kind, (da, L), (da, F), 1, R, 0)
            landed(kind, (da, R), None)
            send(kind, (da, R), (da, F), 1, L, 1)
        else:
            for part in (0, 1):
                landed(kind, (da, F), part)

    m_ref[...] = jnp.full_like(m_ref, -1e30)
    l_ref[...] = jnp.zeros_like(l_ref)
    acc_ref[...] = jnp.zeros_like(acc_ref)

    answered(peers)
    for kind in (EARLY, LATE):
        send(kind, (O, O), (L, O), 0, R)
        send(kind, (O, O), (R, O), 0, L)
        spread(kind, O)

    def unit(q_row, k, v, masked):
        rows = pl.ds(pl.multiple_of(q_row, piece), piece)
        heads = [slice(h * HD, (h + 1) * HD) for h in range(n_heads)]

        def score(cols):
            s = lax.dot_general(q_ref[rows, cols], k, (((1,), (1,)), ((), ())), preferred_element_type=F32)
            if masked:
                row = lax.broadcasted_iota(jnp.int32, (piece, piece), 0)
                col = lax.broadcasted_iota(jnp.int32, (piece, piece), 1)
                s = jnp.where(row >= col, s, -1e30)
            return s

        def absorb(cols, s):
            m_old = m_ref[rows, cols]
            m_new = jnp.maximum(m_old, jnp.max(s, axis=1, keepdims=True) * scale)
            alpha = jnp.exp2(m_old - m_new)
            p = [jnp.exp2(s[:, i * HD:(i + 1) * HD] * scale - m_new) for i in range(piece // HD)]
            psum = p[0]
            for part in p[1:]:
                psum = psum + part
            l_ref[rows, cols] = l_ref[rows, cols] * alpha + psum
            pb = jnp.concatenate([part.astype(BF16) for part in p], axis=1)
            pv = jnp.dot(pb, v, preferred_element_type=F32)
            acc_ref[rows, cols] = acc_ref[rows, cols] * alpha + pv
            m_ref[rows, cols] = m_new

        ahead = score(heads[0])
        for cols, after in zip(heads, heads[1:] + [None]):
            s, ahead = ahead, score(after) if after else None
            absorb(cols, s)

    @pl.loop(0, 2)
    def _(kind):
        unit(kind * piece, kv_ref[kind, 0], kv_ref[kind, 1], True)

    unit(piece, kv_ref[0, 0], kv_ref[0, 1], False)
    seq, waits = attention_order()
    marks = sorted(waits) + [len(seq)]

    @pl.loop(1, len(seq))
    def _(u):
        for mark in marks[:-1]:
            @pl.when(u == mark)
            def _():
                for step in waits[mark]:
                    act(*step)

        dy = pick(u, [p[0] for p, _ in seq])
        dz = pick(u, [p[1] for p, _ in seq])
        which = pick(u, [w for _, w in seq])
        src = ((z + dz) % NX) * NX + (y + dy) % NX
        late = jnp.where(src > me, 1, 0)
        q_row = jnp.where(which == 0, 1, late) * piece
        kind = which * late
        at = dz * NX + dy
        unit(q_row, buf[kind, at, 0], buf[kind, at, 1], False)

    @pl.loop(0, 2)
    def _(part):
        rows = pl.ds(pl.multiple_of(part * piece, piece), piece)
        for h in range(n_heads):
            cols = slice(h * HD, (h + 1) * HD)
            total = jnp.sum(l_ref[rows, cols], axis=1, keepdims=True)
            o_ref[rows, cols] = (acc_ref[rows, cols] / total).astype(BF16)

    for key in started:
        copy_of(*key).wait_send()


def attention(q, kv):
    rows, width = q.shape
    piece = kv.shape[2]
    sem = pltpu.SemaphoreType.DMA
    return pl.pallas_call(
        functools.partial(attention_kernel, width // HD),
        out_shape=jax.ShapeDtypeStruct((rows, width), BF16),
        in_specs=[vmem_spec()] * 2,
        out_specs=vmem_spec(),
        scratch_shapes=[pltpu.VMEM((rows, width), F32)] * 3 + [pltpu.VMEM((2, NX * NX, 2, piece, HD), BF16),
                                                              sem((40,)), sem((2, NX * NX, 2))],
        compiler_params=params(2, 48), name='attention',
        cost_estimate=pl.CostEstimate(flops=18 * 10 ** 9, bytes_accessed=10 * 2 ** 20, transcendentals=35 * 10 ** 6),
    )(q, kv)


def solution(mesh):
    row_spec = P('dp', ('cp', 'tp'), None)
    head_cols = P(None, 'tp', None)
    cp_size = mesh.shape['cp']

    def local_layer(x, g_attn, w_q, w_k, w_v, w_o, g_mlp, w_gate, w_up, w_down):
        x_rows = x[0]
        block, dim = x_rows.shape
        rows = block * mesh.shape['tp']
        piece = rows // 2
        cp_index = lax.axis_index('cp')
        n_heads = w_q.shape[1]
        j = jnp.arange(rows, dtype=jnp.int32)
        positions = jnp.where(j < piece, cp_index * piece + j, (2 * cp_size - 1 - cp_index) * piece + j - piece)
        cos, sin = rope_tables(positions)
        in_hbm = [pltpu.with_memory_space_constraint(v, pltpu.HBM) for v in (x_rows, w_q, w_k.reshape(dim, HD), w_v.reshape(dim, HD))]
        q, kv = gather_qkv(in_hbm[0], g_attn.reshape(dim // HD, HD), cos, sin, *in_hbm[1:], n_heads, piece)
        o = attention(q, kv)
        y_rows = scatter_product(o, w_o.reshape(n_heads * HD, dim), x_rows, 3)
        d_rows = mlp(y_rows, g_mlp.reshape(dim // HD, HD), w_gate, w_up, w_down)
        return (y_rows.astype(F32) + d_rows.astype(F32)).astype(BF16)[None]

    return jax.shard_map(local_layer, mesh=mesh,
                         in_specs=(row_spec, P(), head_cols, head_cols, head_cols, P('tp', None, None),
                                   P(), P(None, 'tp'), P(None, 'tp'), P('tp', None)),
                         out_specs=row_spec, check_vma=False)
```
